32 devices in a mesh: dp: 4 (over z), gx: 4 (over y, x), gy: 2 (over core).
Axes of the slice: x: 2, y: 2, z: 4, core: 2. Of those that a mesh axis runs over, the one named last changes fastest.
Arguments:
- block_input: bfloat16 [2, 576, 8192], P('gy', 'gx', 'dp'), may hold values from -6 to 6
- lengths: int32 [8, 6], P(('dp', 'gy')), may hold values from 0 to 512, as said below
- ln1_gain: float32 [2, 576], P('gy', 'gx'), may hold values from 0.1 to 1.9
- ln1_bias: float32 [2, 576], P('gy', 'gx'), may hold values from -3 to 3
- w_qkv: bfloat16 [2, 576, 3, 1152], P('gy', 'dp', None, 'gx'), may hold values from -0.1875 to 0.1875
- qv_bias: float32 [2, 1152], P(None, 'gx'), may hold values from -3 to 3
- w_out: bfloat16 [1152, 2, 576], P('gx', 'gy', 'dp'), may hold values from -1 to 1
- out_bias: float32 [2, 576], P('gy', 'gx'), may hold values from -3 to 3
- ln2_gain: float32 [2, 576], P('gy', 'gx'), may hold values from 0.1 to 1.9
- ln2_bias: float32 [2, 576], P('gy', 'gx'), may hold values from -3 to 3
- w_up: bfloat16 [2, 576, 4304], P('gy', 'dp', 'gx'), may hold values from -0.1875 to 0.1875
- up_bias: float32 [4304], P('gx'), may hold values from -3 to 3
- w_down: bfloat16 [4304, 2, 576], P('gx', 'gy', 'dp'), may hold values from -0.09375 to 0.09375
- down_bias: float32 [2, 576], P('gy', 'gx'), may hold values from -3 to 3
- cotangent: bfloat16 [2, 576, 8192], P('gy', 'gx', 'dp'), may hold values from -6 to 6
Outputs:
- block_output: bfloat16 [2, 576, 8192], P('gy', 'gx', 'dp')
- input_grad: float32 [2, 576, 8192], P('gy', 'gx', 'dp')
- grad_ln1_gain: float32 [2, 576], P('gy', 'gx')
- grad_ln1_bias: float32 [2, 576], P('gy', 'gx')
- grad_w_qkv: float32 [2, 576, 3, 1152], P('gy', 'dp', None, 'gx')
- grad_qv_bias: float32 [2, 1152], P(None, 'gx')
- grad_w_out: float32 [1152, 2, 576], P('gx', 'gy', 'dp')
- grad_out_bias: float32 [2, 576], P('gy', 'gx')
- grad_ln2_gain: float32 [2, 576], P('gy', 'gx')
- grad_ln2_bias: float32 [2, 576], P('gy', 'gx')
- grad_w_up: float32 [2, 576, 4304], P('gy', 'dp', 'gx')
- grad_up_bias: float32 [4304], P('gx')
- grad_w_down: float32 [4304, 2, 576], P('gx', 'gy', 'dp')
- grad_down_bias: float32 [2, 576], P('gy', 'gx')
The draws below stay inside these ranges and needn't reach their ends.
Inputs may be any that keep to these rules, and one draw needn't show every extreme that they name: In each row the nonzero lengths come first, each between 100 and 512, and sum to at most 1024; a zero marks an unused slot; the first slot of every row is used; some row holds a picture of 512 patches.
All inputs are finite; a program needn't handle non-finite values.
Results may differ from the reference program's by a relative error of at most 0.019.
Values may be sent and summed in bfloat16 or wider, within the bound.
A program may use at most 128 MiB of HBM per device.

```python
from functools import partial
import jax
import jax.numpy as jnp
from jax import lax

D = 1152
HEADS = 16
HEAD_DIM = 72
FF = 4304
LEN = 1024
NPIC = 6
MINPIC = 100
MAXPIC = 512
DH = 576
PACKED = 8
TOKENS = 8192
N_GY = 2


def draw_lengths(key, part):
    size_key, row_key = jax.random.split(key)
    slot_sizes = jax.random.randint(size_key, (PACKED, NPIC), MINPIC, MAXPIC + 1)
    chosen_row = jax.random.randint(row_key, (), 0, PACKED)
    first_slot = (lax.iota(jnp.int32, NPIC) == 0)[None, :] & (lax.iota(jnp.int32, PACKED) == chosen_row)[:, None]
    slot_sizes = jnp.where(first_slot, MAXPIC, slot_sizes)
    slot_ends = jnp.cumsum(slot_sizes, axis=1)
    return jnp.where(slot_ends <= LEN, slot_sizes, 0).astype(jnp.int32)


def strengthened(values, stream_key, source, target, shards_of, factor):
    def block_of(axis_at):
        return (jnp.arange(values.shape[axis_at]) // (values.shape[axis_at] // shards_of)).reshape((-1,) + (1,) * (values.ndim - 1 - axis_at))

    near = jax.random.permutation(stream_key, shards_of)[block_of(target)]
    other_side = (block_of(target) + shards_of // 2) % shards_of
    return jnp.where((block_of(source) == near) | (block_of(source) == other_side), factor * values, values)


def level_of(own_key, dims, pieces, least, top_value):
    def one(dim, parts):
        heights = jax.random.uniform(jax.random.fold_in(jax.random.fold_in(own_key, 6), dim), (parts,), jnp.float32, least / len(pieces), top_value / len(pieces))
        return jnp.repeat(jnp.exp(heights), dims[dim] // parts).reshape((-1,) + (1,) * (len(dims) - dim - 1))

    gain = one(*pieces[0])
    for cut in pieces[1:]:
        gain = gain * one(*cut)
    return gain


def gaussian(stream_key, shape, scale, reach, pieces=(), held_as=jnp.bfloat16):
    factor_of = level_of(stream_key, shape, pieces, -0.22, 0.18) if pieces else 1.0
    values = jax.random.normal(stream_key, shape, jnp.float32) * scale * factor_of
    return jnp.minimum(jnp.maximum(values, -reach), reach).astype(held_as)


def heavy_noise(own_key, extent, scale, limit, pieces, heavy, held_as=jnp.bfloat16):
    values = scale * jax.random.normal(own_key, extent, jnp.float32)
    if pieces:
        values = values * level_of(own_key, extent, pieces, -0.22, 0.18)
    return jnp.clip(strengthened(values, jax.random.fold_in(own_key, 3), *heavy), -limit, limit).astype(held_as)


def setup_inputs(seed: int = 0) -> dict:
    key_list = jax.random.split(jax.random.key(seed), 16)
    block_input = gaussian(key_list[0], (N_GY, DH, TOKENS), 1.0, 6.0, ((0, 2), (1, 4), (2, 4)))
    lengths = draw_lengths(jax.random.fold_in(key_list[15], 71), 0)
    ln1_gain = jnp.clip(1.0 + 0.18 * jax.random.normal(key_list[2], (N_GY, DH), jnp.float32), 0.1, 1.9)
    ln1_bias = gaussian(key_list[3], (N_GY, DH), 0.5, 3.0, ((0, 2), (1, 4)), jnp.float32)
    w_qkv = gaussian(key_list[4], (N_GY, DH, 3, D), D ** -0.5, 0.1875, ((0, 2), (1, 4), (3, 4)))
    qv_bias = gaussian(key_list[5], (2, D), 0.5, 3.0, ((1, 4),), jnp.float32)
    w_out = gaussian(key_list[6], (D, N_GY, DH), (D // 32) ** -0.5, 1.0, ((0, 4), (1, 2), (2, 4)))
    out_bias = gaussian(key_list[7], (N_GY, DH), 0.5, 3.0, ((0, 2), (1, 4)), jnp.float32)
    ln2_gain = jnp.clip(1.0 + 0.18 * jax.random.normal(key_list[8], (N_GY, DH), jnp.float32), 0.1, 1.9)
    ln2_bias = gaussian(key_list[9], (N_GY, DH), 0.5, 3.0, ((0, 2), (1, 4)), jnp.float32)
    w_up = gaussian(key_list[10], (N_GY, DH, FF), D ** -0.5, 0.1875, ((0, 2), (1, 4), (2, 4)))
    up_bias = gaussian(key_list[11], (FF,), 0.5, 3.0, ((0, 4),), jnp.float32)
    w_down = gaussian(key_list[12], (FF, N_GY, DH), FF ** -0.5, 0.09375, ((0, 4), (1, 2), (2, 4)))
    down_bias = gaussian(key_list[13], (N_GY, DH), 0.5, 3.0, ((0, 2), (1, 4)), jnp.float32)
    cotangent = heavy_noise(key_list[14], (N_GY, DH, TOKENS), 1.0, 6.0, ((0, 2), (1, 4), (2, 4)), (2, 1, 4, 2.0))
    return dict(block_input=block_input, lengths=lengths, ln1_gain=ln1_gain, ln1_bias=ln1_bias, w_qkv=w_qkv, qv_bias=qv_bias, w_out=w_out, out_bias=out_bias, ln2_gain=ln2_gain, ln2_bias=ln2_bias, w_up=w_up, up_bias=up_bias, w_down=w_down, down_bias=down_bias, cotangent=cotangent)


EPSILON = 1e-06
HIGH = lax.Precision.HIGHEST

@jax.custom_vjp
def low(v):
    return lax.optimization_barrier(v.astype(jnp.bfloat16)).astype(jnp.float32)

@jax.custom_vjp
def low_back(v):
    return v

def low_keep(v):
    return (low(v), None)

def low_pass(kept, grad):
    return (grad,)

def back_keep(v):
    return (v, None)

def back_low(kept, grad):
    return (low(grad),)
low.defvjp(low_keep, low_pass)
low_back.defvjp(back_keep, back_low)

def layer_norm(stream, gain_row, shift_row):
    average = lax.optimization_barrier(jnp.mean(stream, axis=1, keepdims=True))
    spread = lax.optimization_barrier(jnp.mean(stream * stream, axis=1, keepdims=True)) - average * average
    return (stream - average) * lax.rsqrt(spread + EPSILON) * gain_row.reshape(D) + shift_row.reshape(D)

def attend(packed):
    queries, key_rows, values, picture, valid_token = packed
    factor = HEAD_DIM ** (-0.5)
    scores = low_back(jnp.einsum('qhd,khd->hqk', queries, key_rows, precision=HIGH) * factor)
    allowed = ((picture[:, None] == picture[None, :]) & valid_token[None, :])[None]
    weight_kept = jnp.where(allowed, jnp.exp(scores), 0.0)
    denominator = jnp.where(valid_token[None, :], lax.optimization_barrier(jnp.sum(weight_kept, axis=2)), 1.0)
    probs_low = low(weight_kept / denominator[:, :, None])
    return jnp.einsum('hqk,khd->qhd', probs_low, values, precision=HIGH)

def forward(picture, valid_token, block_input, ln1_gain, ln1_bias, w_qkv, qv_bias, w_out, out_bias, ln2_gain, ln2_bias, w_up, up_bias, w_down, down_bias):
    tokens = jnp.transpose(block_input, (2, 0, 1)).reshape(TOKENS, D)
    hidden1 = low(layer_norm(tokens, ln1_gain, ln1_bias))
    projected = jnp.dot(hidden1, w_qkv.reshape(D, 3 * D), precision=HIGH).reshape(TOKENS, 3, D)
    queries = low(low_back(projected[:, 0] + qv_bias[0]))
    key_rows = low(low_back(projected[:, 1]))
    values = low(low_back(projected[:, 2] + qv_bias[1]))
    shape_four = (PACKED, LEN, HEADS, HEAD_DIM)
    attended = lax.map(jax.checkpoint(attend), (queries.reshape(shape_four), key_rows.reshape(shape_four), values.reshape(shape_four), picture, valid_token))
    attended = low(low_back(attended.reshape(TOKENS, D)))
    branch = low_back(jnp.dot(attended, w_out.reshape(D, D), precision=HIGH) + out_bias.reshape(D))
    residual = tokens + branch
    hidden2 = low(layer_norm(residual, ln2_gain, ln2_bias))
    pre_act = low_back(jnp.dot(hidden2, w_up.reshape(D, FF), precision=HIGH) + up_bias)
    activated = low(jax.nn.gelu(pre_act, approximate=True))
    mlp_out = low_back(jnp.dot(activated, w_down.reshape(FF, D), precision=HIGH) + down_bias.reshape(D))
    return jnp.transpose((residual + mlp_out).reshape(TOKENS, N_GY, D // N_GY), (1, 2, 0))

def reference(block_input, lengths, ln1_gain, ln1_bias, w_qkv, qv_bias, w_out, out_bias, ln2_gain, ln2_bias, w_up, up_bias, w_down, down_bias, cotangent):
    slot_ends = jnp.cumsum(lengths, axis=1)
    position = jnp.arange(LEN, dtype=jnp.int32)
    picture = lax.optimization_barrier(jnp.sum((position[None, :, None] >= slot_ends[:, None, :]).astype(jnp.int32), axis=2))
    valid_token = position[None, :] < slot_ends[:, -1:]
    params = tuple((array.astype(jnp.float32) for array in (block_input, ln1_gain, ln1_bias, w_qkv, qv_bias, w_out, out_bias, ln2_gain, ln2_bias, w_up, up_bias, w_down, down_bias)))
    result, pullback = jax.vjp(partial(forward, picture, valid_token), *params)
    gradients = pullback(cotangent.astype(jnp.float32))
    return (result.astype(jnp.bfloat16), gradients[0], gradients[1], gradients[2], gradients[3], gradients[4], gradients[5], gradients[6], gradients[7], gradients[8], gradients[9], gradients[10], gradients[11], gradients[12])
```

```python
import functools

import jax
import jax.numpy as jnp
from jax import lax
from jax.experimental import pallas as pl
from jax.experimental.pallas import tpu as pltpu
from jax.sharding import PartitionSpec as P

HEAD_DIM = 72
HEAD_PAD = 80
EPSILON = 1e-06
MESH = pl.DeviceIdType.MESH
BF16 = jnp.bfloat16
F32 = jnp.float32
NN = (((1,), (0,)), ((), ()))
NT = (((1,), (1,)), ((), ()))
TN = (((0,), (0,)), ((), ()))
GELU_A = 0.044715
GELU_C = 0.7978845608028654


def mm(a, b, dims):
    return lax.dot_general(a, b, dims, preferred_element_type=F32)


def round_up(value, unit):
    return (value + unit - 1) // unit * unit


def block_kernel(
    cfg,
    len_ref,
    prm_ref,
    x_ref,
    cot_ref,
    wq_in,
    wo_in,
    wu_in,
    wd_in,
    qb_ref,
    ub_ref,
    out_ref,
    ig_ref,
    dq_out,
    do_out,
    du_out,
    dd_out,
    sm_out,
    prm_all,
    prm_col,
    x_t,
    cot_t,
    h1_t,
    h2_t,
    gb_t,
    wq,
    wo,
    wu,
    wd,
    qkv_t,
    att_t,
    gatt_t,
    act_t,
    gpre_t,
    resid,
    tsend,
    trecv,
    mrecv,
    grecv,
    dk_acc,
    dv_acc,
    fa,
    fb,
    pk,
    rows_f,
    sums_col,
    uv_send,
    uv_recv,
    sm_send,
    sm_recv,
    smz_recv,
    cq,
    co,
    cu,
    cd,
    zq,
    zo,
    zu,
    zd,
    sem_s,
    sem_r,
):
    nz, zin = cfg["nz"], cfg["zin"]
    fb_rows, tok, heads = cfg["fb"], cfg["tok"], cfg["heads"]
    half, width = 4 * fb_rows, 8 * fb_rows
    tb = tok // 4
    hp = heads * HEAD_PAD
    factor = HEAD_DIM ** (-0.5)
    z, g, c = lax.axis_index("dp"), lax.axis_index("gx"), lax.axis_index("gy")
    g_hi, g_lo = g // 2, g % 2

    def gx_of(dd):
        return ((g_hi + dd // 2) % 2) * 2 + (g_lo + dd % 2) % 2

    def row_of(dc):
        return (c + dc) % 2

    counter = [0]

    def take(count):
        first = counter[0]
        counter[0] += count
        return first

    def rcopy(src, dst, sem, dev):
        return pltpu.make_async_remote_copy(
            src_ref=src,
            dst_ref=dst,
            send_sem=sem_s.at[sem],
            recv_sem=sem_r.at[sem],
            device_id=dev,
            device_id_type=MESH,
        )

    def lcopy(src, dst, sem):
        return pltpu.make_async_copy(src, dst, sem_r.at[sem])

    others = [(dd, dc) for dd in (1, 2, 3, 0) for dc in (0, 1) if dd or dc]

    def feat(dd, dc):
        return pl.ds(pl.multiple_of(row_of(dc) * half + gx_of(dd) * fb_rows, 16), fb_rows)

    def toks(j):
        return pl.ds(pl.multiple_of(j * tb, 128), tb)

    pending = []

    barrier = pltpu.get_barrier_semaphore()
    for dd, dc in others:
        pl.semaphore_signal(barrier, inc=1, device_id=(z, gx_of(dd), row_of(dc)), device_id_type=MESH)
    for k in range(1, nz):
        pl.semaphore_signal(barrier, inc=1, device_id=((z + k) % nz, g, c), device_id_type=MESH)
    pl.semaphore_wait(barrier, 7 + nz - 1)

    own_feat = feat(0, 0)

    p0 = take(8)
    xs0 = take(8)
    cs0 = take(8)
    me = c * 4 + g

    def exchange(first, src_of, dst, start=True):
        copies = {}
        for dd, dc in others:
            cp = rcopy(src_of(dd, dc), dst, first + dd * 2 + dc, (z, gx_of(dd), row_of(dc)))
            cp.start()
            copies[(dd, dc)] = cp
            pending.append(cp)
        return copies

    cp_prm = exchange(p0, lambda dd, dc: prm_ref, prm_all.at[me])

    def row_tok(dc):
        return pl.ds(pl.multiple_of(row_of(dc) * tok, 128), tok)

    exchange(xs0, lambda dd, dc: x_ref.at[:, row_tok(dc)], x_t.at[own_feat, :])
    own_x = lcopy(x_ref.at[:, row_tok(0)], x_t.at[own_feat, :], xs0)
    own_x.start()
    own_prm = lcopy(prm_ref, prm_all.at[me], p0)
    own_prm.start()

    weights = ((wq_in, wq), (wo_in, wo), (wu_in, wu), (wd_in, wd))
    wz0 = take(4 * nz)
    wc0 = take(4 * nz)

    def zrows(zz, core):
        return pl.ds(pl.multiple_of(core * half + zz * fb_rows, 16), fb_rows)

    partner = (z, g, 1 - c)
    if zin:
        for i, (src, dst) in enumerate(weights):
            for k in range(1, nz):
                cp = rcopy(src, dst.at[zrows(z, c), :], wz0 + i * nz + k, ((z + k) % nz, g, c))
                cp.start()
                pending.append(cp)
            lcopy(src, dst.at[zrows(z, c), :], wz0 + i * nz).start()
            cp = rcopy(src, dst.at[zrows(z, c), :], wc0 + i * nz, partner)
            cp.start()
            pending.append(cp)
    else:
        for i, (src, dst) in enumerate(weights):
            lcopy(src, dst, wz0 + i * nz).start()

    passed = [[], [], [], []]

    def weight_passed(i):
        for cp in passed[i]:
            cp.wait_send()

    def weight_ready(i):
        src, dst = weights[i]
        if not zin:
            lcopy(src, dst, wz0 + i * nz).wait()
            return
        for k in range(1, nz):
            zz = (z + nz - k) % nz
            rows = dst.at[zrows(zz, c), :]
            rcopy(src, rows, wz0 + i * nz + k, partner).wait_recv()
            cp = rcopy(rows, rows, wc0 + i * nz + k, partner)
            cp.start()
            passed[i].append(cp)
        lcopy(src, dst.at[zrows(z, c), :], wz0 + i * nz).wait()
        for k in range(nz):
            zz = (z + nz - k) % nz
            rcopy(src, dst.at[zrows(zz, 1 - c), :], wc0 + i * nz + k, partner).wait_recv()

    exchange(cs0, lambda dd, dc: cot_ref.at[:, row_tok(dc)], cot_t.at[own_feat, :])
    own_cot = lcopy(cot_ref.at[:, row_tok(0)], cot_t.at[own_feat, :], cs0)
    own_cot.start()

    def wait_feat(first, src, dst, own):
        own.wait()
        for dd, dc in others:
            rcopy(src.at[:, row_tok(0)], dst.at[feat(dd, dc), :], first + dd * 2 + dc, partner).wait_recv()

    ends = []
    total = len_ref[0, 0]
    ends.append(total)
    for s in range(1, len_ref.shape[1]):
        total = total + len_ref[0, s]
        ends.append(total)

    def pictures(pos):
        picture = jnp.zeros_like(pos)
        for end in ends:
            picture = picture + jnp.where(pos >= end, 1, 0)
        return picture

    pos_col = lax.broadcasted_iota(jnp.int32, (tok, 128), 0)
    pk[...] = jnp.where(pos_col < total, pictures(pos_col), -1)
    pos_row = lax.broadcasted_iota(jnp.int32, (8, tok), 1)
    pic_row = pictures(pos_row)
    rows_f[0, :, :] = pic_row.astype(F32)
    rows_f[1, :, :] = jnp.where(pos_row < total, 1.0, 0.0)
    sums_col[...] = jnp.zeros_like(sums_col)
    att_t[...] = jnp.zeros_like(att_t)

    own_prm.wait()
    for dd, dc in others:
        rcopy(prm_ref, prm_all.at[row_of(dc) * 4 + gx_of(dd)], p0 + dd * 2 + dc, partner).wait_recv()
    for b in range(8):
        rows = jnp.concatenate([prm_all[b], jnp.zeros((120, 256), F32)], axis=0)
        prm_col[b * fb_rows : (b + 1) * fb_rows, :] = jnp.transpose(rows)[:fb_rows, :]

    def par(k):
        return prm_col[:, k : k + 1]

    wait_feat(xs0, x_ref, x_t, own_x)

    def ln1(j, carry):
        t = toks(j)
        x = x_t[:, t].astype(F32)
        m = jnp.sum(x, axis=0, keepdims=True) * (1.0 / width)
        q = jnp.sum(x * x, axis=0, keepdims=True) * (1.0 / width)
        r = lax.rsqrt(q - m * m + EPSILON)
        rows_f[2, 0:1, t] = m
        rows_f[3, 0:1, t] = r
        h1_t[:, t] = ((x - m) * r * par(0) + par(1)).astype(BF16)
        return carry

    lax.fori_loop(0, 4, ln1, 0)

    weight_ready(0)

    def project(j, carry):
        t = toks(j)
        qkv_t[:, t] = (mm(wq[...], h1_t[:, t], TN) + qb_ref[...]).astype(BF16)
        return carry

    lax.fori_loop(0, 4, project, 0)

    def head_rows(part, h):
        return pl.ds(pl.multiple_of((part * heads + h) * HEAD_PAD, 16), HEAD_PAD)

    def kept_of(h, t):
        scores = mm(qkv_t[head_rows(1, h), :], qkv_t[head_rows(0, h), t], TN) * factor
        key_pic = pk[...]
        query_pic = rows_f[0, 0:1, t].astype(jnp.int32)
        allowed = jnp.concatenate([key_pic] * (tb // 128), axis=1) == query_pic
        return jnp.where(allowed, jnp.exp(scores), 0.0)

    br0 = take(4)
    weight_ready(1)

    def attend(i, carry):
        dd = 3 - i
        j = gx_of(dd)
        t = toks(j)

        def head(h, inner):
            kept = kept_of(h, t)
            den = jnp.sum(kept, axis=0, keepdims=True)
            den = jnp.where(rows_f[1, 0:1, t] > 0.5, den, 1.0)
            scale = jnp.where(den > 1e30, 2.0**-40, 1.0)
            inv = 1.0 / (den * scale)
            rows_f[4 + 2 * h, 0:1, t] = scale
            rows_f[5 + 2 * h, 0:1, t] = inv
            probs = (kept * scale * inv).astype(BF16)
            att = mm(qkv_t[head_rows(2, h), :], probs, NN)
            att_t[head_rows(0, h), t] = att.astype(BF16)
            return inner

        lax.fori_loop(0, heads, head, 0)
        fa[...] = mm(wo[...], att_t[:, t], NN)
        for step in (3, 2, 1):

            @pl.when(i == 3 - step)
            def _(step=step):
                gb_t[:, t] = fa[...].astype(BF16)
                rcopy(gb_t.at[:, t], trecv.at[step - 1], br0 + step, (z, gx_of(step), c)).start()

        return carry

    lax.fori_loop(0, 4, attend, 0)

    def wait_tokens(first, step):
        rcopy(gb_t.at[:, toks(g)], trecv.at[step - 1], first + step, partner).wait_recv()

    def wait_tokens_sent(first):
        for step in (1, 2, 3):
            rcopy(gb_t.at[:, toks(gx_of(step))], trecv.at[step - 1], first + step, partner).wait_send()

    weight_ready(2)
    weight_ready(3)

    own_t = toks(g)
    for step in (3, 2, 1):
        wait_tokens(br0, step)
    residual = (
        x_t[:, own_t].astype(F32)
        + fa[...]
        + trecv[0].astype(F32)
        + trecv[1].astype(F32)
        + trecv[2].astype(F32)
        + par(2)
    )
    resid[...] = residual
    m2 = jnp.sum(residual, axis=0, keepdims=True) * (1.0 / width)
    q2 = jnp.sum(residual * residual, axis=0, keepdims=True) * (1.0 / width)
    r2 = lax.rsqrt(q2 - m2 * m2 + EPSILON)
    rows_f[2, 1:2, own_t] = m2
    rows_f[3, 1:2, own_t] = r2
    h2_t[:, own_t] = ((residual - m2) * r2 * par(3) + par(4)).astype(BF16)

    def spread(first, buf):
        copies = []
        for step in (3, 1, 2):
            cp = rcopy(buf.at[:, own_t], buf.at[:, own_t], first + step, (z, gx_of(step), c))
            cp.start()
            copies.append(cp)
        return copies

    def wait_block(first, buf, step):
        t = toks(gx_of(step))
        rcopy(buf.at[:, t], buf.at[:, t], first + step, partner).wait_recv()

    h20 = take(4)
    h2_copies = spread(h20, h2_t)
    wait_tokens_sent(br0)
    wait_feat(cs0, cot_ref, cot_t, own_cot)

    g20 = take(4)

    def mlp(i, carry):
        j = gx_of(i)
        t = toks(j)
        for step in (1, 2, 3):

            @pl.when(i == step)
            def _(step=step):
                wait_block(h20, h2_t, step)

        fa[...] = mm(wu[...], h2_t[:, t], TN) + ub_ref[...]
        fb[...] = mm(wd[...], cot_t[:, t], TN)

        def chunk(n, inner):
            rows = pl.ds(pl.multiple_of(n * 48, 16), 48)
            v = fa[rows, :]
            v2 = v * v
            th = jnp.tanh(GELU_C * (v + GELU_A * v2 * v))
            hf = 0.5 * (1.0 + th)
            act_t[rows, t] = (v * hf).astype(BF16)
            slope = hf + (0.5 * GELU_C) * v * (1.0 - th * th) * (1.0 + (3.0 * GELU_A) * v2)
            gpre_t[rows, t] = (fb[rows, :] * slope).astype(BF16)
            return inner

        lax.fori_loop(0, fa.shape[0] // 48, chunk, 0)
        fa[...] = mm(wu[...], gpre_t[:, t], NN)
        for step in (1, 2, 3):

            @pl.when(i == step)
            def _(step=step):
                tsend[step - 1] = fa[...].astype(BF16)
                rcopy(tsend.at[step - 1], trecv.at[step - 1], g20 + step, (z, gx_of(step), c)).start()

        @pl.when(i == 0)
        def _():
            gb_t[:, t] = fa[...].astype(BF16)

        return carry

    lax.fori_loop(0, 4, mlp, 0)

    lane_block = 384
    dwc0 = take(4)

    def weight_grad(i, left, right):
        weight_passed(i)
        dst = w_refs[i]
        cols = dst.shape[1]
        step_cols = lane_block if cols % lane_block == 0 else 256

        def one(n, carry):
            cs = pl.ds(pl.multiple_of(n * step_cols, 128), step_cols)
            dst[:, cs] = mm(left[...], right[pl.ds(pl.multiple_of(n * step_cols, 16), step_cols), :], NT).astype(BF16)
            return carry

        lax.fori_loop(0, cols // step_cols, one, 0)

    core_recv = (cq, co, cu, cd)
    z_recv = (zq, zo, zu, zd)
    w_refs = (wq, wo, wu, wd)
    dw_outs = (dq_out, do_out, du_out, dd_out)

    def core_half(core):
        return pl.ds(pl.multiple_of(core * half, 16), half)

    def send_core(i):
        if zin:
            cp = rcopy(w_refs[i].at[core_half(1 - c), :], core_recv[i], dwc0 + i, partner)
            cp.start()
            pending.append(cp)
        else:
            cp = lcopy(w_refs[i], dw_outs[i], dwc0 + i)
            cp.start()

    dwz0 = take(4 * nz)
    do0 = take(16)
    slots = [0]
    leaving = []

    def sum_core(i):
        if not zin:
            return
        rcopy(w_refs[i].at[core_half(c), :], core_recv[i], dwc0 + i, partner).wait_recv()
        w = w_refs[i]
        for zz in range(nz):
            rows = pl.ds(pl.multiple_of(c * half + zz * fb_rows, 16), fb_rows)
            w[rows, :] = (
                w[rows, :].astype(F32) + core_recv[i][zz * fb_rows : (zz + 1) * fb_rows, :].astype(F32)
            ).astype(BF16)
        for k in range(1, nz):
            zz = (z + k) % nz
            cp = rcopy(w.at[zrows(zz, c), :], z_recv[i].at[k - 1], dwz0 + i * nz + k, (zz, g, c))
            cp.start()
            pending.append(cp)

    def sum_z(i):
        if not zin:
            lcopy(w_refs[i], dw_outs[i], dwc0 + i).wait()
            return
        for k in range(1, nz):
            rcopy(
                w_refs[i].at[zrows(z, c), :], z_recv[i].at[k - 1], dwz0 + i * nz + k, partner
            ).wait_recv()
        cols = w_refs[i].shape[1]
        for n in range(0, cols, tb):
            size = min(tb, cols - n)
            part = w_refs[i][zrows(z, c), n : n + size].astype(F32)
            for k in range(1, nz):
                part = part + z_recv[i][k - 1, :, n : n + size].astype(F32)
            slot = slots[0]
            slots[0] += 1
            stage = (fa, fb)[slot // 8].at[(slot % 8) * fb_rows : (slot % 8 + 1) * fb_rows, 0:size]
            stage[...] = part
            cp = lcopy(stage, dw_outs[i].at[:, n : n + size], do0 + slot)
            cp.start()
            leaving.append(cp)

    weight_grad(2, h2_t, gpre_t)
    send_core(2)
    ones = jnp.ones((tok, 128), BF16)
    sums_col[0 : act_t.shape[0], 6:7] = mm(gpre_t[...], ones, NN)[:, 0:1]

    for step in (1, 2, 3):
        wait_tokens(g20, step)
    gh2 = (
        gb_t[:, own_t].astype(F32)
        + trecv[0].astype(F32)
        + trecv[1].astype(F32)
        + trecv[2].astype(F32)
    )
    m2 = rows_f[2, 1:2, own_t]
    r2 = rows_f[3, 1:2, own_t]
    normed2 = (resid[...] - m2) * r2
    gn = gh2 * par(3)
    s1 = jnp.sum(gn, axis=0, keepdims=True) * (1.0 / width)
    s2 = jnp.sum(gn * normed2, axis=0, keepdims=True) * (1.0 / width)
    cot_own = cot_t[:, own_t].astype(F32)
    g_res = cot_own + r2 * (gn - s1 - normed2 * s2)
    fb[...] = g_res
    g_low = g_res.astype(BF16)
    for cp in h2_copies:
        cp.wait_send()
    wait_tokens_sent(g20)
    gb_t[:, own_t] = g_low
    gb0 = take(4)
    gb_copies = spread(gb0, gb_t)
    sums_col[0:width, 2:3] = jnp.sum(g_low.astype(F32), axis=1, keepdims=True)
    sums_col[0:width, 3:4] = jnp.sum(gh2 * normed2, axis=1, keepdims=True)
    sums_col[0:width, 4:5] = jnp.sum(gh2, axis=1, keepdims=True)
    sums_col[0:width, 5:6] = jnp.sum(cot_own, axis=1, keepdims=True)

    def lower(j, carry):
        t = toks(j)
        h2_t[:, t] = mm(wd[...], act_t[:, t], NN).astype(BF16)
        return carry

    lax.fori_loop(0, 4, lower, 0)
    h2_t[:, own_t] = (mm(wd[...], act_t[:, own_t], NN) + resid[...] + par(5)).astype(BF16)
    resid[...] = fb[...]
    ml0 = take(8)
    gh0 = take(8)
    uv0 = take(8)

    def scatter(first, recv):
        copies = []
        for dd, dc in others:
            cp = rcopy(
                h2_t.at[feat(dd, dc), :], recv.at[dd * 2 + dc], first + dd * 2 + dc, (z, gx_of(dd), row_of(dc))
            )
            cp.start()
            copies.append(cp)
        return copies

    ml_copies = scatter(ml0, mrecv)
    keep_own = lcopy(h2_t.at[own_feat, :], mrecv.at[0], ml0)
    keep_own.start()
    sum_core(2)

    weight_grad(3, cot_t, act_t)
    send_core(3)

    dk_acc[...] = jnp.zeros_like(dk_acc)
    dv_acc[...] = jnp.zeros_like(dv_acc)

    def attend_back(i, carry):
        j = gx_of(i)
        t = toks(j)
        for step in (1, 2, 3):

            @pl.when(i == step)
            def _(step=step):
                wait_block(gb0, gb_t, step)

        gatt_t[...] = mm(wo[...], gb_t[:, t], TN)[0:hp, :].astype(BF16)

        def head(h, inner):
            kept = kept_of(h, t)
            probs = kept * rows_f[4 + 2 * h, 0:1, t] * rows_f[5 + 2 * h, 0:1, t]
            q_rows = head_rows(0, h)
            grad = gatt_t[q_rows, :]
            grad_probs = mm(qkv_t[head_rows(2, h), :], grad, TN)
            weighted = probs * grad_probs
            delta = jnp.sum(weighted, axis=0, keepdims=True)
            grad_scores = (weighted - probs * delta).astype(BF16)
            act_t[q_rows, t] = (mm(qkv_t[head_rows(1, h), :], grad_scores, NN) * factor).astype(BF16)
            dk_acc[q_rows, :] += mm(qkv_t[q_rows, t], grad_scores, NT)
            dv_acc[q_rows, :] += mm(grad, probs.astype(BF16), NT)
            return inner

        lax.fori_loop(0, heads, head, 0)
        return carry

    lax.fori_loop(0, 4, attend_back, 0)
    act_t[hp : 2 * hp, :] = (dk_acc[...] * factor).astype(BF16)
    act_t[2 * hp : 3 * hp, :] = dv_acc[...].astype(BF16)
    kq = wq.shape[1]
    act_t[3 * hp : kq, :] = jnp.zeros((kq - 3 * hp, tok), BF16)
    sums_col[0:kq, 7:8] = mm(act_t[0:kq, :], ones, NN)[:, 0:1]
    for cp in ml_copies:
        cp.wait_send()
    keep_own.wait()
    sum_core(3)

    def back1(j, carry):
        t = toks(j)
        gh1 = mm(wq[...], act_t[0:kq, t], NN)
        m = rows_f[2, 0:1, t]
        r = rows_f[3, 0:1, t]
        normed = (x_t[:, t].astype(F32) - m) * r
        gn1 = gh1 * par(0)
        prod = gh1 * normed
        sums_col[0:width, 0:1] += jnp.sum(prod, axis=1, keepdims=True)
        sums_col[0:width, 1:2] += jnp.sum(gh1, axis=1, keepdims=True)
        a1 = jnp.sum(gn1, axis=0, keepdims=True) * (1.0 / width)
        a2 = jnp.sum(gn1 * normed, axis=0, keepdims=True) * (1.0 / width)
        v = r * r * a2
        uv_send[0:1, t] = r * a1 - m * v
        uv_send[1:2, t] = v
        fa[...] = r * gn1

        @pl.when(j == g)
        def _():
            fa[...] += resid[...]

        h2_t[:, t] = fa[...].astype(BF16)
        return carry

    lax.fori_loop(0, 4, back1, 0)
    gh_copies = scatter(gh0, grecv)
    keep_grad = lcopy(h2_t.at[own_feat, :], grecv.at[0], gh0)
    keep_grad.start()
    exchange(uv0, lambda dd, dc: uv_send, uv_recv.at[me])
    keep_uv = lcopy(uv_send, uv_recv.at[me], uv0)
    keep_uv.start()

    weight_grad(0, h1_t, act_t)
    send_core(0)
    weight_grad(1, gb_t, att_t)
    send_core(1)

    sm0 = take(8)
    sz0 = take(nz)
    for n in range(0, sm_send.shape[1], 128):
        sm_send[:, n : n + 128] = jnp.transpose(sums_col[n : n + 128, :])[0:8, :]
    exchange(sm0, lambda dd, dc: sm_send, sm_recv.at[me])
    sum_core(0)
    sum_core(1)

    total_sm = sm_send[...]
    row8 = lax.broadcasted_iota(jnp.int32, total_sm.shape, 0)
    for dd, dc in others:
        rcopy(sm_send, sm_recv.at[row_of(dc) * 4 + gx_of(dd)], sm0 + dd * 2 + dc, partner).wait_recv()
        part = sm_recv[row_of(dc) * 4 + gx_of(dd)]
        total_sm = total_sm + (part if dd == 0 else jnp.where(row8 < 6, part, 0.0))
    smz_recv[0] = total_sm
    for k in range(1, nz):
        cp = rcopy(smz_recv.at[0], smz_recv.at[k], sz0 + k, ((z + k) % nz, g, c))
        cp.start()
        pending.append(cp)

    for dd, dc in others:
        rcopy(h2_t.at[own_feat, :], mrecv.at[dd * 2 + dc], ml0 + dd * 2 + dc, partner).wait_recv()
    for dc in (0, 1):
        acc = mrecv[dc].astype(F32)
        for dd in (1, 2, 3):
            acc = acc + mrecv[dd * 2 + dc].astype(F32)
        out_ref[:, row_tok(dc)] = acc.astype(BF16)

    sum_z(2)
    sum_z(3)

    keep_grad.wait()
    keep_uv.wait()
    for dd, dc in others:
        rcopy(h2_t.at[own_feat, :], grecv.at[dd * 2 + dc], gh0 + dd * 2 + dc, partner).wait_recv()
        rcopy(uv_send, uv_recv.at[row_of(dc) * 4 + gx_of(dd)], uv0 + dd * 2 + dc, partner).wait_recv()
    for dc in (0, 1):
        acc = grecv[dc].astype(F32)
        uv = uv_recv[row_of(dc) * 4 + g]
        for dd in (1, 2, 3):
            acc = acc + grecv[dd * 2 + dc].astype(F32)
            uv = uv + uv_recv[row_of(dc) * 4 + gx_of(dd)]
        x_own = x_ref[:, row_tok(dc)].astype(F32)
        ig_ref[:, row_tok(dc)] = acc - uv[0:1, :] - x_own * uv[1:2, :]

    total_z = smz_recv[0]
    for k in range(1, nz):
        rcopy(smz_recv.at[0], smz_recv.at[k], sz0 + k, partner).wait_recv()
        total_z = total_z + smz_recv[k]
    sm_out[...] = total_z
    sum_z(0)
    sum_z(1)

    for cp in leaving:
        cp.wait()
    for cp in pending + gb_copies + gh_copies:
        cp.wait_send()


def local(
    block_input,
    lengths,
    ln1_gain,
    ln1_bias,
    w_qkv,
    qv_bias,
    w_out,
    out_bias,
    ln2_gain,
    ln2_bias,
    w_up,
    up_bias,
    w_down,
    down_bias,
    cotangent,
):
    nz = lax.axis_size("dp")
    fb_rows, tok2 = block_input.shape[1], block_input.shape[2]
    tok = tok2 // 2
    width = 8 * fb_rows
    heads = w_qkv.shape[3] // HEAD_DIM
    hp = heads * HEAD_PAD
    kq, ko = round_up(3 * hp, 128), round_up(hp, 128)
    hid = w_up.shape[2]
    kh = round_up(hid, 384)
    zrow = w_qkv.shape[1]
    zin = zrow == fb_rows and nz == 4

    def pad_heads(a):
        parts = a.shape[-1] // HEAD_DIM
        a = a.reshape(a.shape[:-1] + (parts, HEAD_DIM))
        a = jnp.pad(a, [(0, 0)] * (a.ndim - 1) + [(0, HEAD_PAD - HEAD_DIM)])
        return a.reshape(a.shape[:-2] + (parts * HEAD_PAD,))

    def widen(a, cols):
        return jnp.pad(a, ((0, 0), (0, cols - a.shape[1])))

    prm = jnp.concatenate([ln1_gain, ln1_bias, out_bias, ln2_gain, ln2_bias, down_bias], axis=0)
    prm = jnp.pad(prm, ((0, 2), (0, 256 - fb_rows)))
    wq = widen(pad_heads(w_qkv[0].reshape(zrow, -1)), kq)
    wo = widen(pad_heads(jnp.transpose(w_out[:, 0, :])), ko)
    wu = widen(w_up[0], kh)
    wd = widen(jnp.transpose(w_down[:, 0, :]), kh)
    qb = jnp.concatenate([qv_bias[0:1], jnp.zeros_like(qv_bias[0:1]), qv_bias[1:2]], axis=1)
    qb = widen(pad_heads(qb), kq).reshape(kq, 1)
    ub = jnp.pad(up_bias, (0, kh - hid)).reshape(kh, 1)
    if not zin:
        wq, wo, wu, wd = (
            lax.all_gather(lax.all_gather(w, "dp", axis=0, tiled=True), "gy", axis=0, tiled=True)
            for w in (wq, wo, wu, wd)
        )

    cfg = dict(nz=nz, zin=zin, fb=fb_rows, tok=tok, heads=heads)
    tb = tok // 4
    half = width // 2
    vm = pltpu.VMEM
    n_sems = 8 * 3 + 8 * nz + 4 * 4 + 4 + 4 * nz + 8 * 4 + nz + 24
    dw_specs = [pl.BlockSpec(memory_space=pl.ANY)] * 4
    if zin:
        dw_shapes = tuple(jax.ShapeDtypeStruct((fb_rows, k), F32) for k in (kq, ko, kh, kh))
        core_shapes = [vm((half, k), BF16) for k in (kq, ko, kh, kh)]
        z_shapes = [vm((nz - 1, fb_rows, k), BF16) for k in (kq, ko, kh, kh)]
    else:
        dw_shapes = tuple(jax.ShapeDtypeStruct((width, k), BF16) for k in (kq, ko, kh, kh))
        core_shapes = [vm((16, 128), BF16)] * 4
        z_shapes = [vm((16, 128), BF16)] * 4
    scratch = [
        vm((8, 8, 256), F32),
        vm((width, 128), F32),
        vm((width, tok), BF16),
        vm((width, tok), BF16),
        vm((width, tok), BF16),
        vm((width, tok), BF16),
        vm((width, tok), BF16),
        vm((width, kq), BF16),
        vm((width, ko), BF16),
        vm((width, kh), BF16),
        vm((width, kh), BF16),
        vm((kq, tok), BF16),
        vm((ko, tok), BF16),
        vm((hp, tb), BF16),
        vm((kh, tok), BF16),
        vm((kh, tok), BF16),
        vm((width, tb), F32),
        vm((3, width, tb), BF16),
        vm((3, width, tb), BF16),
        vm((8, fb_rows, tok), BF16),
        vm((8, fb_rows, tok), BF16),
        vm((hp, tok), F32),
        vm((hp, tok), F32),
        vm((max(width, kh), tb), F32),
        vm((max(width, kh), tb), F32),
        vm((tok, 128), jnp.int32),
        vm((4 + 2 * heads, 8, tok), F32),
        vm((max(width, kh), 128), F32),
        vm((8, tok), F32),
        vm((8, 8, tok), F32),
        vm((8, max(width, kh)), F32),
        vm((8, 8, max(width, kh)), F32),
        vm((nz, 8, max(width, kh)), F32),
        *core_shapes,
        *z_shapes,
        pltpu.SemaphoreType.DMA((n_sems,)),
        pltpu.SemaphoreType.DMA((n_sems,)),
    ]
    any_spec = pl.BlockSpec(memory_space=pl.ANY)
    vmem_spec = pl.BlockSpec(memory_space=pltpu.VMEM)
    out, ig, dq, do, du, dd, sm = pl.pallas_call(
        functools.partial(block_kernel, cfg),
        out_shape=(
            jax.ShapeDtypeStruct((fb_rows, tok2), BF16),
            jax.ShapeDtypeStruct((fb_rows, tok2), F32),
            *dw_shapes,
            jax.ShapeDtypeStruct((8, max(width, kh)), F32),
        ),
        in_specs=[
            pl.BlockSpec(memory_space=pltpu.SMEM),
            vmem_spec,
            vmem_spec,
            any_spec,
            any_spec,
            any_spec,
            any_spec,
            any_spec,
            vmem_spec,
            vmem_spec,
        ],
        out_specs=(vmem_spec, vmem_spec, *dw_specs, vmem_spec),
        scratch_shapes=scratch,
        compiler_params=pltpu.CompilerParams(
            collective_id=0, has_side_effects=True, vmem_limit_bytes=67043328
        ),
        name="encoder_block",
    )(lengths, prm, block_input[0], cotangent[0], wq, wo, wu, wd, qb, ub)

    if not zin:

        def reduce(a):
            a = lax.psum_scatter(a, "gy", scatter_dimension=0, tiled=True)
            return lax.optimization_barrier(lax.psum_scatter(a, "dp", scatter_dimension=0, tiled=True)).astype(F32)

        dq, do, du, dd = reduce(dq), reduce(do), reduce(du), reduce(dd)

    def cut_heads(a):
        parts = a.shape[-1] // HEAD_PAD
        a = a.reshape(a.shape[:-1] + (parts, HEAD_PAD))[..., :HEAD_DIM]
        return a.reshape(a.shape[:-2] + (parts * HEAD_DIM,))

    mine = lax.axis_index("gy") * (width // 2) + lax.axis_index("gx") * fb_rows
    feats = lax.dynamic_slice(sm, (0, mine), (6, fb_rows))
    qkv_sum = cut_heads(sm[7:8, : 3 * hp]).reshape(3, -1)
    return (
        out[None],
        ig[None],
        feats[0:1],
        feats[1:2],
        cut_heads(dq[:, : 3 * hp]).reshape(1, zrow, 3, -1),
        jnp.stack([qkv_sum[0], qkv_sum[2]]),
        jnp.transpose(cut_heads(do[:, :hp]))[:, None, :],
        feats[2:3],
        feats[3:4],
        feats[4:5],
        du[None, :, :hid],
        sm[6, :hid],
        jnp.transpose(dd[:, :hid])[:, None, :],
        feats[5:6],
    )


def solution(mesh):
    in_specs = (
        P("gy", "gx", "dp"),
        P(("dp", "gy"), None),
        P("gy", "gx"),
        P("gy", "gx"),
        P("gy", "dp", None, "gx"),
        P(None, "gx"),
        P("gx", "gy", "dp"),
        P("gy", "gx"),
        P("gy", "gx"),
        P("gy", "gx"),
        P("gy", "dp", "gx"),
        P("gx"),
        P("gx", "gy", "dp"),
        P("gy", "gx"),
        P("gy", "gx", "dp"),
    )
    out_specs = (
        P("gy", "gx", "dp"),
        P("gy", "gx", "dp"),
        P("gy", "gx"),
        P("gy", "gx"),
        P("gy", "dp", None, "gx"),
        P(None, "gx"),
        P("gx", "gy", "dp"),
        P("gy", "gx"),
        P("gy", "gx"),
        P("gy", "gx"),
        P("gy", "dp", "gx"),
        P("gx"),
        P("gx", "gy", "dp"),
        P("gy", "gx"),
    )
    return jax.shard_map(local, mesh=mesh, in_specs=in_specs, out_specs=out_specs, check_vma=False)
```

```python
import functools

import jax
import jax.numpy as jnp
from jax import lax
from jax.experimental import pallas as pl
from jax.experimental.pallas import tpu as pltpu
from jax.sharding import PartitionSpec as P

HEAD_DIM = 72
HEAD_PAD = 80
EPSILON = 1e-06
MESH = pl.DeviceIdType.MESH
BF16 = jnp.bfloat16
F32 = jnp.float32
NN = (((1,), (0,)), ((), ()))
NT = (((1,), (1,)), ((), ()))
TN = (((0,), (0,)), ((), ()))
GELU_A = 0.044715
GELU_C = 0.7978845608028654


def mm(a, b, dims):
    return lax.dot_general(a, b, dims, preferred_element_type=F32)


def round_up(value, unit):
    return (value + unit - 1) // unit * unit


def block_kernel(
    cfg,
    len_ref,
    prm_ref,
    x_ref,
    cot_ref,
    wq_in,
    wo_in,
    wu_in,
    wd_in,
    qb_ref,
    ub_ref,
    out_ref,
    ig_ref,
    dq_out,
    do_out,
    du_out,
    dd_out,
    sm_out,
    prm_all,
    prm_col,
    x_t,
    cot_t,
    h1_t,
    h2_t,
    gb_t,
    wq,
    wo,
    wu,
    wd,
    qkv_t,
    att_t,
    gatt_t,
    act_t,
    gpre_t,
    resid,
    tsend,
    trecv,
    mrecv,
    grecv,
    dk_acc,
    dv_acc,
    fa,
    fb,
    pk,
    rows_f,
    sums_col,
    uv_send,
    uv_recv,
    sm_send,
    sm_recv,
    smz_recv,
    cq,
    co,
    cu,
    cd,
    zq,
    zo,
    zu,
    zd,
    sem_s,
    sem_r,
):
    nz, zin = cfg["nz"], cfg["zin"]
    fb_rows, tok, heads = cfg["fb"], cfg["tok"], cfg["heads"]
    half, width = 4 * fb_rows, 8 * fb_rows
    tb = tok // 4
    hp = heads * HEAD_PAD
    factor = HEAD_DIM ** (-0.5)
    z, g, c = lax.axis_index("dp"), lax.axis_index("gx"), lax.axis_index("gy")
    g_hi, g_lo = g // 2, g % 2

    def gx_of(dd):
        return ((g_hi + dd // 2) % 2) * 2 + (g_lo + dd % 2) % 2

    def row_of(dc):
        return (c + dc) % 2

    counter = [0]

    def take(count):
        first = counter[0]
        counter[0] += count
        return first

    def rcopy(src, dst, sem, dev):
        return pltpu.make_async_remote_copy(
            src_ref=src,
            dst_ref=dst,
            send_sem=sem_s.at[sem],
            recv_sem=sem_r.at[sem],
            device_id=dev,
            device_id_type=MESH,
        )

    def lcopy(src, dst, sem):
        return pltpu.make_async_copy(src, dst, sem_r.at[sem])

    others = [(dd, dc) for dd in (1, 2, 3, 0) for dc in (0, 1) if dd or dc]
    near = [(dd, dc) for dd, dc in others if dd < 3]

    def dev(dd, dc):
        return (z, gx_of(dd), row_of(dc))

    def feat(dd, dc):
        return pl.ds(pl.multiple_of(row_of(dc) * half + gx_of(dd) * fb_rows, 16), fb_rows)

    def toks(j):
        return pl.ds(pl.multiple_of(j * tb, 128), tb)

    def row_tok(dc):
        return pl.ds(pl.multiple_of(row_of(dc) * tok, 128), tok)

    pending = []

    barrier = pltpu.get_barrier_semaphore()
    for dd, dc in others:
        pl.semaphore_signal(barrier, inc=1, device_id=dev(dd, dc), device_id_type=MESH)
    for k in range(1, nz):
        pl.semaphore_signal(barrier, inc=1, device_id=((z + k) % nz, g, c), device_id_type=MESH)
    pl.semaphore_wait(barrier, 7 + nz - 1)

    own_feat = feat(0, 0)
    own_t = toks(g)
    partner = (z, g, 1 - c)
    me = c * 4 + g
    th = tok // 2

    def exchange(first, src, dst):
        for dd, dc in others:
            rcopy(src, dst, first + dd * 2 + dc, dev(dd, dc)).start()
            pending.append(lambda dd=dd, dc=dc: rcopy(src, dst, first + dd * 2 + dc, dev(dd, dc)).wait_send())

    def gather_start(first, src, dst):
        for dd, dc in near:
            rcopy(src.at[:, row_tok(dc)], dst.at[own_feat, :], first + dd * 2 + dc, dev(dd, dc)).start()
            pending.append(
                lambda dd=dd, dc=dc: rcopy(
                    src.at[:, row_tok(dc)], dst.at[own_feat, :], first + dd * 2 + dc, dev(dd, dc)
                ).wait_send()
            )
        lcopy(src.at[:, row_tok(0)], dst.at[own_feat, :], first).start()

    def relay_ref(dst, dd, dc):
        return dst.at[feat(dd, dc), (dd - 1) * th : dd * th]

    def gather_relay(first, src, dst):
        for dd in (1, 2):
            for dc in (0, 1):
                rcopy(src.at[:, row_tok(0)], dst.at[feat(dd, dc), :], first + dd * 2 + dc, partner).wait_recv()
                part = relay_ref(dst, dd, dc)
                rcopy(part, part, first + 6 + dd * 2 + dc, dev(3 - dd, 0)).start()

    def gather_done(first, src, dst):
        lcopy(src.at[:, row_tok(0)], dst.at[own_feat, :], first).wait()
        rcopy(src.at[:, row_tok(0)], dst.at[feat(0, 1), :], first + 1, partner).wait_recv()
        for dd in (1, 2):
            for dc in (0, 1):
                part = dst.at[feat(3, dc), (dd - 1) * th : dd * th]
                rcopy(part, part, first + 6 + dd * 2 + dc, partner).wait_recv()

    def gather_sent(first, dst):
        for dd in (1, 2):
            for dc in (0, 1):
                part = relay_ref(dst, dd, dc)
                rcopy(part, part, first + 6 + dd * 2 + dc, partner).wait_send()

    weights = ((wq_in, wq), (wo_in, wo), (wu_in, wu), (wd_in, wd))
    steps = nz - 1
    nw = nz if zin else 1
    wz0 = take(4 * 2 * nw)
    wc0 = take(4 * 2 * nw)

    def zrows(zz, core):
        return pl.ds(pl.multiple_of(core * half + zz * fb_rows, 16), fb_rows)

    def w_rows(i, zz, core):
        return weights[i][1].at[zrows(zz, core), :]

    def hop(i, s, d):
        origin = z - (s - 1) if d == 0 else z + (s - 1)
        here = jnp.logical_and(z >= s - 1, z < nz - 1) if d == 0 else jnp.logical_and(z < nz - s + 1, z > 0)
        to = z + 1 if d == 0 else z - 1
        src = weights[i][0] if s == 1 else w_rows(i, origin, c)
        return here, lambda: rcopy(src, w_rows(i, origin, c), wz0 + i * 2 * nw + s * 2 + d, (to, g, c))

    def arrival(s, d):
        return (z >= s, z - s) if d == 0 else (z < nz - s, z + s)

    def z_send(i, s):
        if not zin:
            if s == 1:
                lcopy(weights[i][0], weights[i][1], wz0 + i * 2 * nw).start()
            return
        for d in (0, 1):
            here, make = hop(i, s, d)
            pl.when(here)(lambda make=make: make().start())
        if s == 1:
            lcopy(weights[i][0], w_rows(i, z, c), wz0 + i * 2 * nw).start()
            rcopy(weights[i][0], w_rows(i, z, c), wc0 + i * 2 * nw, partner).start()

    def z_recv(i, s):
        if not zin:
            return
        for d in (0, 1):
            here, origin = arrival(s, d)

            @pl.when(here)
            def _(s=s, d=d, origin=origin):
                rows = w_rows(i, origin, c)
                rcopy(rows, rows, wz0 + i * 2 * nw + s * 2 + d, partner).wait_recv()
                rcopy(rows, rows, wc0 + i * 2 * nw + s * 2 + d, partner).start()

        if s < steps:
            z_send(i, s + 1)

    def weight_ready(i):
        if not zin:
            lcopy(weights[i][0], weights[i][1], wz0 + i * 2 * nw).wait()
            return
        lcopy(weights[i][0], w_rows(i, z, c), wz0 + i * 2 * nw).wait()
        rcopy(weights[i][0], w_rows(i, z, 1 - c), wc0 + i * 2 * nw, partner).wait_recv()
        for s in range(1, nz):
            for d in (0, 1):
                here, origin = arrival(s, d)

                @pl.when(here)
                def _(s=s, d=d, origin=origin):
                    rows = w_rows(i, origin, 1 - c)
                    rcopy(rows, rows, wc0 + i * 2 * nw + s * 2 + d, partner).wait_recv()

    def weight_passed(i):
        if not zin:
            return
        rcopy(weights[i][0], w_rows(i, z, c), wc0 + i * 2 * nw, partner).wait_send()
        for s in range(1, nz):
            for d in (0, 1):
                here, make = hop(i, s, d)
                pl.when(here)(lambda make=make: make().wait_send())
                here, origin = arrival(s, d)

                @pl.when(here)
                def _(s=s, d=d, origin=origin):
                    rows = w_rows(i, origin, c)
                    rcopy(rows, rows, wc0 + i * 2 * nw + s * 2 + d, partner).wait_send()

    p0 = take(8)
    xs0 = take(12)
    cs0 = take(12)
    exchange(p0, prm_ref, prm_all.at[me])
    lcopy(prm_ref, prm_all.at[me], p0).start()
    gather_start(xs0, x_ref, x_t)
    z_send(0, 1)

    ends = []
    total = len_ref[0, 0]
    ends.append(total)
    for s in range(1, len_ref.shape[1]):
        total = total + len_ref[0, s]
        ends.append(total)

    def pictures(pos):
        picture = jnp.zeros_like(pos)
        for end in ends:
            picture = picture + jnp.where(pos >= end, 1, 0)
        return picture

    pos_col = lax.broadcasted_iota(jnp.int32, (tok, 128), 0)
    pk[...] = jnp.where(pos_col < total, pictures(pos_col), -1)
    pos_row = lax.broadcasted_iota(jnp.int32, (8, tok), 1)
    pic_row = pictures(pos_row)
    rows_f[0, :, :] = pic_row.astype(F32)
    rows_f[1, :, :] = jnp.where(pos_row < total, 1.0, 0.0)
    sums_col[...] = jnp.zeros_like(sums_col)
    att_t[...] = jnp.zeros_like(att_t)

    lcopy(prm_ref, prm_all.at[me], p0).wait()
    for dd, dc in others:
        rcopy(prm_ref, prm_all.at[row_of(dc) * 4 + gx_of(dd)], p0 + dd * 2 + dc, partner).wait_recv()
    for b in range(8):
        rows = jnp.concatenate([prm_all[b], jnp.zeros((120, 256), F32)], axis=0)
        prm_col[b * fb_rows : (b + 1) * fb_rows, :] = jnp.transpose(rows)[:fb_rows, :]

    def par(k):
        return prm_col[:, k : k + 1]

    z_recv(0, 1)
    z_send(1, 1)
    gather_relay(xs0, x_ref, x_t)
    gather_start(cs0, cot_ref, cot_t)
    if steps > 1:
        z_recv(0, 2)
    z_recv(1, 1)
    z_send(2, 1)
    gather_done(xs0, x_ref, x_t)

    def ln1(j, carry):
        t = toks(j)
        x = x_t[:, t].astype(F32)
        m = jnp.sum(x, axis=0, keepdims=True) * (1.0 / width)
        q = jnp.sum(x * x, axis=0, keepdims=True) * (1.0 / width)
        r = lax.rsqrt(q - m * m + EPSILON)
        rows_f[2, 0:1, t] = m
        rows_f[3, 0:1, t] = r
        h1_t[:, t] = ((x - m) * r * par(0) + par(1)).astype(BF16)
        return carry

    lax.fori_loop(0, 4, ln1, 0)

    for s in range(3, nz):
        z_recv(0, s)
    if steps > 1:
        z_recv(1, 2)
    weight_ready(0)

    def project(j, carry):
        t = toks(j)
        qkv_t[:, t] = (mm(wq[...], h1_t[:, t], TN) + qb_ref[...]).astype(BF16)
        return carry

    lax.fori_loop(0, 4, project, 0)
    z_recv(2, 1)
    for s in range(3, nz):
        z_recv(1, s)

    def head_rows(part, h):
        return pl.ds(pl.multiple_of((part * heads + h) * HEAD_PAD, 16), HEAD_PAD)

    def kept_of(h, t):
        scores = mm(qkv_t[head_rows(1, h), :], qkv_t[head_rows(0, h), t], TN) * factor
        key_pic = pk[...]
        query_pic = rows_f[0, 0:1, t].astype(jnp.int32)
        allowed = jnp.concatenate([key_pic] * (tb // 128), axis=1) == query_pic
        return jnp.where(allowed, jnp.exp(scores), 0.0)

    br0 = take(4)

    def attend(i, carry):
        dd = 3 - i
        j = gx_of(dd)
        t = toks(j)

        def head(h, inner):
            kept = kept_of(h, t)
            den = jnp.sum(kept, axis=0, keepdims=True)
            den = jnp.where(rows_f[1, 0:1, t] > 0.5, den, 1.0)
            scale = jnp.where(den > 1e30, 2.0**-40, 1.0)
            inv = 1.0 / (den * scale)
            rows_f[4 + 2 * h, 0:1, t] = scale
            rows_f[5 + 2 * h, 0:1, t] = inv
            probs = (kept * scale * inv).astype(BF16)
            att = mm(qkv_t[head_rows(2, h), :], probs, NN)
            att_t[head_rows(0, h), t] = att.astype(BF16)
            return inner

        lax.fori_loop(0, heads, head, 0)

        @pl.when(i == 0)
        def _():
            weight_ready(1)

        fa[...] = mm(wo[...], att_t[:, t], NN)
        for step in (3, 2, 1):

            @pl.when(i == 3 - step)
            def _(step=step):
                gb_t[:, t] = fa[...].astype(BF16)
                rcopy(gb_t.at[:, t], trecv.at[step - 1], br0 + step, (z, gx_of(step), c)).start()

        @pl.when(i == 1)
        def _():
            if steps > 1:
                z_recv(2, 2)
            z_send(3, 1)
            gather_relay(cs0, cot_ref, cot_t)

        return carry

    lax.fori_loop(0, 4, attend, 0)

    def wait_tokens(first, step):
        rcopy(gb_t.at[:, own_t], trecv.at[step - 1], first + step, partner).wait_recv()

    def wait_tokens_sent(first):
        for step in (1, 2, 3):
            rcopy(gb_t.at[:, toks(gx_of(step))], trecv.at[step - 1], first + step, partner).wait_send()

    for s in range(3, nz):
        z_recv(2, s)
    z_recv(3, 1)

    for step in (3, 2, 1):
        wait_tokens(br0, step)
    residual = (
        x_t[:, own_t].astype(F32)
        + fa[...]
        + trecv[0].astype(F32)
        + trecv[1].astype(F32)
        + trecv[2].astype(F32)
        + par(2)
    )
    resid[...] = residual
    m2 = jnp.sum(residual, axis=0, keepdims=True) * (1.0 / width)
    q2 = jnp.sum(residual * residual, axis=0, keepdims=True) * (1.0 / width)
    r2 = lax.rsqrt(q2 - m2 * m2 + EPSILON)
    rows_f[2, 1:2, own_t] = m2
    rows_f[3, 1:2, own_t] = r2
    h2_t[:, own_t] = ((residual - m2) * r2 * par(3) + par(4)).astype(BF16)

    def spread(first, buf):
        for step in (1, 2):
            rcopy(buf.at[:, own_t], buf.at[:, own_t], first + step, (z, gx_of(step), c)).start()

    def halves(buf, step, k):
        return buf.at[(k - 1) * half : k * half, toks(gx_of(step))]

    def spread_relay(first, buf):
        for step in (1, 2):
            block = buf.at[:, toks(gx_of(step))]
            rcopy(block, block, first + step, partner).wait_recv()
            part = halves(buf, step, step)
            rcopy(part, part, first + 2 + step, (z, gx_of(3 - step), c)).start()

    def spread_done(first, buf):
        for k in (1, 2):
            part = halves(buf, 3, k)
            rcopy(part, part, first + 2 + k, partner).wait_recv()

    def spread_sent(first, buf):
        for step in (1, 2):
            rcopy(buf.at[:, own_t], buf.at[:, own_t], first + step, partner).wait_send()
            part = halves(buf, step, step)
            rcopy(part, part, first + 2 + step, partner).wait_send()

    h20 = take(5)
    spread(h20, h2_t)
    wait_tokens_sent(br0)
    weight_ready(2)
    if steps > 1:
        z_recv(3, 2)
    gather_done(cs0, cot_ref, cot_t)

    g20 = take(4)

    def mlp(i, carry):
        dd = (i + 1) % 4
        t = toks(gx_of(dd))

        @pl.when(i == 0)
        def _():
            spread_relay(h20, h2_t)
            for s in range(3, nz):
                z_recv(3, s)
            weight_ready(3)

        @pl.when(i == 2)
        def _():
            spread_done(h20, h2_t)

        fa[...] = mm(wu[...], h2_t[:, t], TN) + ub_ref[...]
        fb[...] = mm(wd[...], cot_t[:, t], TN)

        def chunk(n, inner):
            rows = pl.ds(pl.multiple_of(n * 48, 16), 48)
            v = fa[rows, :]
            v2 = v * v
            thv = jnp.tanh(GELU_C * (v + GELU_A * v2 * v))
            hf = 0.5 * (1.0 + thv)
            act_t[rows, t] = (v * hf).astype(BF16)
            slope = hf + (0.5 * GELU_C) * v * (1.0 - thv * thv) * (1.0 + (3.0 * GELU_A) * v2)
            gpre_t[rows, t] = (fb[rows, :] * slope).astype(BF16)
            return inner

        lax.fori_loop(0, fa.shape[0] // 48, chunk, 0)
        fa[...] = mm(wu[...], gpre_t[:, t], NN)
        for step in (1, 2, 3):

            @pl.when(i == step - 1)
            def _(step=step):
                tsend[step - 1] = fa[...].astype(BF16)
                rcopy(tsend.at[step - 1], trecv.at[step - 1], g20 + step, (z, gx_of(step), c)).start()

        return carry

    lax.fori_loop(0, 4, mlp, 0)

    dwc0 = take(4)
    dwz0 = take(4 * nw)
    do0 = take(16)
    core_recv = (cq, co, cu, cd)
    z_recvs = (zq, zo, zu, zd)
    dw_refs = (gpre_t, wo, wu, wd)
    dw_cols = (wq.shape[1], wo.shape[1], wu.shape[1], wd.shape[1])
    dw_outs = (dq_out, do_out, du_out, dd_out)
    slots = [0]
    leaving = []

    def weight_grad(i, left, right):
        weight_passed(i)
        dst, cols = dw_refs[i], dw_cols[i]
        step_cols = 384 if cols % 384 == 0 else 256

        def one(n, carry):
            cs = pl.ds(pl.multiple_of(n * step_cols, 128), step_cols)
            dst[:, cs] = mm(left[...], right[pl.ds(pl.multiple_of(n * step_cols, 16), step_cols), :], NT).astype(BF16)
            return carry

        lax.fori_loop(0, cols // step_cols, one, 0)

    def core_half(i, core):
        return dw_refs[i].at[pl.ds(pl.multiple_of(core * half, 16), half), :]

    def send_core(i):
        if zin:
            rcopy(core_half(i, 1 - c), core_recv[i], dwc0 + i, partner).start()
            pending.append(lambda: rcopy(core_half(i, 1 - c), core_recv[i], dwc0 + i, partner).wait_send())
        else:
            lcopy(dw_refs[i], dw_outs[i], dwc0 + i).start()

    def sum_core(i):
        if not zin:
            return
        rcopy(core_half(i, c), core_recv[i], dwc0 + i, partner).wait_recv()
        w = dw_refs[i]
        for zz in range(nz):
            rows = pl.ds(pl.multiple_of(c * half + zz * fb_rows, 16), fb_rows)
            w[rows, :] = (
                w[rows, :].astype(F32) + core_recv[i][zz * fb_rows : (zz + 1) * fb_rows, :].astype(F32)
            ).astype(BF16)
        for k in range(1, nz):

            def make(k=k):
                zz = (z + k) % nz
                return rcopy(w.at[zrows(zz, c), :], z_recvs[i].at[k - 1], dwz0 + i * nz + k, (zz, g, c))

            make().start()
            pending.append(lambda make=make: make().wait_send())

    def sum_z(i):
        if not zin:
            lcopy(dw_refs[i], dw_outs[i], dwc0 + i).wait()
            return
        for k in range(1, nz):
            rcopy(dw_refs[i].at[zrows(z, c), :], z_recvs[i].at[k - 1], dwz0 + i * nz + k, partner).wait_recv()
        cols = dw_cols[i]
        for n in range(0, cols, tb):
            size = min(tb, cols - n)
            part = dw_refs[i][zrows(z, c), n : n + size].astype(F32)
            for k in range(1, nz):
                part = part + z_recvs[i][k - 1, :, n : n + size].astype(F32)
            slot = slots[0]
            slots[0] += 1
            stage = (fa, fb)[slot // 8].at[(slot % 8) * fb_rows : (slot % 8 + 1) * fb_rows, 0:size]
            stage[...] = part
            cp = lcopy(stage, dw_outs[i].at[:, n : n + size], do0 + slot)
            cp.start()
            leaving.append(cp)

    ml0 = take(8)
    gh0 = take(4 * 8)
    uv0 = take(8)
    sm0 = take(8)
    sz0 = take(nz)

    def scatter(first, recv, start):
        for dd, dc in others:
            cp = rcopy(h2_t.at[feat(dd, dc), :], recv.at[dd * 2 + dc], first + dd * 2 + dc, dev(dd, dc))
            cp.start() if start else cp.wait_send()
        cp = lcopy(h2_t.at[own_feat, :], recv.at[0], first)
        cp.start() if start else cp.wait()

    weight_grad(2, h2_t, gpre_t)
    send_core(2)

    spread_sent(h20, h2_t)

    def lower(j, carry):
        t = toks(j)
        h2_t[:, t] = mm(wd[...], act_t[:, t], NN).astype(BF16)
        return carry

    lax.fori_loop(0, 4, lower, 0)
    h2_t[:, own_t] = (mm(wd[...], act_t[:, own_t], NN) + resid[...] + par(5)).astype(BF16)
    sum_core(2)
    ones = jnp.ones((tok, 128), BF16)
    sums_col[0 : act_t.shape[0], 6:7] = mm(gpre_t[...], ones, NN)[:, 0:1]

    for step in (1, 2, 3):
        wait_tokens(g20, step)
    gh2 = fa[...] + trecv[0].astype(F32) + trecv[1].astype(F32) + trecv[2].astype(F32)
    m2 = rows_f[2, 1:2, own_t]
    r2 = rows_f[3, 1:2, own_t]
    normed2 = (resid[...] - m2) * r2
    gn = gh2 * par(3)
    s1 = jnp.sum(gn, axis=0, keepdims=True) * (1.0 / width)
    s2 = jnp.sum(gn * normed2, axis=0, keepdims=True) * (1.0 / width)
    cot_own = cot_t[:, own_t].astype(F32)
    g_res = cot_own + r2 * (gn - s1 - normed2 * s2)
    g_low = g_res.astype(BF16)
    gb_t[:, own_t] = g_low
    gb0 = take(5)
    spread(gb0, gb_t)
    resid[...] = g_res
    sums_col[0:width, 2:3] = jnp.sum(g_low.astype(F32), axis=1, keepdims=True)
    sums_col[0:width, 3:4] = jnp.sum(gh2 * normed2, axis=1, keepdims=True)
    sums_col[0:width, 4:5] = jnp.sum(gh2, axis=1, keepdims=True)
    sums_col[0:width, 5:6] = jnp.sum(cot_own, axis=1, keepdims=True)
    for step in (1, 2, 3):
        rcopy(tsend.at[step - 1], trecv.at[step - 1], g20 + step, partner).wait_send()
    weight_grad(3, cot_t, act_t)
    send_core(3)

    dk_acc[...] = jnp.zeros_like(dk_acc)
    dv_acc[...] = jnp.zeros_like(dv_acc)

    def attend_back(i, carry):
        t = toks(gx_of(i))

        @pl.when(i == 1)
        def _():
            spread_relay(gb0, gb_t)
            scatter(ml0, mrecv, True)

        @pl.when(i == 3)
        def _():
            spread_done(gb0, gb_t)

        gatt_t[...] = mm(wo[...], gb_t[:, t], TN)[0:hp, :].astype(BF16)

        @pl.when(i == 1)
        def _():
            sum_core(3)

        @pl.when(i == 3)
        def _():
            weight_grad(1, gb_t, att_t)
            send_core(1)

        def head(h, inner):
            kept = kept_of(h, t)
            probs = kept * rows_f[4 + 2 * h, 0:1, t] * rows_f[5 + 2 * h, 0:1, t]
            q_rows = head_rows(0, h)
            grad = gatt_t[q_rows, :]
            grad_probs = mm(qkv_t[head_rows(2, h), :], grad, TN)
            weighted = probs * grad_probs
            delta = jnp.sum(weighted, axis=0, keepdims=True)
            grad_scores = (weighted - probs * delta).astype(BF16)
            act_t[q_rows, t] = (mm(qkv_t[head_rows(1, h), :], grad_scores, NN) * factor).astype(BF16)
            dk_acc[q_rows, :] += mm(qkv_t[q_rows, t], grad_scores, NT)
            dv_acc[q_rows, :] += mm(grad, probs.astype(BF16), NT)
            return inner

        lax.fori_loop(0, heads, head, 0)
        return carry

    lax.fori_loop(0, 4, attend_back, 0)
    kq = wq.shape[1]
    act_t[hp : 2 * hp, :] = (dk_acc[...] * factor).astype(BF16)
    act_t[2 * hp : 3 * hp, :] = dv_acc[...].astype(BF16)
    act_t[3 * hp : kq, :] = jnp.zeros((kq - 3 * hp, tok), BF16)
    weight_grad(0, h1_t, act_t)
    send_core(0)
    sum_core(1)
    sums_col[0:kq, 7:8] = mm(act_t[0:kq, :], ones, NN)[:, 0:1]
    sum_core(0)
    scatter(ml0, mrecv, False)

    def gh_pieces(j, start):
        t = toks(j)
        for dd, dc in others:
            slot = dd * 2 + dc
            cp = rcopy(h2_t.at[feat(dd, dc), t], grecv.at[slot, :, t], gh0 + j * 8 + slot, dev(dd, dc))
            cp.start() if start else cp.wait_send()
        cp = lcopy(h2_t.at[own_feat, t], grecv.at[0, :, t], gh0 + j * 8)
        cp.start() if start else cp.wait()

    def back1(j, carry):
        t = toks(j)
        gh1 = mm(wq[...], act_t[0:kq, t], NN)
        m = rows_f[2, 0:1, t]
        r = rows_f[3, 0:1, t]
        normed = (x_t[:, t].astype(F32) - m) * r
        gn1 = gh1 * par(0)
        prod = gh1 * normed
        sums_col[0:width, 0:1] += jnp.sum(prod, axis=1, keepdims=True)
        sums_col[0:width, 1:2] += jnp.sum(gh1, axis=1, keepdims=True)
        a1 = jnp.sum(gn1, axis=0, keepdims=True) * (1.0 / width)
        a2 = jnp.sum(gn1 * normed, axis=0, keepdims=True) * (1.0 / width)
        v = r * r * a2
        uv_send[0:1, t] = r * a1 - m * v
        uv_send[1:2, t] = v
        fa[...] = r * gn1

        @pl.when(j == g)
        def _():
            fa[...] += resid[...]

        h2_t[:, t] = fa[...].astype(BF16)

        @pl.when(j < 3)
        def _():
            gh_pieces(j, True)

        return carry

    lax.fori_loop(0, 4, back1, 0)

    for n in range(0, sm_send.shape[1], 128):
        sm_send[:, n : n + 128] = jnp.transpose(sums_col[n : n + 128, :])[0:8, :]
    exchange(sm0, sm_send, sm_recv.at[me])
    exchange(uv0, uv_send, uv_recv.at[me])
    lcopy(uv_send, uv_recv.at[me], uv0).start()
    gh_pieces(3, True)

    for dd, dc in others:
        rcopy(h2_t.at[own_feat, :], mrecv.at[dd * 2 + dc], ml0 + dd * 2 + dc, partner).wait_recv()
    for dc in (0, 1):
        acc = mrecv[dc].astype(F32)
        for dd in (1, 2, 3):
            acc = acc + mrecv[dd * 2 + dc].astype(F32)
        out_ref[:, row_tok(dc)] = acc.astype(BF16)

    sum_z(2)
    sum_z(3)

    total_sm = sm_send[...]
    row8 = lax.broadcasted_iota(jnp.int32, total_sm.shape, 0)
    for dd, dc in others:
        rcopy(sm_send, sm_recv.at[row_of(dc) * 4 + gx_of(dd)], sm0 + dd * 2 + dc, partner).wait_recv()
        part = sm_recv[row_of(dc) * 4 + gx_of(dd)]
        total_sm = total_sm + (part if dd == 0 else jnp.where(row8 < 6, part, 0.0))
    smz_recv[0] = total_sm
    for k in range(1, nz):

        def make(k=k):
            return rcopy(smz_recv.at[0], smz_recv.at[k], sz0 + k, ((z + k) % nz, g, c))

        make().start()
        pending.append(lambda make=make: make().wait_send())

    sum_z(1)

    lcopy(uv_send, uv_recv.at[me], uv0).wait()
    for dd, dc in others:
        slot = dd * 2 + dc
        rcopy(uv_send, uv_recv.at[row_of(dc) * 4 + gx_of(dd)], uv0 + slot, partner).wait_recv()
        for j in range(4):
            t = toks(j)
            rcopy(h2_t.at[own_feat, t], grecv.at[slot, :, t], gh0 + j * 8 + slot, partner).wait_recv()
    for j in range(4):
        gh_pieces(j, False)
    for dc in (0, 1):
        acc = grecv[dc].astype(F32)
        uv = uv_recv[row_of(dc) * 4 + g]
        for dd in (1, 2, 3):
            acc = acc + grecv[dd * 2 + dc].astype(F32)
            uv = uv + uv_recv[row_of(dc) * 4 + gx_of(dd)]
        x_own = x_ref[:, row_tok(dc)].astype(F32)
        ig_ref[:, row_tok(dc)] = acc - uv[0:1, :] - x_own * uv[1:2, :]

    sum_z(0)
    total_z = smz_recv[0]
    for k in range(1, nz):
        rcopy(smz_recv.at[0], smz_recv.at[k], sz0 + k, partner).wait_recv()
        total_z = total_z + smz_recv[k]
    sm_out[...] = total_z

    for cp in leaving:
        cp.wait()
    for wait in pending:
        wait()
    gather_sent(xs0, x_t)
    gather_sent(cs0, cot_t)
    spread_sent(gb0, gb_t)


def local(
    block_input,
    lengths,
    ln1_gain,
    ln1_bias,
    w_qkv,
    qv_bias,
    w_out,
    out_bias,
    ln2_gain,
    ln2_bias,
    w_up,
    up_bias,
    w_down,
    down_bias,
    cotangent,
):
    nz = lax.axis_size("dp")
    fb_rows, tok2 = block_input.shape[1], block_input.shape[2]
    tok = tok2 // 2
    width = 8 * fb_rows
    heads = w_qkv.shape[3] // HEAD_DIM
    hp = heads * HEAD_PAD
    kq, ko = round_up(3 * hp, 128), round_up(hp, 128)
    hid = w_up.shape[2]
    kh = round_up(hid, 384)
    zrow = w_qkv.shape[1]
    zin = zrow == fb_rows and nz == 4

    def pad_heads(a):
        parts = a.shape[-1] // HEAD_DIM
        a = a.reshape(a.shape[:-1] + (parts, HEAD_DIM))
        a = jnp.pad(a, [(0, 0)] * (a.ndim - 1) + [(0, HEAD_PAD - HEAD_DIM)])
        return a.reshape(a.shape[:-2] + (parts * HEAD_PAD,))

    def widen(a, cols):
        return jnp.pad(a, ((0, 0), (0, cols - a.shape[1])))

    prm = jnp.concatenate([ln1_gain, ln1_bias, out_bias, ln2_gain, ln2_bias, down_bias], axis=0)
    prm = jnp.pad(prm, ((0, 2), (0, 256 - fb_rows)))
    wq = widen(pad_heads(w_qkv[0].reshape(zrow, -1)), kq)
    wo = widen(pad_heads(jnp.transpose(w_out[:, 0, :])), ko)
    wu = widen(w_up[0], kh)
    wd = widen(jnp.transpose(w_down[:, 0, :]), kh)
    qb = jnp.concatenate([qv_bias[0:1], jnp.zeros_like(qv_bias[0:1]), qv_bias[1:2]], axis=1)
    qb = widen(pad_heads(qb), kq).reshape(kq, 1)
    ub = jnp.pad(up_bias, (0, kh - hid)).reshape(kh, 1)
    if not zin:
        wq, wo, wu, wd = (
            lax.all_gather(lax.all_gather(w, "dp", axis=0, tiled=True), "gy", axis=0, tiled=True)
            for w in (wq, wo, wu, wd)
        )

    cfg = dict(nz=nz, zin=zin, fb=fb_rows, tok=tok, heads=heads)
    tb = tok // 4
    half = width // 2
    vm = pltpu.VMEM
    n_sems = 130 + nz + (20 * nz if zin else 20)
    dw_specs = [pl.BlockSpec(memory_space=pl.ANY)] * 4
    if zin:
        dw_shapes = tuple(jax.ShapeDtypeStruct((fb_rows, k), F32) for k in (kq, ko, kh, kh))
        core_shapes = [vm((half, k), BF16) for k in (kq, ko, kh, kh)]
        z_shapes = [vm((nz - 1, fb_rows, k), BF16) for k in (kq, ko, kh, kh)]
    else:
        dw_shapes = tuple(jax.ShapeDtypeStruct((width, k), BF16) for k in (kq, ko, kh, kh))
        core_shapes = [vm((16, 128), BF16)] * 4
        z_shapes = [vm((16, 128), BF16)] * 4
    scratch = [
        vm((8, 8, 256), F32),
        vm((width, 128), F32),
        vm((width, tok), BF16),
        vm((width, tok), BF16),
        vm((width, tok), BF16),
        vm((width, tok), BF16),
        vm((width, tok), BF16),
        vm((width, kq), BF16),
        vm((width, ko), BF16),
        vm((width, kh), BF16),
        vm((width, kh), BF16),
        vm((kq, tok), BF16),
        vm((ko, tok), BF16),
        vm((hp, tb), BF16),
        vm((kh, tok), BF16),
        vm((kh, tok), BF16),
        vm((width, tb), F32),
        vm((3, width, tb), BF16),
        vm((3, width, tb), BF16),
        vm((8, fb_rows, tok), BF16),
        vm((8, fb_rows, tok), BF16),
        vm((hp, tok), F32),
        vm((hp, tok), F32),
        vm((max(width, kh), tb), F32),
        vm((max(width, kh), tb), F32),
        vm((tok, 128), jnp.int32),
        vm((4 + 2 * heads, 8, tok), F32),
        vm((max(width, kh), 128), F32),
        vm((8, tok), F32),
        vm((8, 8, tok), F32),
        vm((8, max(width, kh)), F32),
        vm((8, 8, max(width, kh)), F32),
        vm((nz, 8, max(width, kh)), F32),
        *core_shapes,
        *z_shapes,
        pltpu.SemaphoreType.DMA((n_sems,)),
        pltpu.SemaphoreType.DMA((n_sems,)),
    ]
    any_spec = pl.BlockSpec(memory_space=pl.ANY)
    vmem_spec = pl.BlockSpec(memory_space=pltpu.VMEM)
    out, ig, dq, do, du, dd, sm = pl.pallas_call(
        functools.partial(block_kernel, cfg),
        out_shape=(
            jax.ShapeDtypeStruct((fb_rows, tok2), BF16),
            jax.ShapeDtypeStruct((fb_rows, tok2), F32),
            *dw_shapes,
            jax.ShapeDtypeStruct((8, max(width, kh)), F32),
        ),
        in_specs=[
            pl.BlockSpec(memory_space=pltpu.SMEM),
            vmem_spec,
            vmem_spec,
            any_spec,
            any_spec,
            any_spec,
            any_spec,
            any_spec,
            vmem_spec,
            vmem_spec,
        ],
        out_specs=(vmem_spec, vmem_spec, *dw_specs, vmem_spec),
        scratch_shapes=scratch,
        compiler_params=pltpu.CompilerParams(
            collective_id=0, has_side_effects=True, vmem_limit_bytes=67043328
        ),
        name="encoder_block",
    )(lengths, prm, block_input[0], cotangent[0], wq, wo, wu, wd, qb, ub)

    if not zin:

        def reduce(a):
            a = lax.psum_scatter(a, "gy", scatter_dimension=0, tiled=True)
            return lax.optimization_barrier(lax.psum_scatter(a, "dp", scatter_dimension=0, tiled=True)).astype(F32)

        dq, do, du, dd = reduce(dq), reduce(do), reduce(du), reduce(dd)

    def cut_heads(a):
        parts = a.shape[-1] // HEAD_PAD
        a = a.reshape(a.shape[:-1] + (parts, HEAD_PAD))[..., :HEAD_DIM]
        return a.reshape(a.shape[:-2] + (parts * HEAD_DIM,))

    mine = lax.axis_index("gy") * (width // 2) + lax.axis_index("gx") * fb_rows
    feats = lax.dynamic_slice(sm, (0, mine), (6, fb_rows))
    qkv_sum = cut_heads(sm[7:8, : 3 * hp]).reshape(3, -1)
    return (
        out[None],
        ig[None],
        feats[0:1],
        feats[1:2],
        cut_heads(dq[:, : 3 * hp]).reshape(1, zrow, 3, -1),
        jnp.stack([qkv_sum[0], qkv_sum[2]]),
        jnp.transpose(cut_heads(do[:, :hp]))[:, None, :],
        feats[2:3],
        feats[3:4],
        feats[4:5],
        du[None, :, :hid],
        sm[6, :hid],
        jnp.transpose(dd[:, :hid])[:, None, :],
        feats[5:6],
    )


def solution(mesh):
    in_specs = (
        P("gy", "gx", "dp"),
        P(("dp", "gy"), None),
        P("gy", "gx"),
        P("gy", "gx"),
        P("gy", "dp", None, "gx"),
        P(None, "gx"),
        P("gx", "gy", "dp"),
        P("gy", "gx"),
        P("gy", "gx"),
        P("gy", "gx"),
        P("gy", "dp", "gx"),
        P("gx"),
        P("gx", "gy", "dp"),
        P("gy", "gx"),
        P("gy", "gx", "dp"),
    )
    out_specs = (
        P("gy", "gx", "dp"),
        P("gy", "gx", "dp"),
        P("gy", "gx"),
        P("gy", "gx"),
        P("gy", "dp", None, "gx"),
        P(None, "gx"),
        P("gx", "gy", "dp"),
        P("gy", "gx"),
        P("gy", "gx"),
        P("gy", "gx"),
        P("gy", "dp", "gx"),
        P("gx"),
        P("gx", "gy", "dp"),
        P("gy", "gx"),
    )
    return jax.shard_map(local, mesh=mesh, in_specs=in_specs, out_specs=out_specs, check_vma=False)
```

```python
import functools

import jax
import jax.numpy as jnp
from jax import lax
from jax.experimental import pallas as pl
from jax.experimental.pallas import tpu as pltpu
from jax.sharding import PartitionSpec as P

HEAD_DIM = 72
HEAD_PAD = 80
EPSILON = 1e-06
MESH = pl.DeviceIdType.MESH
BF16 = jnp.bfloat16
F32 = jnp.float32
NN = (((1,), (0,)), ((), ()))
NT = (((1,), (1,)), ((), ()))
TN = (((0,), (0,)), ((), ()))
GELU_A = 0.044715
GELU_C = 0.7978845608028654


def mm(a, b, dims):
    return lax.dot_general(a, b, dims, preferred_element_type=F32)


def round_up(value, unit):
    return (value + unit - 1) // unit * unit


def block_kernel(
    cfg,
    len_ref,
    g1_ref,
    b1_ref,
    ob_ref,
    g2_ref,
    b2_ref,
    db_ref,
    x_ref,
    cot_ref,
    wq_in,
    wo_in,
    wu_in,
    wd_in,
    qv_ref,
    up_ref,
    out_ref,
    ig_ref,
    dq_out,
    do_out,
    du_out,
    dd_out,
    sm_out,
    prm_send,
    prm_all,
    prm_col,
    x_t,
    cot_t,
    h1_t,
    h2_t,
    gb_t,
    wq,
    wo,
    wu,
    wd,
    qkv_t,
    att_t,
    wo_n,
    gatt_t,
    act_t,
    gpre_t,
    resid,
    trecv,
    mrecv,
    grecv,
    mrelay,
    grelay,
    dqf,
    fa,
    fb,
    pk,
    rows_f,
    sums_col,
    uv_send,
    uv_recv,
    sm_send,
    sm_recv,
    smz_recv,
    cq,
    co,
    cu,
    cd,
    zq,
    zo,
    zu,
    zd,
    sem_s,
    sem_r,
):
    prm_refs = (g1_ref, b1_ref, ob_ref, g2_ref, b2_ref, db_ref)
    nz, zin = cfg["nz"], cfg["zin"]
    fb_rows, tok, heads = cfg["fb"], cfg["tok"], cfg["heads"]
    half, width = 4 * fb_rows, 8 * fb_rows
    tb = tok // 4
    hd = heads * HEAD_DIM
    hw = cfg["hw"]
    factor = HEAD_DIM ** (-0.5)
    z, g, c = lax.axis_index("dp"), lax.axis_index("gx"), lax.axis_index("gy")
    g_hi, g_lo = g // 2, g % 2

    def gx_of(dd):
        return ((g_hi + dd // 2) % 2) * 2 + (g_lo + dd % 2) % 2

    def row_of(dc):
        return (c + dc) % 2

    counter = [0]

    def take(count):
        first = counter[0]
        counter[0] += count
        return first

    def rcopy(src, dst, sem, dev):
        return pltpu.make_async_remote_copy(
            src_ref=src,
            dst_ref=dst,
            send_sem=sem_s.at[sem],
            recv_sem=sem_r.at[sem],
            device_id=dev,
            device_id_type=MESH,
        )

    def lcopy(src, dst, sem):
        return pltpu.make_async_copy(src, dst, sem_r.at[sem])

    others = [(dd, dc) for dd in (1, 2, 3, 0) for dc in (0, 1) if dd or dc]
    near = [(dd, dc) for dd, dc in others if dd < 3]

    def dev(dd, dc):
        return (z, gx_of(dd), row_of(dc))

    def feat(dd, dc):
        return pl.ds(pl.multiple_of(row_of(dc) * half + gx_of(dd) * fb_rows, 16), fb_rows)

    def toks(j):
        return pl.ds(pl.multiple_of(j * tb, 128), tb)

    def row_tok(dc):
        return pl.ds(pl.multiple_of(row_of(dc) * tok, 128), tok)

    pending = []

    barrier = pltpu.get_barrier_semaphore()
    for dd, dc in others:
        pl.semaphore_signal(barrier, inc=1, device_id=dev(dd, dc), device_id_type=MESH)
    for k in range(1, nz):
        pl.semaphore_signal(barrier, inc=1, device_id=((z + k) % nz, g, c), device_id_type=MESH)
    ends = []
    total = len_ref[0, 0]
    ends.append(total)
    for s in range(1, len_ref.shape[1]):
        total = total + len_ref[0, s]
        ends.append(total)

    def pictures(pos):
        picture = jnp.zeros_like(pos)
        for end in ends:
            picture = picture + jnp.where(pos >= end, 1, 0)
        return picture

    pos_col = lax.broadcasted_iota(jnp.int32, (tok, 128), 0)
    pk[...] = jnp.where(pos_col < total, pictures(pos_col), -1)
    pos_row = lax.broadcasted_iota(jnp.int32, (8, tok), 1)
    pic_row = pictures(pos_row)
    rows_f[0, :, :] = pic_row.astype(F32)
    rows_f[1, :, :] = jnp.where(pos_row < total, 1.0, 0.0)
    sums_col[...] = jnp.zeros_like(sums_col)
    qkv_t[...] = jnp.zeros_like(qkv_t)
    gatt_t[...] = jnp.zeros_like(gatt_t)

    prm_send[...] = jnp.zeros_like(prm_send)
    for k, ref in enumerate(prm_refs):
        prm_send[k : k + 1, 0:fb_rows] = ref[...]
    sm_send[...] = jnp.zeros_like(sm_send)
    sm_send[0:1, 0 : up_ref.shape[1]] = up_ref[...]
    sm_send[1:2, 0:hd] = qv_ref[0:1, :]
    sm_send[1:2, 2 * hw : 2 * hw + hd] = qv_ref[1:2, :]
    for n in range(0, sm_send.shape[1], 128):
        rows = jnp.concatenate([sm_send[:, n : n + 128], jnp.zeros((120, 128), F32)], axis=0)
        prm_col[n : n + 128, 8:16] = jnp.transpose(rows)[:, 0:8]
    pl.semaphore_wait(barrier, 7 + nz - 1)

    own_feat = feat(0, 0)
    own_t = toks(g)
    partner = (z, g, 1 - c)
    me = c * 4 + g
    th = tok // 2

    def exchange(first, src, dst):
        for dd, dc in others:
            rcopy(src, dst, first + dd * 2 + dc, dev(dd, dc)).start()
            pending.append(lambda dd=dd, dc=dc: rcopy(src, dst, first + dd * 2 + dc, dev(dd, dc)).wait_send())

    def gather_start(first, src, dst):
        for dd, dc in near:
            rcopy(src.at[:, row_tok(dc)], dst.at[own_feat, :], first + dd * 2 + dc, dev(dd, dc)).start()
            pending.append(
                lambda dd=dd, dc=dc: rcopy(
                    src.at[:, row_tok(dc)], dst.at[own_feat, :], first + dd * 2 + dc, dev(dd, dc)
                ).wait_send()
            )
        lcopy(src.at[:, row_tok(0)], dst.at[own_feat, :], first).start()

    def relay_ref(dst, dd, dc):
        return dst.at[feat(dd, dc), (dd - 1) * th : dd * th]

    def gather_relay(first, src, dst):
        for dd in (1, 2):
            for dc in (0, 1):
                rcopy(src.at[:, row_tok(0)], dst.at[feat(dd, dc), :], first + dd * 2 + dc, partner).wait_recv()
                part = relay_ref(dst, dd, dc)
                rcopy(part, part, first + 6 + dd * 2 + dc, dev(3 - dd, 0)).start()

    def gather_done(first, src, dst):
        lcopy(src.at[:, row_tok(0)], dst.at[own_feat, :], first).wait()
        rcopy(src.at[:, row_tok(0)], dst.at[feat(0, 1), :], first + 1, partner).wait_recv()
        for dd in (1, 2):
            for dc in (0, 1):
                part = dst.at[feat(3, dc), (dd - 1) * th : dd * th]
                rcopy(part, part, first + 6 + dd * 2 + dc, partner).wait_recv()

    def gather_sent(first, dst):
        for dd in (1, 2):
            for dc in (0, 1):
                part = relay_ref(dst, dd, dc)
                rcopy(part, part, first + 6 + dd * 2 + dc, partner).wait_send()

    weights = tuple((wq_in.at[p], wq.at[:, p * hw : (p + 1) * hw]) for p in range(3))
    weights += ((wo_in, wo), (wu_in, wu), (wd_in, wd))
    n_w = len(weights)
    all_s = range(1, nz)
    steps = nz - 1
    nw = nz if zin else 1
    wz0 = take(n_w * 2 * nw)
    wc0 = take(n_w * 2 * nw)

    def zrows(zz, core):
        return pl.ds(pl.multiple_of(core * half + zz * fb_rows, 16), fb_rows)

    def w_rows(i, zz, core):
        return weights[i][1].at[zrows(zz, core), :]

    def hop(i, s, d):
        origin = z - (s - 1) if d == 0 else z + (s - 1)
        here = jnp.logical_and(z >= s - 1, z < nz - 1) if d == 0 else jnp.logical_and(z < nz - s + 1, z > 0)
        to = z + 1 if d == 0 else z - 1
        src = weights[i][0] if s == 1 else w_rows(i, origin, c)
        return here, lambda: rcopy(src, w_rows(i, origin, c), wz0 + i * 2 * nw + s * 2 + d, (to, g, c))

    def arrival(s, d):
        return (z >= s, z - s) if d == 0 else (z < nz - s, z + s)

    def z_send(i, s):
        if not zin:
            if s == 1:
                lcopy(weights[i][0], weights[i][1], wz0 + i * 2 * nw).start()
            return
        for d in (0, 1):
            here, make = hop(i, s, d)
            pl.when(here)(lambda make=make: make().start())
        if s == 1:
            lcopy(weights[i][0], w_rows(i, z, c), wz0 + i * 2 * nw).start()
            rcopy(weights[i][0], w_rows(i, z, c), wc0 + i * 2 * nw, partner).start()

    def z_recv(i, s):
        if not zin:
            return
        for d in (0, 1):
            here, origin = arrival(s, d)

            @pl.when(here)
            def _(s=s, d=d, origin=origin):
                rows = w_rows(i, origin, c)
                rcopy(rows, rows, wz0 + i * 2 * nw + s * 2 + d, partner).wait_recv()
                rcopy(rows, rows, wc0 + i * 2 * nw + s * 2 + d, partner).start()

        if s < steps:
            z_send(i, s + 1)

    def weight_ready(i):
        if not zin:
            lcopy(weights[i][0], weights[i][1], wz0 + i * 2 * nw).wait()
            return
        lcopy(weights[i][0], w_rows(i, z, c), wz0 + i * 2 * nw).wait()
        rcopy(weights[i][0], w_rows(i, z, 1 - c), wc0 + i * 2 * nw, partner).wait_recv()
        for s in range(1, nz):
            for d in (0, 1):
                here, origin = arrival(s, d)

                @pl.when(here)
                def _(s=s, d=d, origin=origin):
                    rows = w_rows(i, origin, 1 - c)
                    rcopy(rows, rows, wc0 + i * 2 * nw + s * 2 + d, partner).wait_recv()

    def weight_passed(i):
        if not zin:
            return
        rcopy(weights[i][0], w_rows(i, z, c), wc0 + i * 2 * nw, partner).wait_send()
        for s in range(1, nz):
            for d in (0, 1):
                here, make = hop(i, s, d)
                pl.when(here)(lambda make=make: make().wait_send())
                here, origin = arrival(s, d)

                @pl.when(here)
                def _(s=s, d=d, origin=origin):
                    rows = w_rows(i, origin, c)
                    rcopy(rows, rows, wc0 + i * 2 * nw + s * 2 + d, partner).wait_send()

    p0 = take(8)
    xs0 = take(12)
    cs0 = take(12)
    exchange(p0, prm_send, prm_all.at[me])
    lcopy(prm_send, prm_all.at[me], p0).start()
    gather_start(xs0, x_ref, x_t)
    for i in range(3):
        z_send(i, 1)

    lcopy(prm_send, prm_all.at[me], p0).wait()
    for dd, dc in others:
        rcopy(prm_send, prm_all.at[row_of(dc) * 4 + gx_of(dd)], p0 + dd * 2 + dc, partner).wait_recv()
    for b in range(8):
        rows = jnp.concatenate([prm_all[b], jnp.zeros((120, 256), F32)], axis=0)
        prm_col[b * fb_rows : (b + 1) * fb_rows, 0:8] = jnp.transpose(rows)[:fb_rows, 0:8]

    def par(k):
        return prm_col[:, k : k + 1]

    def z_recv_all(pairs):
        for i, step in pairs:
            if step < nz:
                z_recv(i, step)

    z_recv_all(((0, 1), (1, 1), (0, 2), (2, 1), (1, 2), (0, 3)))
    gather_relay(xs0, x_ref, x_t)
    gather_start(cs0, cot_ref, cot_t)
    z_recv_all(((2, 2), (1, 3)))
    z_send(3, 1)
    z_recv_all(((2, 3),))
    for i in range(3):
        z_recv_all((i, step) for step in range(4, nz))
    gather_done(xs0, x_ref, x_t)

    def ln1(j, carry):
        t = toks(j)
        x = x_t[:, t].astype(F32)
        m = jnp.sum(x, axis=0, keepdims=True) * (1.0 / width)
        q = jnp.sum(x * x, axis=0, keepdims=True) * (1.0 / width)
        r = lax.rsqrt(q - m * m + EPSILON)
        rows_f[2, 0:1, t] = m
        rows_f[3, 0:1, t] = r
        h1_t[:, t] = ((x - m) * r * par(0) + par(1)).astype(BF16)
        return carry

    lax.fori_loop(0, 4, ln1, 0)

    z_recv_all(((3, 1),))
    z_send(4, 1)
    for i in range(3):
        weight_ready(i)

    def head_rows(part, h):
        return pl.ds(pl.multiple_of((part * heads + h) * HEAD_PAD, 16), HEAD_PAD)

    def project(j, carry):
        t = toks(j)
        for p in range(3):
            part = mm(wq[:, p * hw : (p + 1) * hw], h1_t[:, t], TN)
            if p != 1:
                part = part + prm_col[p * hw : (p + 1) * hw, 9:10]
            for h in range(heads):
                first = (p * heads + h) * HEAD_PAD
                qkv_t[first : first + HEAD_DIM, t] = part[h * HEAD_DIM : (h + 1) * HEAD_DIM, :].astype(BF16)
        return carry

    lax.fori_loop(0, 4, project, 0)
    z_recv_all(((3, 2),))

    def kept_of(h, t):
        scores = mm(qkv_t[head_rows(1, h), :], qkv_t[head_rows(0, h), t], TN) * factor
        key_pic = pk[...]
        query_pic = rows_f[0, 0:1, t].astype(jnp.int32)
        allowed = jnp.concatenate([key_pic] * (tb // 128), axis=1) == query_pic
        return jnp.where(allowed, jnp.exp(scores), 0.0)

    wn0 = take(8)

    def wo_part(gx, core, first=0, last=None):
        rows = (fb_rows if last is None else last) - first
        return wo_n.at[pl.ds(pl.multiple_of(gx * hd + core * fb_rows + first, 16), rows), :]

    cut = fb_rows // 32 * 16 + 16

    def wo_copy(n):
        if n < 2:
            own = wo_part(g, c)
            return rcopy(own, own, wn0 + n + 1, (z, gx_of(n + 1), c))
        if n < 4:
            got = wo_part(gx_of(n - 1), c)
            return rcopy(got, got, wn0 + n + 1, partner)
        if n < 6:
            on = wo_part(gx_of(1), c, 0, cut) if n == 4 else wo_part(gx_of(2), c, cut)
            return rcopy(on, on, wn0 + n + 1, (z, gx_of(6 - n), c))
        far = wo_part(gx_of(3), c)
        return rcopy(far, far, wn0 + 7, partner)

    def wo_first():
        turned = jnp.transpose(wo[...])
        wo_n[pl.ds(pl.multiple_of(g * hd, 16), hd), :] = turned[0:hd, :]
        for n in (0, 1):
            wo_copy(n).start()

    def wo_second():
        for step in (1, 2):
            got = wo_part(gx_of(step), c)
            rcopy(got, got, wn0 + step, partner).wait_recv()
        for n in (4, 5, 2, 3):
            wo_copy(n).start()

    def wo_third():
        for step, on in ((1, wo_part(gx_of(3), c, 0, cut)), (2, wo_part(gx_of(3), c, cut))):
            rcopy(on, on, wn0 + 4 + step, partner).wait_recv()
        wo_copy(6).start()

    def wo_ready():
        for step in (1, 2):
            got = wo_part(gx_of(step), 1 - c)
            rcopy(got, got, wn0 + 2 + step, partner).wait_recv()
        far = wo_part(gx_of(3), 1 - c)
        rcopy(far, far, wn0 + 7, partner).wait_recv()

    at0 = take(4 * 3)
    own_heads = pl.ds(pl.multiple_of(g * hd, 16), hd)

    def att_piece(dd, j):
        return att_t.at[pl.ds(pl.multiple_of(gx_of(dd) * hd, 16), hd), toks(j)]

    def att_send(j, start):
        for step in (1, 2):
            piece = att_piece(0, j)
            cp = rcopy(piece, piece, at0 + j * 3 + step - 1, (z, gx_of(step), c))
            cp.start() if start else cp.wait_send()

    def att_relay(j):
        for step in (1, 2):
            piece = att_piece(step, j)
            rcopy(piece, piece, at0 + j * 3 + step - 1, partner).wait_recv()
        step = 1 if j < 2 else 2
        piece = att_piece(step, j)
        rcopy(piece, piece, at0 + j * 3 + 2, (z, gx_of(3 - step), c)).start()

    def att_relayed(j):
        piece = att_piece(1 if j < 2 else 2, j)
        rcopy(piece, piece, at0 + j * 3 + 2, partner).wait_send()

    def attend(j, carry):
        t = toks(j)

        def head(h, inner):
            kept = kept_of(h, t)
            den = jnp.sum(kept, axis=0, keepdims=True)
            den = jnp.where(rows_f[1, 0:1, t] > 0.5, den, 1.0)
            scale = jnp.where(den > 1e30, 2.0**-40, 1.0)
            inv = 1.0 / (den * scale)
            rows_f[4 + 2 * h, 0:1, t] = scale
            rows_f[5 + 2 * h, 0:1, t] = inv
            probs = (kept * scale * inv).astype(BF16)
            att = mm(qkv_t[head_rows(2, h), :], probs, NN)
            dqf[pl.ds(pl.multiple_of(h * HEAD_DIM, 8), HEAD_DIM), :] = att[0:HEAD_DIM, :]
            return inner

        lax.fori_loop(0, heads, head, 0)
        att_t[own_heads, t] = dqf[...].astype(BF16)

        @pl.when(j == 0)
        def _():
            z_recv_all((3, step) for step in range(3, nz))
            weight_ready(3)
            wo_first()

        att_send(j, True)

        @pl.when(j == 0)
        def _():
            z_recv_all(((4, 1),))
            gather_relay(cs0, cot_ref, cot_t)

        @pl.when(j == 2)
        def _():
            wo_second()
            z_recv_all(((4, 2),))
            z_send(5, 1)
            att_relay(0)

        return carry

    lax.fori_loop(0, 4, attend, 0)
    att_relay(1)
    wo_third()
    z_recv_all((4, step) for step in range(3, nz))

    def project_out(j, carry):
        t = toks(j)

        @pl.when(j == 0)
        def _():
            att_relay(2)
            wo_ready()

        @pl.when(j == 1)
        def _():
            att_relay(3)
            z_recv_all(((5, 1),))

        far = att_piece(3, j)
        rcopy(far, far, at0 + j * 3 + 2, partner).wait_recv()
        residual = mm(wo_n[...], att_t[:, t], TN) + x_t[:, t].astype(F32) + par(2)
        m2 = jnp.sum(residual, axis=0, keepdims=True) * (1.0 / width)
        q2 = jnp.sum(residual * residual, axis=0, keepdims=True) * (1.0 / width)
        r2 = lax.rsqrt(q2 - m2 * m2 + EPSILON)
        rows_f[2, 1:2, t] = m2
        rows_f[3, 1:2, t] = r2
        h2_t[:, t] = ((residual - m2) * r2 * par(3) + par(4)).astype(BF16)

        @pl.when(j == g)
        def _():
            resid[...] = residual

        return carry

    lax.fori_loop(0, 4, project_out, 0)
    weight_ready(4)
    z_recv_all(((5, 2),))
    gather_done(cs0, cot_ref, cot_t)
    for n in range(7):
        wo_copy(n).wait_send()

    def spread(first, buf):
        for step in (1, 2):
            rcopy(buf.at[:, own_t], buf.at[:, own_t], first + step, (z, gx_of(step), c)).start()

    def halves(buf, step, k):
        return buf.at[(k - 1) * half : k * half, toks(gx_of(step))]

    def spread_relay(first, buf):
        for step in (1, 2):
            block = buf.at[:, toks(gx_of(step))]
            rcopy(block, block, first + step, partner).wait_recv()
            part = halves(buf, step, step)
            rcopy(part, part, first + 2 + step, (z, gx_of(3 - step), c)).start()

    def spread_done(first, buf):
        for k in (1, 2):
            part = halves(buf, 3, k)
            rcopy(part, part, first + 2 + k, partner).wait_recv()

    def spread_sent(first, buf):
        for step in (1, 2):
            rcopy(buf.at[:, own_t], buf.at[:, own_t], first + step, partner).wait_send()
            part = halves(buf, step, step)
            rcopy(part, part, first + 2 + step, partner).wait_send()

    g20 = take(4)

    def tsend(step):
        return wo_n.at[:, (step - 1) * tb : step * tb]

    def mlp(i, carry):
        t = toks(gx_of(3 - i))
        fa[...] = mm(wu[...], h2_t[:, t], TN) + prm_col[:, 8:9]

        @pl.when(i == 0)
        def _():
            z_recv_all((5, step) for step in range(3, nz))
            weight_ready(5)

        fb[...] = mm(wd[...], cot_t[:, t], TN)

        def chunk(n, inner):
            rows = pl.ds(pl.multiple_of(n * 48, 16), 48)
            v = fa[rows, :]
            v2 = v * v
            thv = jnp.tanh(GELU_C * (v + GELU_A * v2 * v))
            hf = 0.5 * (1.0 + thv)
            act_t[rows, t] = (v * hf).astype(BF16)
            slope = hf + (0.5 * GELU_C) * v * (1.0 - thv * thv) * (1.0 + (3.0 * GELU_A) * v2)
            gpre_t[rows, t] = (fb[rows, :] * slope).astype(BF16)
            return inner

        lax.fori_loop(0, fa.shape[0] // 48, chunk, 0)
        fa[...] = mm(wu[...], gpre_t[:, t], NN)
        for step in (1, 2, 3):

            @pl.when(i == 3 - step)
            def _(step=step):
                tsend(step)[...] = fa[...].astype(BF16)
                rcopy(tsend(step), trecv.at[step - 1], g20 + step, (z, gx_of(step), c)).start()

        return carry

    lax.fori_loop(0, 4, mlp, 0)

    dwc0 = take(4)
    dwz0 = take(4 * 8)
    do0 = take(16)
    gath = ((0, 1, 2), (3,), (4,), (5,))
    core_recv = (cq, co, cu, cd)
    z_recvs = (zq, zo, zu, zd)
    dw_refs = (wo_n, wo, wu, wd)
    kp = cfg["kp"]
    dw_cols = (kp, wo.shape[1], wu.shape[1], wd.shape[1])
    dw_outs = (dq_out, do_out, du_out, dd_out)
    slots = [0]
    leaving = []

    def weight_grad(i, left, right):
        for n in gath[i]:
            weight_passed(n)
        dst, cols = dw_refs[i], dw_cols[i]
        step_cols = 384

        def one(n, carry):
            cs = pl.ds(pl.multiple_of(n * step_cols, 128), step_cols)
            dst[:, cs] = mm(left[...], right[pl.ds(pl.multiple_of(n * step_cols, 16), step_cols), :], NT).astype(BF16)
            return carry

        lax.fori_loop(0, cols // step_cols, one, 0)
        rest = cols // step_cols * step_cols
        if rest < cols:
            dst[:, rest:cols] = mm(left[...], right[rest:cols, :], NT).astype(BF16)

    def core_half(i, core):
        return dw_refs[i].at[pl.ds(pl.multiple_of(core * half, 16), half), 0 : dw_cols[i]]

    def send_core(i):
        if zin:
            rcopy(core_half(i, 1 - c), core_recv[i], dwc0 + i, partner).start()
            pending.append(lambda: rcopy(core_half(i, 1 - c), core_recv[i], dwc0 + i, partner).wait_send())
        else:
            lcopy(dw_refs[i].at[:, 0 : dw_cols[i]], dw_outs[i], dwc0 + i).start()

    def sum_core(i):
        if not zin:
            return
        rcopy(core_half(i, c), core_recv[i], dwc0 + i, partner).wait_recv()
        w = dw_refs[i]
        for zz in range(nz):
            rows = pl.ds(pl.multiple_of(c * half + zz * fb_rows, 16), fb_rows)
            cols = dw_cols[i]
            w[rows, 0:cols] = (
                w[rows, 0:cols].astype(F32) + core_recv[i][zz * fb_rows : (zz + 1) * fb_rows, :].astype(F32)
            ).astype(BF16)

        @pl.when(leaf)
        def _():
            for slot, zz in enumerate((far_end, far_inner, inner)):
                z_piece(i, slot, zz, slot, inner).start()

        @pl.when(jnp.logical_not(leaf))
        def _():
            z_piece(i, 3, end, 0, end).start()

    leaf = z % 3 == 0
    low = z < 2
    end, inner = jnp.where(low, 0, 3), jnp.where(low, 1, 2)
    far_end, far_inner = 3 - end, 3 - inner

    def z_piece(i, sem, zz, slot, to):
        rows = dw_refs[i].at[zrows(zz, c), 0 : dw_cols[i]]
        return rcopy(rows, z_recvs[i].at[slot], dwz0 + i * 8 + sem, (to, g, c))

    def z_land(i, slot):
        rows = dw_refs[i].at[zrows(z, c), 0 : dw_cols[i]]
        return rcopy(rows, z_recvs[i].at[min(slot, 3) if slot != 3 else 0], dwz0 + i * 8 + slot, partner)

    def relay_z(i, slot):
        if not zin:
            return

        @pl.when(jnp.logical_not(leaf))
        def _():
            z_land(i, slot).wait_recv()
            zz = far_end if slot == 0 else far_inner
            w, cols = dw_refs[i], dw_cols[i]
            rows = zrows(zz, c)
            w[rows, 0:cols] = (w[rows, 0:cols].astype(F32) + z_recvs[i][slot].astype(F32)).astype(BF16)
            z_piece(i, 4 + slot, zz, 3, zz).start()

    def z_sent(i):
        if not zin:
            return

        @pl.when(leaf)
        def _():
            for slot, zz in enumerate((far_end, far_inner, inner)):
                z_piece(i, slot, zz, slot, inner).wait_send()

        @pl.when(jnp.logical_not(leaf))
        def _():
            z_piece(i, 3, end, 0, end).wait_send()
            z_piece(i, 4, far_end, 3, far_end).wait_send()
            z_piece(i, 5, far_inner, 3, far_inner).wait_send()

    def sum_z(i):
        if not zin:
            lcopy(dw_refs[i].at[:, 0 : dw_cols[i]], dw_outs[i], dwc0 + i).wait()
            return

        @pl.when(leaf)
        def _():
            z_land(i, 3).wait_recv()
            z_land(i, 4).wait_recv()

        @pl.when(jnp.logical_not(leaf))
        def _():
            z_land(i, 2).wait_recv()
            z_land(i, 5).wait_recv()

        near_slot = jnp.where(leaf, 0, 2)
        cols = dw_cols[i]

        def total_of(n, size):
            part = dw_refs[i][zrows(z, c), n : n + size].astype(F32)
            return part + z_recvs[i][near_slot, :, n : n + size].astype(F32) + z_recvs[i][3, :, n : n + size].astype(F32)

        if i == 0:
            whole = total_of(0, cols)
            gap = jnp.zeros((fb_rows, hw - hd), F32)
            pieces = []
            for p in range(3):
                part = jnp.concatenate([whole[:, p * hd : (p + 1) * hd], gap], axis=1)
                for n in range(0, hw, tb):
                    size = min(tb, hw - n)
                    pieces.append((part[:, n : n + size], dq_out.at[p, :, n : n + size]))
        else:
            pieces = []
            for n in range(0, cols, tb):
                size = min(tb, cols - n)
                pieces.append((total_of(n, size), dw_outs[i].at[:, n : n + size]))
        for part, goes in pieces:
            size = part.shape[1]
            slot = slots[0] % 16
            if slots[0] >= 16:
                leaving[slot].wait()
            slots[0] += 1
            stage = (fa, fb)[slot // 8].at[(slot % 8) * fb_rows : (slot % 8 + 1) * fb_rows, 0:size]
            stage[...] = part
            cp = lcopy(stage, goes, do0 + slot)
            cp.start()
            if len(leaving) > slot:
                leaving[slot] = cp
            else:
                leaving.append(cp)

    ml0 = take(16)
    gh0 = take(16)
    uv0 = take(8)
    sm0 = take(8)
    sz0 = take(nz)

    direct, added = ((1, 0), (2, 1), (0, 1)), ((1, 1), (2, 0))

    def hand(buf, relay, first, j, n):
        part = relay.at[n, :, toks(j)]
        return rcopy(buf.at[feat(3, n), toks(j)], part, first + 8 + j * 2 + n, (z, gx_of(n + 1), c))

    def block_copy(buf, recv, first, dd, dc):
        slot = dd * 2 + dc
        return rcopy(buf.at[feat(dd, dc), :], recv.at[slot], first + slot, dev(dd, dc))

    def add_relayed(buf, relay, recv, first):
        for n, (dd, dc) in ((0, (2, 0)), (1, (1, 1))):
            for j in range(4):
                hand(buf, relay, first, j, n).wait_recv()
            rows = feat(dd, dc)
            buf[rows, :] = (buf[rows, :].astype(F32) + relay[n].astype(F32)).astype(BF16)
            block_copy(buf, recv, first, dd, dc).start()

    def scatter_sent(buf, relay, recv, first):
        for dd, dc in direct + added:
            block_copy(buf, recv, first, dd, dc).wait_send()
        for n in (0, 1):
            for j in range(4):
                hand(buf, relay, first, j, n).wait_send()

    def scatter_start(buf, recv, first):
        for dd, dc in direct:
            block_copy(buf, recv, first, dd, dc).start()
        lcopy(buf.at[own_feat, :], recv.at[0], first).start()

    def scatter_sum(buf, recv, first, dc):
        if dc == 0:
            lcopy(buf.at[own_feat, :], recv.at[0], first).wait()
        acc = 0.0
        for dd in (0, 1, 2):
            if dd or dc:
                block_copy(buf, recv, first, dd, dc).wait_recv()
            acc = acc + recv[dd * 2 + dc].astype(F32)
        return acc

    weight_grad(2, h2_t, gpre_t)
    send_core(2)


    def lower(j, carry):
        t = toks(j)
        h2_t[:, t] = mm(wd[...], act_t[:, t], NN).astype(BF16)
        return carry

    lax.fori_loop(0, 4, lower, 0)
    h2_t[:, own_t] = (mm(wd[...], act_t[:, own_t], NN) + resid[...] + par(5)).astype(BF16)
    sum_core(2)
    ones = jnp.ones((tok, 128), BF16)
    sums_col[0 : act_t.shape[0], 6:7] = mm(gpre_t[...], ones, NN)[:, 0:1]

    for step in (1, 2, 3):
        rcopy(tsend(step), trecv.at[step - 1], g20 + step, partner).wait_recv()
    gh2 = fa[...] + trecv[0].astype(F32) + trecv[1].astype(F32) + trecv[2].astype(F32)
    m2 = rows_f[2, 1:2, own_t]
    r2 = rows_f[3, 1:2, own_t]
    normed2 = (resid[...] - m2) * r2
    gn = gh2 * par(3)
    s1 = jnp.sum(gn, axis=0, keepdims=True) * (1.0 / width)
    s2 = jnp.sum(gn * normed2, axis=0, keepdims=True) * (1.0 / width)
    cot_own = cot_t[:, own_t].astype(F32)
    g_res = cot_own + r2 * (gn - s1 - normed2 * s2)
    g_low = g_res.astype(BF16)
    gb_t[:, own_t] = g_low
    gb0 = take(5)
    spread(gb0, gb_t)
    resid[...] = g_res
    sums_col[0:width, 2:3] = jnp.sum(g_low.astype(F32), axis=1, keepdims=True)
    sums_col[0:width, 3:4] = jnp.sum(gh2 * normed2, axis=1, keepdims=True)
    sums_col[0:width, 4:5] = jnp.sum(gh2, axis=1, keepdims=True)
    sums_col[0:width, 5:6] = jnp.sum(cot_own, axis=1, keepdims=True)
    for step in (1, 2, 3):
        rcopy(tsend(step), trecv.at[step - 1], g20 + step, partner).wait_send()
    weight_grad(3, cot_t, act_t)
    send_core(3)
    relay_z(2, 0)

    fa[...] = jnp.zeros_like(fa)
    fb[...] = jnp.zeros_like(fb)
    for p in range(3):
        act_t[p * hw + hd : (p + 1) * hw, :] = jnp.zeros((hw - hd, tok), BF16)
    gpre_t[3 * hd : kp, :] = jnp.zeros((kp - 3 * hd, tok), BF16)

    def attend_back(i, carry):
        t = toks(gx_of(i))

        @pl.when(i == 1)
        def _():
            spread_relay(gb0, gb_t)
            for n in (0, 1):
                for k in range(4):
                    hand(h2_t, mrelay, ml0, k, n).start()
            scatter_start(h2_t, mrecv, ml0)

        @pl.when(i == 3)
        def _():
            spread_done(gb0, gb_t)

        gatt = mm(wo[...], gb_t[:, t], TN)
        for h in range(heads):
            gatt_t[h * HEAD_PAD : h * HEAD_PAD + HEAD_DIM, :] = gatt[h * HEAD_DIM : (h + 1) * HEAD_DIM, :].astype(BF16)

        @pl.when(i == 1)
        def _():
            sum_core(3)

        @pl.when(i == 2)
        def _():
            relay_z(2, 1)

        @pl.when(i == 3)
        def _():
            add_relayed(h2_t, mrelay, mrecv, ml0)
            weight_passed(3)
            wo[:, 0:hd] = mm(gb_t[...], att_t[own_heads, :], NT).astype(BF16)
            send_core(1)

        def head(h, inner):
            kept = kept_of(h, t)
            probs = kept * rows_f[4 + 2 * h, 0:1, t] * rows_f[5 + 2 * h, 0:1, t]
            q_rows = head_rows(0, h)
            grad = gatt_t[q_rows, :]
            grad_probs = mm(qkv_t[head_rows(2, h), :], grad, TN)
            weighted = probs * grad_probs
            delta = jnp.sum(weighted, axis=0, keepdims=True)
            grad_scores = (weighted - probs * delta).astype(BF16)
            dq = mm(qkv_t[head_rows(1, h), :], grad_scores, NN) * factor
            dqf[pl.ds(pl.multiple_of(h * HEAD_DIM, 8), HEAD_DIM), :] = dq[0:HEAD_DIM, :]
            dk = mm(qkv_t[q_rows, t], grad_scores, NT)
            dv = mm(grad, probs.astype(BF16), NT)
            for kb in range(4):
                rows = pl.ds(pl.multiple_of(kb * hd + h * HEAD_DIM, 8), HEAD_DIM)
                fa[rows, :] += dk[0:HEAD_DIM, kb * tb : (kb + 1) * tb]
                fb[rows, :] += dv[0:HEAD_DIM, kb * tb : (kb + 1) * tb]
            return inner

        lax.fori_loop(0, heads, head, 0)
        act_t[0:hd, t] = dqf[...].astype(BF16)
        gpre_t[0:hd, t] = dqf[...].astype(BF16)
        return carry

    lax.fori_loop(0, 4, attend_back, 0)
    kq = wq.shape[1]
    for kb in range(4):
        cols, rows = slice(kb * tb, (kb + 1) * tb), slice(kb * hd, (kb + 1) * hd)
        dk_low, dv_low = (fa[rows, :] * factor).astype(BF16), fb[rows, :].astype(BF16)
        act_t[hw : hw + hd, cols] = dk_low
        act_t[2 * hw : 2 * hw + hd, cols] = dv_low
        gpre_t[hd : 2 * hd, cols] = dk_low
        gpre_t[2 * hd : 3 * hd, cols] = dv_low
    weight_grad(0, h1_t, gpre_t)
    send_core(0)
    sum_core(1)
    relay_z(3, 0)
    sums_col[0:kq, 7:8] = mm(act_t[0:kq, :], ones, NN)[:, 0:1]
    sum_core(0)
    gather_sent(cs0, cot_t)

    def back1(j, carry):
        t = toks(j)
        gh1 = mm(wq[...], act_t[0:kq, t], NN)
        m = rows_f[2, 0:1, t]
        r = rows_f[3, 0:1, t]
        normed = (x_t[:, t].astype(F32) - m) * r
        gn1 = gh1 * par(0)
        prod = gh1 * normed
        sums_col[0:width, 0:1] += jnp.sum(prod, axis=1, keepdims=True)
        sums_col[0:width, 1:2] += jnp.sum(gh1, axis=1, keepdims=True)
        a1 = jnp.sum(gn1, axis=0, keepdims=True) * (1.0 / width)
        a2 = jnp.sum(gn1 * normed, axis=0, keepdims=True) * (1.0 / width)
        v = r * r * a2
        u = r * a1 - m * v
        for n in range(tb // 128):
            row = j * (tb // 128) + n
            uv_send[pl.ds(row, 1), :] = u[:, n * 128 : (n + 1) * 128]
            uv_send[pl.ds(tok // 128 + row, 1), :] = v[:, n * 128 : (n + 1) * 128]
        fa[...] = r * gn1

        @pl.when(j == g)
        def _():
            fa[...] += resid[...]

        cot_t[:, t] = fa[...].astype(BF16)
        for n in (0, 1):
            hand(cot_t, grelay, gh0, j, n).start()
        return carry

    lax.fori_loop(0, 4, back1, 0)

    relay_z(3, 1)
    relay_z(1, 0)
    relay_z(1, 1)

    for n in range(0, sm_send.shape[1], 128):
        sm_send[:, n : n + 128] = jnp.transpose(sums_col[n : n + 128, :])[0:8, :]
    exchange(sm0, sm_send, sm_recv.at[me])
    exchange(uv0, uv_send, uv_recv.at[me])
    lcopy(uv_send, uv_recv.at[me], uv0).start()
    scatter_start(cot_t, grecv, gh0)
    add_relayed(cot_t, grelay, grecv, gh0)
    relay_z(0, 0)

    for dc in (0, 1):
        out_ref[:, row_tok(dc)] = scatter_sum(h2_t, mrecv, ml0, dc).astype(BF16)

    sum_z(2)
    sum_z(3)

    total_sm = sm_send[...]
    row8 = lax.broadcasted_iota(jnp.int32, total_sm.shape, 0)
    for dd, dc in others:
        rcopy(sm_send, sm_recv.at[row_of(dc) * 4 + gx_of(dd)], sm0 + dd * 2 + dc, partner).wait_recv()
        part = sm_recv[row_of(dc) * 4 + gx_of(dd)]
        total_sm = total_sm + (part if dd == 0 else jnp.where(row8 < 6, part, 0.0))
    smz_recv[0] = total_sm
    for k in range(1, nz):

        def make(k=k):
            return rcopy(smz_recv.at[0], smz_recv.at[k], sz0 + k, ((z + k) % nz, g, c))

        make().start()
        pending.append(lambda make=make: make().wait_send())

    relay_z(0, 1)
    sum_z(1)

    lcopy(uv_send, uv_recv.at[me], uv0).wait()
    for dd, dc in others:
        rcopy(uv_send, uv_recv.at[row_of(dc) * 4 + gx_of(dd)], uv0 + dd * 2 + dc, partner).wait_recv()
    for dc in (0, 1):
        acc = scatter_sum(cot_t, grecv, gh0, dc)
        uv = uv_recv[row_of(dc) * 4 + g]
        for dd in (1, 2, 3):
            uv = uv + uv_recv[row_of(dc) * 4 + gx_of(dd)]
        n_rows = tok // 128
        u_row = jnp.concatenate([uv[n : n + 1, :] for n in range(n_rows)], axis=1)
        v_row = jnp.concatenate([uv[n_rows + n : n_rows + n + 1, :] for n in range(n_rows)], axis=1)
        x_own = x_ref[:, row_tok(dc)].astype(F32)
        ig_ref[:, row_tok(dc)] = acc - u_row - x_own * v_row

    sum_z(0)
    total_z = smz_recv[0]
    for k in range(1, nz):
        rcopy(smz_recv.at[0], smz_recv.at[k], sz0 + k, partner).wait_recv()
        total_z = total_z + smz_recv[k]
    sm_out[...] = total_z

    for cp in leaving:
        cp.wait()
    for wait in pending:
        wait()
    gather_sent(xs0, x_t)
    for j in range(4):
        att_send(j, False)
        att_relayed(j)
    scatter_sent(h2_t, mrelay, mrecv, ml0)
    scatter_sent(cot_t, grelay, grecv, gh0)
    for i in range(4):
        z_sent(i)
    spread_sent(gb0, gb_t)


def local(
    block_input,
    lengths,
    ln1_gain,
    ln1_bias,
    w_qkv,
    qv_bias,
    w_out,
    out_bias,
    ln2_gain,
    ln2_bias,
    w_up,
    up_bias,
    w_down,
    down_bias,
    cotangent,
):
    nz = lax.axis_size("dp")
    fb_rows, tok2 = block_input.shape[1], block_input.shape[2]
    tok = tok2 // 2
    width = 8 * fb_rows
    heads = w_qkv.shape[3] // HEAD_DIM
    hd = heads * HEAD_DIM
    hw = round_up(hd, 128)
    hp = heads * HEAD_PAD
    hid = w_up.shape[2]
    kh = round_up(hid, 384)
    kq = 3 * hw
    kp = round_up(3 * hd, 128)
    zrow = w_qkv.shape[1]
    zin = zrow == fb_rows and nz == 4

    def widen(a, cols):
        return jnp.pad(a, [(0, 0)] * (a.ndim - 1) + [(0, cols - a.shape[-1])])

    wq = widen(jnp.transpose(w_qkv[0], (1, 0, 2)), hw)
    wo = widen(jnp.transpose(w_out[:, 0, :]), hw)
    wu = widen(w_up[0], kh)
    wd = widen(jnp.transpose(w_down[:, 0, :]), kh)
    if not zin:

        def gather(w):
            axis = w.ndim - 2
            return lax.all_gather(lax.all_gather(w, "dp", axis=axis, tiled=True), "gy", axis=axis, tiled=True)

        wq, wo, wu, wd = gather(wq), gather(wo), gather(wu), gather(wd)

    cfg = dict(nz=nz, zin=zin, fb=fb_rows, tok=tok, heads=heads, hw=hw, kp=kp)
    tb = tok // 4
    half = width // 2
    vm = pltpu.VMEM
    n_sems = 160 + nz + (28 * nz if zin else 30)
    dw_specs = [pl.BlockSpec(memory_space=pl.ANY)] * 4
    if zin:
        dw_shapes = (jax.ShapeDtypeStruct((3, fb_rows, hw), F32),)
        dw_shapes += tuple(jax.ShapeDtypeStruct((fb_rows, k), F32) for k in (hw, kh, kh))
        core_shapes = [vm((half, k), BF16) for k in (kp, hw, kh, kh)]
        z_shapes = [vm((4, fb_rows, k), BF16) for k in (kp, hw, kh, kh)]
    else:
        dw_shapes = tuple(jax.ShapeDtypeStruct((width, k), BF16) for k in (kp, hw, kh, kh))
        core_shapes = [vm((16, 128), BF16)] * 4
        z_shapes = [vm((16, 128), BF16)] * 4
    scratch = [
        vm((8, 256), F32),
        vm((8, 8, 256), F32),
        vm((width, 128), F32),
        vm((width, tok), BF16),
        vm((width, tok), BF16),
        vm((width, tok), BF16),
        vm((width, tok), BF16),
        vm((width, tok), BF16),
        vm((width, kq), BF16),
        vm((width, hw), BF16),
        vm((width, kh), BF16),
        vm((width, kh), BF16),
        vm((3 * hp, tok), BF16),
        vm((4 * hd, tok), BF16),
        vm((4 * hd, width), BF16),
        vm((hp, tb), BF16),
        vm((kh, tok), BF16),
        vm((kh, tok), BF16),
        vm((width, tb), F32),
        vm((3, width, tb), BF16),
        vm((6, fb_rows, tok), BF16),
        vm((6, fb_rows, tok), BF16),
        vm((2, fb_rows, tok), BF16),
        vm((2, fb_rows, tok), BF16),
        vm((hd, tb), F32),
        vm((max(width, kh), tb), F32),
        vm((max(width, kh), tb), F32),
        vm((tok, 128), jnp.int32),
        vm((4 + 2 * heads, 8, tok), F32),
        vm((max(width, kh), 128), F32),
        vm((tok // 64, 128), F32),
        vm((8, tok // 64, 128), F32),
        vm((8, max(width, kh)), F32),
        vm((8, 8, max(width, kh)), F32),
        vm((nz, 8, max(width, kh)), F32),
        *core_shapes,
        *z_shapes,
        pltpu.SemaphoreType.DMA((n_sems,)),
        pltpu.SemaphoreType.DMA((n_sems,)),
    ]
    any_spec = pl.BlockSpec(memory_space=pl.ANY)
    vmem_spec = pl.BlockSpec(memory_space=pltpu.VMEM)
    out, ig, dq, do, du, dd, sm = pl.pallas_call(
        functools.partial(block_kernel, cfg),
        out_shape=(
            jax.ShapeDtypeStruct((fb_rows, tok2), BF16),
            jax.ShapeDtypeStruct((fb_rows, tok2), F32),
            *dw_shapes,
            jax.ShapeDtypeStruct((8, max(width, kh)), F32),
        ),
        in_specs=[pl.BlockSpec(memory_space=pltpu.SMEM)] + [vmem_spec] * 7 + [any_spec] * 5 + [vmem_spec] * 2,
        out_specs=(vmem_spec, vmem_spec, *dw_specs, vmem_spec),
        scratch_shapes=scratch,
        compiler_params=pltpu.CompilerParams(
            collective_id=0, has_side_effects=True, vmem_limit_bytes=67043328
        ),
        name="encoder_block",
    )(
        lengths,
        ln1_gain,
        ln1_bias,
        out_bias,
        ln2_gain,
        ln2_bias,
        down_bias,
        block_input[0],
        cotangent[0],
        wq,
        wo,
        wu,
        wd,
        qv_bias,
        up_bias.reshape(1, hid),
    )

    if not zin:

        def reduce(a):
            a = lax.psum_scatter(a, "gy", scatter_dimension=0, tiled=True)
            return lax.optimization_barrier(lax.psum_scatter(a, "dp", scatter_dimension=0, tiled=True)).astype(F32)

        dq, do, du, dd = reduce(dq), reduce(do), reduce(du), reduce(dd)
        dq = jnp.transpose(dq[:, : 3 * hd].reshape(zrow, 3, hd), (1, 0, 2))

    mine = lax.axis_index("gy") * (width // 2) + lax.axis_index("gx") * fb_rows
    feats = lax.dynamic_slice(sm, (0, mine), (6, fb_rows))
    return (
        out[None],
        ig[None],
        feats[0:1],
        feats[1:2],
        jnp.transpose(dq[:, :, :hd], (1, 0, 2))[None],
        jnp.concatenate([sm[7:8, :hd], sm[7:8, 2 * hw : 2 * hw + hd]], axis=0),
        jnp.transpose(do[:, :hd])[:, None, :],
        feats[2:3],
        feats[3:4],
        feats[4:5],
        du[None, :, :hid],
        sm[6, :hid],
        jnp.transpose(dd[:, :hid])[:, None, :],
        feats[5:6],
    )


def solution(mesh):
    in_specs = (
        P("gy", "gx", "dp"),
        P(("dp", "gy"), None),
        P("gy", "gx"),
        P("gy", "gx"),
        P("gy", "dp", None, "gx"),
        P(None, "gx"),
        P("gx", "gy", "dp"),
        P("gy", "gx"),
        P("gy", "gx"),
        P("gy", "gx"),
        P("gy", "dp", "gx"),
        P("gx"),
        P("gx", "gy", "dp"),
        P("gy", "gx"),
        P("gy", "gx", "dp"),
    )
    out_specs = (
        P("gy", "gx", "dp"),
        P("gy", "gx", "dp"),
        P("gy", "gx"),
        P("gy", "gx"),
        P("gy", "dp", None, "gx"),
        P(None, "gx"),
        P("gx", "gy", "dp"),
        P("gy", "gx"),
        P("gy", "gx"),
        P("gy", "gx"),
        P("gy", "dp", "gx"),
        P("gx"),
        P("gx", "gy", "dp"),
        P("gy", "gx"),
    )
    return jax.shard_map(local, mesh=mesh, in_specs=in_specs, out_specs=out_specs, check_vma=False)
```

```python
import functools

import jax
import jax.numpy as jnp
from jax import lax
from jax.experimental import pallas as pl
from jax.experimental.pallas import tpu as pltpu
from jax.sharding import PartitionSpec as P

HEAD_DIM = 72
HEAD_PAD = 80
EPSILON = 1e-06
MESH = pl.DeviceIdType.MESH
BF16 = jnp.bfloat16
F32 = jnp.float32
NN = (((1,), (0,)), ((), ()))
NT = (((1,), (1,)), ((), ()))
TN = (((0,), (0,)), ((), ()))
GELU_A = 0.044715
GELU_C = 0.7978845608028654


def mm(a, b, dims):
    return lax.dot_general(a, b, dims, preferred_element_type=F32)


def round_up(value, unit):
    return (value + unit - 1) // unit * unit


def block_kernel(
    cfg,
    len_ref,
    g1_ref,
    b1_ref,
    ob_ref,
    g2_ref,
    b2_ref,
    db_ref,
    x_ref,
    cot_ref,
    wq_in,
    wo_in,
    wu_in,
    wd_in,
    qv_ref,
    up_ref,
    out_ref,
    ig_ref,
    dq_out,
    do_out,
    du_out,
    dd_out,
    sm_out,
    prm_send,
    prm_all,
    prm_col,
    x_t,
    cot_t,
    h1_t,
    h2_t,
    gb_t,
    wq,
    wo,
    wu,
    wd,
    qkv_t,
    att_t,
    wo_n,
    gatt_t,
    act_t,
    gpre_t,
    resid,
    trecv,
    mrecv,
    grecv,
    mrelay,
    grelay,
    dqf,
    fa,
    fb,
    pk,
    rows_f,
    sums_col,
    uv_send,
    uv_recv,
    sm_send,
    sm_recv,
    smz_recv,
    cq,
    co,
    cu,
    cd,
    zq,
    zo,
    zu,
    zd,
    sem_s,
    sem_r,
):
    prm_refs = (g1_ref, b1_ref, ob_ref, g2_ref, b2_ref, db_ref)
    nz, zin = cfg["nz"], cfg["zin"]
    fb_rows, tok, heads = cfg["fb"], cfg["tok"], cfg["heads"]
    half, width = 4 * fb_rows, 8 * fb_rows
    tb = tok // 4
    hd = heads * HEAD_DIM
    hw, kp = cfg["hw"], cfg["kp"]
    factor = HEAD_DIM ** (-0.5)
    z, g, c = lax.axis_index("dp"), lax.axis_index("gx"), lax.axis_index("gy")
    g_hi, g_lo = g // 2, g % 2

    def gx_of(dd):
        return ((g_hi + dd // 2) % 2) * 2 + (g_lo + dd % 2) % 2

    def row_of(dc):
        return (c + dc) % 2

    counter = [0]

    def take(count):
        first = counter[0]
        counter[0] += count
        return first

    def rcopy(src, dst, sem, dev, send=None):
        return pltpu.make_async_remote_copy(
            src_ref=src,
            dst_ref=dst,
            send_sem=sem_s.at[sem if send is None else send],
            recv_sem=sem_r.at[sem],
            device_id=dev,
            device_id_type=MESH,
        )

    def lcopy(src, dst, sem):
        return pltpu.make_async_copy(src, dst, sem_r.at[sem])

    others = [(dd, dc) for dd in (1, 2, 3, 0) for dc in (0, 1) if dd or dc]
    near = [(dd, dc) for dd, dc in others if dd < 3]

    def dev(dd, dc):
        return (z, gx_of(dd), row_of(dc))

    def feat(dd, dc):
        return pl.ds(pl.multiple_of(row_of(dc) * half + gx_of(dd) * fb_rows, 16), fb_rows)

    def toks(j):
        return pl.ds(pl.multiple_of(j * tb, 128), tb)

    def row_tok(dc):
        return pl.ds(pl.multiple_of(row_of(dc) * tok, 128), tok)

    pending = []

    barrier = pltpu.get_barrier_semaphore()
    for dd, dc in others:
        pl.semaphore_signal(barrier, inc=1, device_id=dev(dd, dc), device_id_type=MESH)
    for k in range(1, nz):
        pl.semaphore_signal(barrier, inc=1, device_id=((z + k) % nz, g, c), device_id_type=MESH)
    ends = []
    total = len_ref[0, 0]
    ends.append(total)
    for s in range(1, len_ref.shape[1]):
        total = total + len_ref[0, s]
        ends.append(total)

    def pictures(pos):
        picture = jnp.zeros_like(pos)
        for end in ends:
            picture = picture + jnp.where(pos >= end, 1, 0)
        return picture

    pos_col = lax.broadcasted_iota(jnp.int32, (tok, 128), 0)
    pk[...] = jnp.where(pos_col < total, pictures(pos_col), -1)
    pos_row = lax.broadcasted_iota(jnp.int32, (8, tok), 1)
    pic_row = pictures(pos_row)
    rows_f[0, :, :] = pic_row.astype(F32)
    rows_f[1, :, :] = jnp.where(pos_row < total, 1.0, 0.0)
    sums_col[...] = jnp.zeros_like(sums_col)
    qkv_t[...] = jnp.zeros_like(qkv_t)
    gatt_t[...] = jnp.zeros_like(gatt_t)

    prm_send[...] = jnp.zeros_like(prm_send)
    for k, ref in enumerate(prm_refs):
        prm_send[k : k + 1, 0:fb_rows] = ref[...]
    sm_send[...] = jnp.zeros_like(sm_send)
    sm_send[0:1, 0 : up_ref.shape[0]] = up_ref[...].reshape(1, up_ref.shape[0])
    sm_send[1:2, 0:hd] = qv_ref[0:1, :]
    sm_send[1:2, 2 * hd : 3 * hd] = qv_ref[1:2, :]
    for n in range(0, sm_send.shape[1], 128):
        rows = jnp.concatenate([sm_send[:, n : n + 128], jnp.zeros((120, 128), F32)], axis=0)
        prm_col[n : n + 128, 8:16] = jnp.transpose(rows)[:, 0:8]
    if zin:
        rows = pl.ds(pl.multiple_of(c * half + z * fb_rows, 16), fb_rows)
        gap = jnp.zeros((fb_rows, kp - 3 * hd), BF16)
        wq[rows, :] = jnp.concatenate([wq_in[0], wq_in[1], wq_in[2], gap], axis=1)
        for src, dst in ((wo_in, wo), (wu_in, wu), (wd_in, wd)):
            gap = jnp.zeros((fb_rows, dst.shape[1] - src.shape[1]), BF16)
            dst[rows, :] = jnp.concatenate([src[...], gap], axis=1)
    pl.semaphore_wait(barrier, 7 + nz - 1)

    own_feat = feat(0, 0)
    own_t = toks(g)
    partner = (z, g, 1 - c)
    me = c * 4 + g
    th = tok // 2

    def exchange(first, src, dst):
        for dd, dc in others:
            rcopy(src, dst, first + dd * 2 + dc, dev(dd, dc)).start()
            pending.append(lambda dd=dd, dc=dc: rcopy(src, dst, first + dd * 2 + dc, dev(dd, dc)).wait_send())

    passing = ((0, 1, 0), (1, 2, 1))

    def gather_copy(first, src, dst, n, size, dd, dc):
        tokens = pl.ds(pl.multiple_of(row_of(dc) * tok + n * size, 128), size)
        part = dst.at[own_feat, n * size : (n + 1) * size]
        return rcopy(src.at[:, tokens], part, first + n * 8 + dd * 2 + dc, dev(dd, dc))

    def gather_land(first, dst, n, size, dd, dc, sem):
        part = dst.at[feat(dd, dc), n * size : (n + 1) * size]
        return rcopy(part, part, first + n * 8 + sem, partner)

    def gather_pass(first, dst, n, size, k, dd, dc):
        part = dst.at[feat(dd, dc), n * size : (n + 1) * size]
        return rcopy(part, part, first + n * 8 + 6 + k, dev(3 - dd, 0))

    def gather_own(first, src, dst, n, size):
        tokens = pl.ds(pl.multiple_of(row_of(0) * tok + n * size, 128), size)
        return lcopy(src.at[:, tokens], dst.at[own_feat, n * size : (n + 1) * size], first + n * 8)

    def gather_start(first, src, dst, n, size):
        for dd, dc in near:
            gather_copy(first, src, dst, n, size, dd, dc).start()
        gather_own(first, src, dst, n, size).start()

    def gather_relay(first, dst, n, size):
        for k, dd, dc in passing:
            gather_land(first, dst, n, size, dd, dc, dd * 2 + dc).wait_recv()
            gather_pass(first, dst, n, size, k, dd, dc).start()

    def gather_done(first, src, dst, n, size):
        gather_own(first, src, dst, n, size).wait()
        for dd, dc in ((0, 1), (1, 1), (2, 0)):
            gather_land(first, dst, n, size, dd, dc, dd * 2 + dc).wait_recv()
        for k in (0, 1):
            gather_land(first, dst, n, size, 3, k, 6 + k).wait_recv()

    def gather_sent(first, src, dst, n, size):
        for dd, dc in near:
            gather_copy(first, src, dst, n, size, dd, dc).wait_send()
        for k, dd, dc in passing:
            gather_pass(first, dst, n, size, k, dd, dc).wait_send()

    q_cuts = (0, 256, 512, kp)
    weights = tuple(wq.at[:, q_cuts[p] : q_cuts[p + 1]] for p in range(3)) + (wo, wu, wd)
    inputs = (wq_in, None, None, wo_in, wu_in, wd_in)
    whole = (wq, wq, wq, wo, wu, wd)
    n_w = len(weights)
    steps = nz - 1
    nw = nz if zin else 1
    wz0 = take((n_w + 2) * nw)
    wc0 = take(4 * nw)

    def zrows(zz, core):
        return pl.ds(pl.multiple_of(core * half + zz * fb_rows, 16), fb_rows)

    def w_rows(i, zz, core):
        return weights[i].at[zrows(zz, core), :]

    def whole_rows(i, zz, core):
        return whole[i].at[zrows(zz, core), :]

    def hop(i, s, d):
        origin = z - (s - 1) if d == 0 else z + (s - 1)
        here = jnp.logical_and(z >= s - 1, z < nz - 1) if d == 0 else jnp.logical_and(z < nz - s + 1, z > 0)
        to = z + 1 if d == 0 else z - 1
        send = wz0 + n_w * nw + i if s == 1 and d == 1 else None
        return here, lambda: rcopy(w_rows(i, origin, c), w_rows(i, origin, c), wz0 + i * nw + origin, (to, g, c), send)

    def arrival(s, d):
        return (z >= s, z - s) if d == 0 else (z < nz - s, z + s)

    def pass_on(i, zz):
        first = max(i - 2, 0)
        return rcopy(whole_rows(i, zz, c), whole_rows(i, zz, c), wc0 + first * nw + zz, partner)

    def z_send(i, s):
        if not zin:
            if s == 1 and inputs[i] is not None:
                lcopy(inputs[i], whole[i], wz0 + i * nw).start()
            return
        for d in (0, 1):
            here, make = hop(i, s, d)
            pl.when(here)(lambda make=make: make().start())
        if s == 1 and i >= 2:
            pass_on(i, z).start()

    def z_recv(i, s):
        if not zin:
            return
        for d in (0, 1):
            here, origin = arrival(s, d)

            @pl.when(here)
            def _(s=s, d=d, origin=origin):
                rows = w_rows(i, origin, c)
                rcopy(rows, rows, wz0 + i * nw + origin, partner).wait_recv()
                if i >= 2:
                    pass_on(i, origin).start()

        if s < steps:
            z_send(i, s + 1)

    def weight_ready(i):
        if not zin:
            if inputs[i] is not None:
                lcopy(inputs[i], whole[i], wz0 + i * nw).wait()
            return
        if i >= 2:
            for zz in range(nz):
                rows = whole_rows(i, zz, 1 - c)
                rcopy(rows, rows, wc0 + (i - 2) * nw + zz, partner).wait_recv()

    def weight_passed(i):
        if not zin:
            return
        for s in range(1, nz):
            for d in (0, 1):
                here, make = hop(i, s, d)
                pl.when(here)(lambda make=make: make().wait_send())
        if i >= 2:
            for zz in range(nz):
                pass_on(i, zz).wait_send()

    p0 = take(8)
    xs0 = take(16)
    cs0 = take(16)
    exchange(p0, prm_send, prm_all.at[me])
    lcopy(prm_send, prm_all.at[me], p0).start()
    for n in (0, 1):
        gather_start(xs0, x_ref, x_t, n, th)
    for i in range(3):
        z_send(i, 1)

    def par(k):
        return prm_col[:, k : k + 1]

    def z_recv_all(pairs):
        for i, step in pairs:
            if step < nz:
                z_recv(i, step)

    def head_rows(part, h):
        return pl.ds(pl.multiple_of((part * heads + h) * HEAD_PAD, 16), HEAD_PAD)

    def project(j, carry):
        t = toks(j)
        x = x_t[:, t].astype(F32)
        m = jnp.sum(x, axis=0, keepdims=True) * (1.0 / width)
        q = jnp.sum(x * x, axis=0, keepdims=True) * (1.0 / width)
        r = lax.rsqrt(q - m * m + EPSILON)
        rows_f[2, 0:1, t] = m
        rows_f[3, 0:1, t] = r
        h1_t[:, t] = ((x - m) * r * par(0) + par(1)).astype(BF16)
        part = mm(wq[...], h1_t[:, t], TN) + prm_col[0:kp, 9:10]
        for p in range(3):
            for h in range(heads):
                first, row = (p * heads + h) * HEAD_PAD, p * hd + h * HEAD_DIM
                qkv_t[first : first + HEAD_DIM, t] = part[row : row + HEAD_DIM, :].astype(BF16)
        return carry

    z_recv_all(((0, 1), (1, 1), (2, 1)))
    z_send(3, 1)
    gather_relay(xs0, x_t, 0, th)
    z_recv_all(((0, 2), (1, 2), (2, 2)))
    gather_relay(xs0, x_t, 1, th)
    z_recv_all(((3, 1),))

    lcopy(prm_send, prm_all.at[me], p0).wait()
    for dd, dc in others:
        rcopy(prm_send, prm_all.at[row_of(dc) * 4 + gx_of(dd)], p0 + dd * 2 + dc, partner).wait_recv()
    for b in range(8):
        rows = jnp.concatenate([prm_all[b], jnp.zeros((120, 256), F32)], axis=0)
        prm_col[b * fb_rows : (b + 1) * fb_rows, 0:8] = jnp.transpose(rows)[:fb_rows, 0:8]

    for step in range(3, nz):
        z_recv_all((i, step) for i in range(3))
    for i in range(3):
        weight_ready(i)
    gather_done(xs0, x_ref, x_t, 0, th)
    gather_start(cs0, cot_ref, cot_t, 0, th)
    lax.fori_loop(0, 2, project, 0)
    z_recv_all(((3, 2),))
    z_send(4, 1)
    gather_done(xs0, x_ref, x_t, 1, th)
    lax.fori_loop(2, 4, project, 0)
    z_recv_all((3, step) for step in range(3, nz))
    z_send(5, 1)
    weight_ready(3)

    def kept_of(h, t):
        scores = mm(qkv_t[head_rows(1, h), :], qkv_t[head_rows(0, h), t], TN) * factor
        key_pic = pk[...]
        query_pic = rows_f[0, 0:1, t].astype(jnp.int32)
        allowed = jnp.concatenate([key_pic] * (tb // 128), axis=1) == query_pic
        return jnp.where(allowed, jnp.exp(scores), 0.0)

    wn0 = take(8)

    def wo_part(gx, core, first=0, last=None):
        rows = (fb_rows if last is None else last) - first
        return wo_n.at[pl.ds(pl.multiple_of(gx * hd + core * fb_rows + first, 16), rows), :]

    cut = fb_rows // 32 * 16 + 16

    def wo_copy(n):
        if n < 2:
            own = wo_part(g, c)
            return rcopy(own, own, wn0 + n + 1, (z, gx_of(n + 1), c))
        if n < 4:
            got = wo_part(gx_of(n - 1), c)
            return rcopy(got, got, wn0 + n + 1, partner)
        if n < 6:
            on = wo_part(gx_of(1), c, 0, cut) if n == 4 else wo_part(gx_of(2), c, cut)
            return rcopy(on, on, wn0 + n + 1, (z, gx_of(6 - n), c))
        far = wo_part(gx_of(3), c)
        return rcopy(far, far, wn0 + 7, partner)

    def wo_first():
        turned = jnp.transpose(wo[...])
        wo_n[pl.ds(pl.multiple_of(g * hd, 16), hd), :] = turned[0:hd, :]
        for n in (0, 1):
            wo_copy(n).start()

    def wo_second():
        for step in (1, 2):
            got = wo_part(gx_of(step), c)
            rcopy(got, got, wn0 + step, partner).wait_recv()
        for n in (4, 5, 2, 3):
            wo_copy(n).start()

    def wo_third():
        for step, on in ((1, wo_part(gx_of(3), c, 0, cut)), (2, wo_part(gx_of(3), c, cut))):
            rcopy(on, on, wn0 + 4 + step, partner).wait_recv()
        wo_copy(6).start()

    def wo_ready():
        for step in (1, 2):
            got = wo_part(gx_of(step), 1 - c)
            rcopy(got, got, wn0 + 2 + step, partner).wait_recv()
        far = wo_part(gx_of(3), 1 - c)
        rcopy(far, far, wn0 + 7, partner).wait_recv()

    at0 = take(4 * 3)
    own_heads = pl.ds(pl.multiple_of(g * hd, 16), hd)

    def att_piece(dd, j):
        return att_t.at[pl.ds(pl.multiple_of(gx_of(dd) * hd, 16), hd), toks(j)]

    def att_send(j, start):
        for step in (1, 2):
            piece = att_piece(0, j)
            cp = rcopy(piece, piece, at0 + j * 3 + step - 1, (z, gx_of(step), c))
            cp.start() if start else cp.wait_send()

    def att_relay(j):
        for step in (1, 2):
            piece = att_piece(step, j)
            rcopy(piece, piece, at0 + j * 3 + step - 1, partner).wait_recv()
        step = 1 if j < 2 else 2
        piece = att_piece(step, j)
        rcopy(piece, piece, at0 + j * 3 + 2, (z, gx_of(3 - step), c)).start()

    def att_relayed(j):
        piece = att_piece(1 if j < 2 else 2, j)
        rcopy(piece, piece, at0 + j * 3 + 2, partner).wait_send()

    def attend(j, carry):
        t = toks(j)

        def head(h, inner):
            kept = kept_of(h, t)
            den = jnp.sum(kept, axis=0, keepdims=True)
            den = jnp.where(rows_f[1, 0:1, t] > 0.5, den, 1.0)
            scale = jnp.where(den > 1e30, 2.0**-40, 1.0)
            inv = 1.0 / (den * scale)
            rows_f[4 + 2 * h, 0:1, t] = scale
            rows_f[5 + 2 * h, 0:1, t] = inv
            probs = (kept * scale * inv).astype(BF16)
            att = mm(qkv_t[head_rows(2, h), :], probs, NN)
            dqf[pl.ds(pl.multiple_of(h * HEAD_DIM, 8), HEAD_DIM), :] = att[0:HEAD_DIM, :]
            return inner

        lax.fori_loop(0, heads, head, 0)
        att_t[own_heads, t] = dqf[...].astype(BF16)

        att_send(j, True)

        @pl.when(j == 1)
        def _():
            wo_second()
            z_recv_all(((4, 1),))

        @pl.when(j == 2)
        def _():
            att_relay(0)

        return carry

    wo_first()
    lax.fori_loop(0, 4, attend, 0)
    wo_third()
    att_relay(1)
    z_recv_all(((4, 2),))

    def project_out(j, carry):
        t = toks(j)

        @pl.when(j == 0)
        def _():
            att_relay(2)
            wo_ready()

        @pl.when(j == 1)
        def _():
            att_relay(3)
            gather_relay(cs0, cot_t, 0, th)
            gather_start(cs0, cot_ref, cot_t, 1, th)
            z_recv_all(((5, 1),))

        far = att_piece(3, j)
        rcopy(far, far, at0 + j * 3 + 2, partner).wait_recv()
        residual = mm(wo_n[...], att_t[:, t], TN) + x_t[:, t].astype(F32) + par(2)
        m2 = jnp.sum(residual, axis=0, keepdims=True) * (1.0 / width)
        q2 = jnp.sum(residual * residual, axis=0, keepdims=True) * (1.0 / width)
        r2 = lax.rsqrt(q2 - m2 * m2 + EPSILON)
        rows_f[2, 1:2, t] = m2
        rows_f[3, 1:2, t] = r2
        h2_t[:, t] = ((residual - m2) * r2 * par(3) + par(4)).astype(BF16)

        @pl.when(j == g)
        def _():
            resid[...] = residual

        return carry

    lax.fori_loop(0, 4, project_out, 0)
    z_recv_all((4, step) for step in range(3, nz))
    weight_ready(4)
    for n in range(7):
        wo_copy(n).wait_send()

    def spread(first, buf):
        for step in (1, 2):
            rcopy(buf.at[:, own_t], buf.at[:, own_t], first + step, (z, gx_of(step), c)).start()

    def halves(buf, step, k):
        return buf.at[(k - 1) * half : k * half, toks(gx_of(step))]

    def spread_relay(first, buf):
        for step in (1, 2):
            block = buf.at[:, toks(gx_of(step))]
            rcopy(block, block, first + step, partner).wait_recv()
            part = halves(buf, step, step)
            rcopy(part, part, first + 2 + step, (z, gx_of(3 - step), c)).start()

    def spread_done(first, buf):
        for k in (1, 2):
            part = halves(buf, 3, k)
            rcopy(part, part, first + 2 + k, partner).wait_recv()

    def spread_sent(first, buf):
        for step in (1, 2):
            rcopy(buf.at[:, own_t], buf.at[:, own_t], first + step, partner).wait_send()
            part = halves(buf, step, step)
            rcopy(part, part, first + 2 + step, partner).wait_send()

    def mlp_up(i, carry):
        t = toks(i)
        fa[...] = mm(wu[...], h2_t[:, t], TN) + prm_col[:, 8:9]

        def chunk(n, inner):
            rows = pl.ds(pl.multiple_of(n * 48, 16), 48)
            v = fa[rows, :]
            v2 = v * v
            thv = jnp.tanh(GELU_C * (v + GELU_A * v2 * v))
            hf = 0.5 * (1.0 + thv)
            act_t[rows, t] = (v * hf).astype(BF16)
            slope = hf + (0.5 * GELU_C) * v * (1.0 - thv * thv) * (1.0 + (3.0 * GELU_A) * v2)
            gpre_t[rows, t] = slope.astype(BF16)
            return inner

        lax.fori_loop(0, fa.shape[0] // 48, chunk, 0)

        @pl.when(i == 0)
        def _():
            z_recv_all(((5, 2),))

        @pl.when(i == 1)
        def _():
            gather_relay(cs0, cot_t, 1, th)

        return carry

    lax.fori_loop(0, 4, mlp_up, 0)
    for n in (0, 1):
        gather_done(cs0, cot_ref, cot_t, n, th)
    z_recv_all((5, step) for step in range(3, nz))
    weight_ready(5)

    for n in (0, 1):
        gather_sent(xs0, x_ref, x_t, n, th)
    g20 = xs0

    def tsend(step):
        return wo_n.at[:, (step - 1) * tb : step * tb]

    def g2_copy(n):
        top, bottom = slice(0, half), slice(half, width)
        rows = (top, bottom, top, bottom, bottom, top)[n]
        step = (3, 3, 1, 1, 2, 2)[n]
        slot = (2, 2, 0, 0, 1, 1)[n]
        to = (1, 2, 1, 1, 2, 2)[n]
        src = wo_n.at[rows, (step - 1) * tb : step * tb]
        return rcopy(src, trecv.at[slot, rows, :], g20 + n, (z, gx_of(to), c))

    def mlp_back(i, carry):
        t = toks(gx_of(3 - i))
        gpre_t[:, t] = (mm(wd[...], cot_t[:, t], TN) * gpre_t[:, t].astype(F32)).astype(BF16)
        fa[...] = mm(wu[...], gpre_t[:, t], NN)
        for step, sends in ((3, (0, 1)), (2, (4,)), (1, (2,))):

            @pl.when(i == 3 - step)
            def _(step=step, sends=sends):
                tsend(step)[...] = fa[...].astype(BF16)
                for n in sends:
                    g2_copy(n).start()

        return carry

    lax.fori_loop(0, 4, mlp_back, 0)
    for n, step, rows, then in ((0, 2, slice(0, half), 5), (1, 1, slice(half, width), 3)):
        g2_copy(n).wait_recv()
        cols = slice((step - 1) * tb, step * tb)
        wo_n[rows, cols] = (wo_n[rows, cols].astype(F32) + trecv[2, rows, :].astype(F32)).astype(BF16)
        g2_copy(then).start()

    dwc0 = take(4)
    dwz0 = take(4 * 6)
    do0 = take(4)
    gath = ((0, 1, 2), (3,), (4,), (5,))
    core_recv = (cq, co, cu, cd)
    z_recvs = (zq, zo, zu, zd)
    dw_refs = (wo_n, wo, wu, wd)
    dw_cols = (kp, wo.shape[1], wu.shape[1], wd.shape[1])
    dw_outs = (dq_out, do_out, du_out, dd_out)
    slots = [0]
    leaving = []

    def weight_grad(i, left, right):
        for n in gath[i]:
            weight_passed(n)
        dst, cols = dw_refs[i], dw_cols[i]
        step_cols = 384

        def one(n, carry):
            cs = pl.ds(pl.multiple_of(n * step_cols, 128), step_cols)
            dst[:, cs] = mm(left[...], right[pl.ds(pl.multiple_of(n * step_cols, 16), step_cols), :], NT).astype(BF16)
            return carry

        lax.fori_loop(0, cols // step_cols, one, 0)
        rest = cols // step_cols * step_cols
        if rest < cols:
            dst[:, rest:cols] = mm(left[...], right[rest:cols, :], NT).astype(BF16)

    def core_half(i, core):
        return dw_refs[i].at[pl.ds(pl.multiple_of(core * half, 16), half), 0 : dw_cols[i]]

    def send_core(i):
        if zin:
            rcopy(core_half(i, 1 - c), core_recv[i], dwc0 + i, partner).start()
            pending.append(lambda: rcopy(core_half(i, 1 - c), core_recv[i], dwc0 + i, partner).wait_send())
        else:
            lcopy(dw_refs[i].at[:, 0 : dw_cols[i]], dw_outs[i], dwc0 + i).start()

    def sum_core(i):
        if not zin:
            return
        rcopy(core_half(i, c), core_recv[i], dwc0 + i, partner).wait_recv()
        w = dw_refs[i]
        for zz in range(nz):
            rows = pl.ds(pl.multiple_of(c * half + zz * fb_rows, 16), fb_rows)
            cols = dw_cols[i]
            w[rows, 0:cols] = (
                w[rows, 0:cols].astype(F32) + core_recv[i][zz * fb_rows : (zz + 1) * fb_rows, :].astype(F32)
            ).astype(BF16)

        @pl.when(leaf)
        def _():
            for slot, zz in enumerate((far_end, far_inner, inner)):
                z_piece(i, slot, zz, slot, inner).start()

        @pl.when(jnp.logical_not(leaf))
        def _():
            z_piece(i, 3, end, 0, end).start()

    leaf = z % 3 == 0
    low = z < 2
    end, inner = jnp.where(low, 0, 3), jnp.where(low, 1, 2)
    far_end, far_inner = 3 - end, 3 - inner

    def z_piece(i, sem, zz, slot, to):
        rows = dw_refs[i].at[zrows(zz, c), 0 : dw_cols[i]]
        return rcopy(rows, z_recvs[i].at[slot], dwz0 + i * 6 + sem, (to, g, c))

    def z_land(i, slot):
        rows = dw_refs[i].at[zrows(z, c), 0 : dw_cols[i]]
        return rcopy(rows, z_recvs[i].at[min(slot, 3) if slot != 3 else 0], dwz0 + i * 6 + slot, partner)

    def relay_z(i, slot):
        if not zin:
            return

        @pl.when(jnp.logical_not(leaf))
        def _():
            z_land(i, slot).wait_recv()
            zz = far_end if slot == 0 else far_inner
            w, cols = dw_refs[i], dw_cols[i]
            rows = zrows(zz, c)
            w[rows, 0:cols] = (w[rows, 0:cols].astype(F32) + z_recvs[i][slot].astype(F32)).astype(BF16)
            z_piece(i, 4 + slot, zz, 3, zz).start()

    def z_sent(i):
        if not zin:
            return

        @pl.when(leaf)
        def _():
            for slot, zz in enumerate((far_end, far_inner, inner)):
                z_piece(i, slot, zz, slot, inner).wait_send()

        @pl.when(jnp.logical_not(leaf))
        def _():
            z_piece(i, 3, end, 0, end).wait_send()
            z_piece(i, 4, far_end, 3, far_end).wait_send()
            z_piece(i, 5, far_inner, 3, far_inner).wait_send()

    def sum_z(i):
        if not zin:
            lcopy(dw_refs[i].at[:, 0 : dw_cols[i]], dw_outs[i], dwc0 + i).wait()
            return

        @pl.when(leaf)
        def _():
            z_land(i, 3).wait_recv()
            z_land(i, 4).wait_recv()

        @pl.when(jnp.logical_not(leaf))
        def _():
            z_land(i, 2).wait_recv()
            z_land(i, 5).wait_recv()

        near_slot = jnp.where(leaf, 0, 2)
        cols = dw_cols[i]

        def total_of(n, size):
            part = dw_refs[i][zrows(z, c), n : n + size].astype(F32)
            return part + z_recvs[i][near_slot, :, n : n + size].astype(F32) + z_recvs[i][3, :, n : n + size].astype(F32)

        if i == 0:
            whole = total_of(0, cols)
            gap = jnp.zeros((fb_rows, hw - hd), F32)
            pieces = []
            for p in range(3):
                part = jnp.concatenate([whole[:, p * hd : (p + 1) * hd], gap], axis=1)
                for n in range(0, hw, tb):
                    size = min(tb, hw - n)
                    pieces.append((part[:, n : n + size], dq_out.at[p, :, n : n + size]))
        else:
            pieces = []
            for n in range(0, cols, tb):
                size = min(tb, cols - n)
                pieces.append((total_of(n, size), dw_outs[i].at[:, n : n + size]))
        for part, goes in pieces:
            size = part.shape[1]
            slot = slots[0] % 16
            if slots[0] >= 4:
                leaving[slots[0] - 4].wait()
            slots[0] += 1
            stage = (fa, fb)[slot // 8].at[(slot % 8) * fb_rows : (slot % 8 + 1) * fb_rows, 0:size]
            stage[...] = part
            cp = lcopy(stage, goes, do0 + slot % 4)
            cp.start()
            leaving.append(cp)

    ml0, gh0, uv0, sm0 = cs0, xs0, at0, p0
    for n in (0, 1):
        gather_sent(cs0, cot_ref, cot_t, n, th)
    for j in range(4):
        att_send(j, False)
        att_relayed(j)
    for wait in pending:
        wait()
    pending.clear()
    sz0 = take(nz)

    direct, added = ((1, 0), (2, 1), (0, 1)), ((1, 1), (2, 0))

    def hand(buf, relay, first, j, n):
        part = relay.at[n, :, toks(j)]
        return rcopy(buf.at[feat(3, n), toks(j)], part, first + 8 + j * 2 + n, (z, gx_of(n + 1), c))

    def block_copy(buf, recv, first, dd, dc):
        slot = dd * 2 + dc
        return rcopy(buf.at[feat(dd, dc), :], recv.at[slot], first + slot, dev(dd, dc))

    def add_relayed(buf, relay, recv, first):
        for n, (dd, dc) in ((0, (2, 0)), (1, (1, 1))):
            for j in range(4):
                hand(buf, relay, first, j, n).wait_recv()
            rows = feat(dd, dc)
            buf[rows, :] = (buf[rows, :].astype(F32) + relay[n].astype(F32)).astype(BF16)
            block_copy(buf, recv, first, dd, dc).start()

    def scatter_sent(buf, relay, recv, first):
        for dd, dc in direct + added:
            block_copy(buf, recv, first, dd, dc).wait_send()
        for n in (0, 1):
            for j in range(4):
                hand(buf, relay, first, j, n).wait_send()

    def scatter_start(buf, recv, first):
        for dd, dc in direct:
            block_copy(buf, recv, first, dd, dc).start()
        lcopy(buf.at[own_feat, :], recv.at[0], first).start()

    def scatter_sum(buf, recv, first, dc):
        if dc == 0:
            lcopy(buf.at[own_feat, :], recv.at[0], first).wait()
        acc = 0.0
        for dd in (0, 1, 2):
            if dd or dc:
                block_copy(buf, recv, first, dd, dc).wait_recv()
            acc = acc + recv[dd * 2 + dc].astype(F32)
        return acc

    weight_grad(2, h2_t, gpre_t)
    send_core(2)


    def lower(j, carry):
        t = toks(j)
        h2_t[:, t] = mm(wd[...], act_t[:, t], NN).astype(BF16)
        return carry

    lax.fori_loop(0, 4, lower, 0)
    h2_t[:, own_t] = (mm(wd[...], act_t[:, own_t], NN) + resid[...] + par(5)).astype(BF16)
    sum_core(2)
    ones = jnp.ones((tok, 128), BF16)
    sums_col[0 : act_t.shape[0], 6:7] = mm(gpre_t[...], ones, NN)[:, 0:1]

    for n in (2, 3, 4, 5):
        g2_copy(n).wait_recv()
    gh2 = fa[...] + trecv[0].astype(F32) + trecv[1].astype(F32)
    m2 = rows_f[2, 1:2, own_t]
    r2 = rows_f[3, 1:2, own_t]
    normed2 = (resid[...] - m2) * r2
    gn = gh2 * par(3)
    s1 = jnp.sum(gn, axis=0, keepdims=True) * (1.0 / width)
    s2 = jnp.sum(gn * normed2, axis=0, keepdims=True) * (1.0 / width)
    cot_own = cot_t[:, own_t].astype(F32)
    g_res = cot_own + r2 * (gn - s1 - normed2 * s2)
    g_low = g_res.astype(BF16)
    gb_t[:, own_t] = g_low
    gb0 = wn0
    spread(gb0, gb_t)
    resid[...] = g_res
    sums_col[0:width, 2:3] = jnp.sum(g_low.astype(F32), axis=1, keepdims=True)
    sums_col[0:width, 3:4] = jnp.sum(gh2 * normed2, axis=1, keepdims=True)
    sums_col[0:width, 4:5] = jnp.sum(gh2, axis=1, keepdims=True)
    sums_col[0:width, 5:6] = jnp.sum(cot_own, axis=1, keepdims=True)
    for n in range(6):
        g2_copy(n).wait_send()
    weight_grad(3, cot_t, act_t)
    send_core(3)
    relay_z(2, 0)
    sum_core(3)

    fa[...] = jnp.zeros_like(fa)
    fb[...] = jnp.zeros_like(fb)
    act_t[3 * hd : kp, :] = jnp.zeros((kp - 3 * hd, tok), BF16)

    def attend_back(i, carry):
        t = toks(gx_of(i))

        @pl.when(i == 1)
        def _():
            spread_relay(gb0, gb_t)
            for n in (0, 1):
                for k in range(4):
                    hand(h2_t, mrelay, ml0, k, n).start()
            scatter_start(h2_t, mrecv, ml0)

        @pl.when(i == 3)
        def _():
            spread_done(gb0, gb_t)

        gatt = mm(wo[...], gb_t[:, t], TN)
        for h in range(heads):
            gatt_t[h * HEAD_PAD : h * HEAD_PAD + HEAD_DIM, :] = gatt[h * HEAD_DIM : (h + 1) * HEAD_DIM, :].astype(BF16)

        @pl.when(i == 2)
        def _():
            relay_z(2, 1)

        @pl.when(i == 3)
        def _():
            weight_passed(3)
            wo[:, 0:hd] = mm(gb_t[...], att_t[own_heads, :], NT).astype(BF16)
            send_core(1)

        def head(h, inner):
            kept = kept_of(h, t)
            probs = kept * rows_f[4 + 2 * h, 0:1, t] * rows_f[5 + 2 * h, 0:1, t]
            q_rows = head_rows(0, h)
            grad = gatt_t[q_rows, :]
            grad_probs = mm(qkv_t[head_rows(2, h), :], grad, TN)
            weighted = probs * grad_probs
            delta = jnp.sum(weighted, axis=0, keepdims=True)
            grad_scores = (weighted - probs * delta).astype(BF16)
            dq = mm(qkv_t[head_rows(1, h), :], grad_scores, NN) * factor
            dqf[pl.ds(pl.multiple_of(h * HEAD_DIM, 8), HEAD_DIM), :] = dq[0:HEAD_DIM, :]
            dk = mm(qkv_t[q_rows, t], grad_scores, NT)
            dv = mm(grad, probs.astype(BF16), NT)
            for kb in range(4):
                rows = pl.ds(pl.multiple_of(kb * hd + h * HEAD_DIM, 8), HEAD_DIM)
                fa[rows, :] += dk[0:HEAD_DIM, kb * tb : (kb + 1) * tb]
                fb[rows, :] += dv[0:HEAD_DIM, kb * tb : (kb + 1) * tb]
            return inner

        lax.fori_loop(0, heads, head, 0)
        act_t[0:hd, t] = dqf[...].astype(BF16)
        return carry

    lax.fori_loop(0, 4, attend_back, 0)

    for kb in range(4):
        cols, rows = slice(kb * tb, (kb + 1) * tb), slice(kb * hd, (kb + 1) * hd)
        act_t[hd : 2 * hd, cols] = (fa[rows, :] * factor).astype(BF16)
        act_t[2 * hd : 3 * hd, cols] = fb[rows, :].astype(BF16)
    add_relayed(h2_t, mrelay, mrecv, ml0)
    sum_core(1)
    relay_z(3, 0)

    def back1(j, carry):
        t = toks(j)
        gh1 = mm(wq[...], act_t[0:kp, t], NN)
        m = rows_f[2, 0:1, t]
        r = rows_f[3, 0:1, t]
        normed = (x_t[:, t].astype(F32) - m) * r
        gn1 = gh1 * par(0)
        prod = gh1 * normed
        sums_col[0:width, 0:1] += jnp.sum(prod, axis=1, keepdims=True)
        sums_col[0:width, 1:2] += jnp.sum(gh1, axis=1, keepdims=True)
        a1 = jnp.sum(gn1, axis=0, keepdims=True) * (1.0 / width)
        a2 = jnp.sum(gn1 * normed, axis=0, keepdims=True) * (1.0 / width)
        v = r * r * a2
        u = r * a1 - m * v
        for n in range(tb // 128):
            row = j * (tb // 128) + n
            uv_send[pl.ds(row, 1), :] = u[:, n * 128 : (n + 1) * 128]
            uv_send[pl.ds(tok // 128 + row, 1), :] = v[:, n * 128 : (n + 1) * 128]
        fa[...] = r * gn1

        @pl.when(j == g)
        def _():
            fa[...] += resid[...]

        cot_t[:, t] = fa[...].astype(BF16)
        for n in (0, 1):
            hand(cot_t, grelay, gh0, j, n).start()
        return carry

    lax.fori_loop(0, 4, back1, 0)

    scatter_start(cot_t, grecv, gh0)
    weight_grad(0, h1_t, act_t)
    send_core(0)
    sums_col[0:kp, 7:8] = mm(act_t[0:kp, :], ones, NN)[:, 0:1]
    relay_z(3, 1)
    relay_z(1, 0)
    relay_z(1, 1)
    sum_core(0)

    for n in range(0, sm_send.shape[1], 128):
        sm_send[:, n : n + 128] = jnp.transpose(sums_col[n : n + 128, :])[0:8, :]
    exchange(sm0, sm_send, sm_recv.at[me])
    exchange(uv0, uv_send, uv_recv.at[me])
    lcopy(uv_send, uv_recv.at[me], uv0).start()
    add_relayed(cot_t, grelay, grecv, gh0)
    relay_z(0, 0)

    for dc in (0, 1):
        out_ref[:, row_tok(dc)] = scatter_sum(h2_t, mrecv, ml0, dc).astype(BF16)

    sum_z(2)
    sum_z(3)

    total_sm = sm_send[...]
    row8 = lax.broadcasted_iota(jnp.int32, total_sm.shape, 0)
    for dd, dc in others:
        rcopy(sm_send, sm_recv.at[row_of(dc) * 4 + gx_of(dd)], sm0 + dd * 2 + dc, partner).wait_recv()
        part = sm_recv[row_of(dc) * 4 + gx_of(dd)]
        total_sm = total_sm + (part if dd == 0 else jnp.where(row8 < 6, part, 0.0))
    smz_recv[0] = total_sm
    for k in range(1, nz):

        def make(k=k):
            return rcopy(smz_recv.at[0], smz_recv.at[k], sz0 + k, ((z + k) % nz, g, c))

        make().start()
        pending.append(lambda make=make: make().wait_send())

    relay_z(0, 1)
    sum_z(1)

    lcopy(uv_send, uv_recv.at[me], uv0).wait()
    for dd, dc in others:
        rcopy(uv_send, uv_recv.at[row_of(dc) * 4 + gx_of(dd)], uv0 + dd * 2 + dc, partner).wait_recv()
    for dc in (0, 1):
        acc = scatter_sum(cot_t, grecv, gh0, dc)
        uv = uv_recv[row_of(dc) * 4 + g]
        for dd in (1, 2, 3):
            uv = uv + uv_recv[row_of(dc) * 4 + gx_of(dd)]
        n_rows = tok // 128
        u_row = jnp.concatenate([uv[n : n + 1, :] for n in range(n_rows)], axis=1)
        v_row = jnp.concatenate([uv[n_rows + n : n_rows + n + 1, :] for n in range(n_rows)], axis=1)
        x_own = x_ref[:, row_tok(dc)].astype(F32)
        ig_ref[:, row_tok(dc)] = acc - u_row - x_own * v_row

    sum_z(0)
    total_z = smz_recv[0]
    for k in range(1, nz):
        rcopy(smz_recv.at[0], smz_recv.at[k], sz0 + k, partner).wait_recv()
        total_z = total_z + smz_recv[k]
    sm_out[...] = total_z

    for cp in leaving[-4:]:
        cp.wait()
    for wait in pending:
        wait()
    scatter_sent(h2_t, mrelay, mrecv, ml0)
    scatter_sent(cot_t, grelay, grecv, gh0)
    for i in range(4):
        z_sent(i)
    spread_sent(gb0, gb_t)


def local(
    block_input,
    lengths,
    ln1_gain,
    ln1_bias,
    w_qkv,
    qv_bias,
    w_out,
    out_bias,
    ln2_gain,
    ln2_bias,
    w_up,
    up_bias,
    w_down,
    down_bias,
    cotangent,
):
    nz = lax.axis_size("dp")
    fb_rows, tok2 = block_input.shape[1], block_input.shape[2]
    tok = tok2 // 2
    width = 8 * fb_rows
    heads = w_qkv.shape[3] // HEAD_DIM
    hd = heads * HEAD_DIM
    hw = round_up(hd, 128)
    hp = heads * HEAD_PAD
    hid = w_up.shape[2]
    kh = round_up(hid, 384)
    kp = round_up(3 * hd, 128)
    zrow = w_qkv.shape[1]
    zin = zrow == fb_rows and nz == 4

    wq, wo = jnp.transpose(w_qkv[0], (1, 0, 2)), jnp.transpose(w_out[:, 0, :])
    wu, wd = w_up[0], jnp.transpose(w_down[:, 0, :])
    if not zin:

        def gather(w, cols):
            w = jnp.pad(w, ((0, 0), (0, cols - w.shape[1])))
            return lax.all_gather(lax.all_gather(w, "dp", axis=0, tiled=True), "gy", axis=0, tiled=True)

        wq = gather(w_qkv[0].reshape(zrow, 3 * hd), kp)
        wo, wu, wd = gather(wo, hw), gather(wu, kh), gather(wd, kh)

    cfg = dict(nz=nz, zin=zin, fb=fb_rows, tok=tok, heads=heads, hw=hw, kp=kp)
    tb = tok // 4
    half = width // 2
    vm = pltpu.VMEM
    n_sems = 92 + nz + (12 * nz if zin else 12)
    dw_specs = [pl.BlockSpec(memory_space=pl.ANY)] * 4
    if zin:
        dw_shapes = (jax.ShapeDtypeStruct((3, fb_rows, hw), F32),)
        dw_shapes += tuple(jax.ShapeDtypeStruct((fb_rows, k), F32) for k in (hw, kh, kh))
        core_shapes = [vm((half, k), BF16) for k in (kp, hw, kh, kh)]
        z_shapes = [vm((4, fb_rows, k), BF16) for k in (kp, hw, kh, kh)]
    else:
        dw_shapes = tuple(jax.ShapeDtypeStruct((width, k), BF16) for k in (kp, hw, kh, kh))
        core_shapes = [vm((16, 128), BF16)] * 4
        z_shapes = [vm((16, 128), BF16)] * 4
    scratch = [
        vm((8, 256), F32),
        vm((8, 8, 256), F32),
        vm((width, 128), F32),
        vm((width, tok), BF16),
        vm((width, tok), BF16),
        vm((width, tok), BF16),
        vm((width, tok), BF16),
        vm((width, tok), BF16),
        vm((width, kp), BF16),
        vm((width, hw), BF16),
        vm((width, kh), BF16),
        vm((width, kh), BF16),
        vm((3 * hp, tok), BF16),
        vm((4 * hd, tok), BF16),
        vm((4 * hd, width), BF16),
        vm((hp, tb), BF16),
        vm((kh, tok), BF16),
        vm((kh, tok), BF16),
        vm((width, tb), F32),
        vm((3, width, tb), BF16),
        vm((6, fb_rows, tok), BF16),
        vm((6, fb_rows, tok), BF16),
        vm((2, fb_rows, tok), BF16),
        vm((2, fb_rows, tok), BF16),
        vm((hd, tb), F32),
        vm((max(width, kh), tb), F32),
        vm((max(width, kh), tb), F32),
        vm((tok, 128), jnp.int32),
        vm((4 + 2 * heads, 8, tok), F32),
        vm((max(width, kh), 128), F32),
        vm((tok // 64, 128), F32),
        vm((8, tok // 64, 128), F32),
        vm((8, max(width, kh)), F32),
        vm((8, 8, max(width, kh)), F32),
        vm((nz, 8, max(width, kh)), F32),
        *core_shapes,
        *z_shapes,
        pltpu.SemaphoreType.DMA((n_sems,)),
        pltpu.SemaphoreType.DMA((n_sems,)),
    ]
    any_spec = pl.BlockSpec(memory_space=pl.ANY)
    vmem_spec = pl.BlockSpec(memory_space=pltpu.VMEM)
    w_spec = vmem_spec if zin else any_spec
    out, ig, dq, do, du, dd, sm = pl.pallas_call(
        functools.partial(block_kernel, cfg),
        out_shape=(
            jax.ShapeDtypeStruct((fb_rows, tok2), BF16),
            jax.ShapeDtypeStruct((fb_rows, tok2), F32),
            *dw_shapes,
            jax.ShapeDtypeStruct((8, max(width, kh)), F32),
        ),
        in_specs=[pl.BlockSpec(memory_space=pltpu.SMEM)] + [vmem_spec] * 7 + [any_spec] + [w_spec] * 4 + [vmem_spec] * 2,
        out_specs=(vmem_spec, vmem_spec, *dw_specs, vmem_spec),
        scratch_shapes=scratch,
        compiler_params=pltpu.CompilerParams(
            collective_id=0, has_side_effects=True, vmem_limit_bytes=67043328
        ),
        name="encoder_block",
    )(
        lengths,
        ln1_gain,
        ln1_bias,
        out_bias,
        ln2_gain,
        ln2_bias,
        down_bias,
        block_input[0],
        cotangent[0],
        wq,
        wo,
        wu,
        wd,
        qv_bias,
        up_bias,
    )

    if not zin:

        def reduce(a):
            a = lax.psum_scatter(a, "gy", scatter_dimension=0, tiled=True)
            return lax.optimization_barrier(lax.psum_scatter(a, "dp", scatter_dimension=0, tiled=True)).astype(F32)

        dq, do, du, dd = reduce(dq), reduce(do), reduce(du), reduce(dd)
        dq = jnp.transpose(dq[:, : 3 * hd].reshape(zrow, 3, hd), (1, 0, 2))

    mine = lax.axis_index("gy") * (width // 2) + lax.axis_index("gx") * fb_rows
    feats = lax.dynamic_slice(sm, (0, mine), (6, fb_rows))
    return (
        out[None],
        ig[None],
        feats[0:1],
        feats[1:2],
        jnp.transpose(dq[:, :, :hd], (1, 0, 2))[None],
        jnp.concatenate([sm[7:8, :hd], sm[7:8, 2 * hd : 3 * hd]], axis=0),
        jnp.transpose(do[:, :hd])[:, None, :],
        feats[2:3],
        feats[3:4],
        feats[4:5],
        du[None, :, :hid],
        sm[6, :hid],
        jnp.transpose(dd[:, :hid])[:, None, :],
        feats[5:6],
    )


def solution(mesh):
    in_specs = (
        P("gy", "gx", "dp"),
        P(("dp", "gy"), None),
        P("gy", "gx"),
        P("gy", "gx"),
        P("gy", "dp", None, "gx"),
        P(None, "gx"),
        P("gx", "gy", "dp"),
        P("gy", "gx"),
        P("gy", "gx"),
        P("gy", "gx"),
        P("gy", "dp", "gx"),
        P("gx"),
        P("gx", "gy", "dp"),
        P("gy", "gx"),
        P("gy", "gx", "dp"),
    )
    out_specs = (
        P("gy", "gx", "dp"),
        P("gy", "gx", "dp"),
        P("gy", "gx"),
        P("gy", "gx"),
        P("gy", "dp", None, "gx"),
        P(None, "gx"),
        P("gx", "gy", "dp"),
        P("gy", "gx"),
        P("gy", "gx"),
        P("gy", "gx"),
        P("gy", "dp", "gx"),
        P("gx"),
        P("gx", "gy", "dp"),
        P("gy", "gx"),
    )
    return jax.shard_map(local, mesh=mesh, in_specs=in_specs, out_specs=out_specs, check_vma=False)
```

```python
import functools

import jax
import jax.numpy as jnp
from jax import lax
from jax.experimental import pallas as pl
from jax.experimental.pallas import tpu as pltpu
from jax.sharding import PartitionSpec as P

HEAD_DIM = 72
HEAD_PAD = 80
EPSILON = 1e-06
MESH = pl.DeviceIdType.MESH
BF16 = jnp.bfloat16
F32 = jnp.float32
NN = (((1,), (0,)), ((), ()))
NT = (((1,), (1,)), ((), ()))
TN = (((0,), (0,)), ((), ()))
GELU_A = 0.044715
GELU_C = 0.7978845608028654


def mm(a, b, dims):
    return lax.dot_general(a, b, dims, preferred_element_type=F32)


def round_up(value, unit):
    return (value + unit - 1) // unit * unit


def block_kernel(
    cfg,
    len_ref,
    g1_ref,
    b1_ref,
    ob_ref,
    g2_ref,
    b2_ref,
    db_ref,
    x_ref,
    cot_ref,
    wq_in,
    wo_in,
    wu_in,
    wd_in,
    qv_ref,
    up_ref,
    out_ref,
    ig_ref,
    dq_out,
    do_out,
    du_out,
    dd_out,
    sm_out,
    prm_send,
    prm_all,
    prm_col,
    x_t,
    cot_t,
    h1_t,
    h2_t,
    gb_t,
    wq,
    wo,
    wu,
    wd,
    qkv_t,
    att_t,
    wo_n,
    gatt_t,
    act_t,
    gpre_t,
    resid,
    trecv,
    mrecv,
    grecv,
    mrelay,
    grelay,
    dqf,
    fa,
    fb,
    pk,
    rows_f,
    sums_col,
    uv_send,
    uv_recv,
    sm_send,
    sm_part,
    sm_chip,
    sm_win,
    smz_recv,
    cq,
    co,
    cu,
    cd,
    zq,
    zo,
    zu,
    zd,
    sem_s,
    sem_r,
):
    prm_refs = (g1_ref, b1_ref, ob_ref, g2_ref, b2_ref, db_ref)
    nz, zin = cfg["nz"], cfg["zin"]
    fb_rows, tok, heads = cfg["fb"], cfg["tok"], cfg["heads"]
    half, width = 4 * fb_rows, 8 * fb_rows
    tb = tok // 4
    hd = heads * HEAD_DIM
    hw, kp = cfg["hw"], cfg["kp"]
    factor = HEAD_DIM ** (-0.5)
    z, g, c = lax.axis_index("dp"), lax.axis_index("gx"), lax.axis_index("gy")
    g_hi, g_lo = g // 2, g % 2

    def gx_of(dd):
        return ((g_hi + dd // 2) % 2) * 2 + (g_lo + dd % 2) % 2

    def row_of(dc):
        return (c + dc) % 2

    counter = [0]

    def take(count):
        first = counter[0]
        counter[0] += count
        return first

    def rcopy(src, dst, sem, dev, send=None):
        return pltpu.make_async_remote_copy(
            src_ref=src,
            dst_ref=dst,
            send_sem=sem_s.at[sem if send is None else send],
            recv_sem=sem_r.at[sem],
            device_id=dev,
            device_id_type=MESH,
        )

    def lcopy(src, dst, sem):
        return pltpu.make_async_copy(src, dst, sem_r.at[sem])

    others = [(dd, dc) for dd in (1, 2, 3, 0) for dc in (0, 1) if dd or dc]
    near = [(dd, dc) for dd, dc in others if dd < 3]

    def dev(dd, dc):
        return (z, gx_of(dd), row_of(dc))

    def feat(dd, dc):
        return pl.ds(pl.multiple_of(row_of(dc) * half + gx_of(dd) * fb_rows, 16), fb_rows)

    def toks(j):
        return pl.ds(pl.multiple_of(j * tb, 128), tb)

    def row_tok(dc):
        return pl.ds(pl.multiple_of(row_of(dc) * tok, 128), tok)

    pending = []

    barrier = pltpu.get_barrier_semaphore()
    for dd, dc in others:
        pl.semaphore_signal(barrier, inc=1, device_id=dev(dd, dc), device_id_type=MESH)
    for k in range(1, nz):
        pl.semaphore_signal(barrier, inc=1, device_id=((z + k) % nz, g, c), device_id_type=MESH)
    ends = []
    total = len_ref[0, 0]
    ends.append(total)
    for s in range(1, len_ref.shape[1]):
        total = total + len_ref[0, s]
        ends.append(total)

    def pictures(pos):
        picture = jnp.zeros_like(pos)
        for end in ends:
            picture = picture + jnp.where(pos >= end, 1, 0)
        return picture

    pos_col = lax.broadcasted_iota(jnp.int32, (tok, 128), 0)
    pk[...] = jnp.where(pos_col < total, pictures(pos_col), -1)
    pos_row = lax.broadcasted_iota(jnp.int32, (8, tok), 1)
    pic_row = pictures(pos_row)
    rows_f[0, :, :] = pic_row.astype(F32)
    rows_f[1, :, :] = jnp.where(pos_row < total, 1.0, 0.0)
    sums_col[...] = jnp.zeros_like(sums_col)
    qkv_t[...] = jnp.zeros_like(qkv_t)
    gatt_t[...] = jnp.zeros_like(gatt_t)

    prm_send[...] = jnp.zeros_like(prm_send)
    for k, ref in enumerate(prm_refs):
        prm_send[k : k + 1, 0:fb_rows] = ref[...]
    sm_send[...] = jnp.zeros_like(sm_send)
    sm_send[0:1, 0 : up_ref.shape[0]] = up_ref[...].reshape(1, up_ref.shape[0])
    sm_send[1:2, 0:hd] = qv_ref[0:1, :]
    sm_send[1:2, 2 * hd : 3 * hd] = qv_ref[1:2, :]
    for n in range(0, sm_send.shape[1], 128):
        rows = jnp.concatenate([sm_send[:, n : n + 128], jnp.zeros((120, 128), F32)], axis=0)
        prm_col[n : n + 128, 8:16] = jnp.transpose(rows)[:, 0:8]
    if zin:
        rows = pl.ds(pl.multiple_of(c * half + z * fb_rows, 16), fb_rows)
        gap = jnp.zeros((fb_rows, kp - 3 * hd), BF16)
        wq[rows, :] = jnp.concatenate([wq_in[0], wq_in[1], wq_in[2], gap], axis=1)
        for src, dst in ((wo_in, wo), (wu_in, wu), (wd_in, wd)):
            gap = jnp.zeros((fb_rows, dst.shape[1] - src.shape[1]), BF16)
            dst[rows, :] = jnp.concatenate([src[...], gap], axis=1)
    pl.semaphore_wait(barrier, 7 + nz - 1)

    own_feat = feat(0, 0)
    own_t = toks(g)
    partner = (z, g, 1 - c)
    me = c * 4 + g
    th = tok // 2

    def exchange(first, src, dst):
        for dd, dc in others:
            rcopy(src, dst, first + dd * 2 + dc, dev(dd, dc)).start()
            pending.append(lambda dd=dd, dc=dc: rcopy(src, dst, first + dd * 2 + dc, dev(dd, dc)).wait_send())

    passing = ((0, 1, 0), (1, 2, 1))

    def gather_copy(first, src, dst, n, size, dd, dc):
        tokens = pl.ds(pl.multiple_of(row_of(dc) * tok + n * size, 128), size)
        part = dst.at[own_feat, n * size : (n + 1) * size]
        return rcopy(src.at[:, tokens], part, first + n * 8 + dd * 2 + dc, dev(dd, dc))

    def gather_land(first, dst, n, size, dd, dc, sem):
        part = dst.at[feat(dd, dc), n * size : (n + 1) * size]
        return rcopy(part, part, first + n * 8 + sem, partner)

    def gather_pass(first, dst, n, size, k, dd, dc):
        part = dst.at[feat(dd, dc), n * size : (n + 1) * size]
        return rcopy(part, part, first + n * 8 + 6 + k, dev(3 - dd, 0))

    def gather_own(first, src, dst, n, size):
        tokens = pl.ds(pl.multiple_of(row_of(0) * tok + n * size, 128), size)
        return lcopy(src.at[:, tokens], dst.at[own_feat, n * size : (n + 1) * size], first + n * 8)

    def gather_start(first, src, dst, n, size):
        for dd, dc in near:
            gather_copy(first, src, dst, n, size, dd, dc).start()
        gather_own(first, src, dst, n, size).start()

    def gather_relay(first, dst, n, size):
        for k, dd, dc in passing:
            gather_land(first, dst, n, size, dd, dc, dd * 2 + dc).wait_recv()
            gather_pass(first, dst, n, size, k, dd, dc).start()

    def gather_done(first, src, dst, n, size):
        gather_own(first, src, dst, n, size).wait()
        for dd, dc in ((0, 1), (1, 1), (2, 0)):
            gather_land(first, dst, n, size, dd, dc, dd * 2 + dc).wait_recv()
        for k in (0, 1):
            gather_land(first, dst, n, size, 3, k, 6 + k).wait_recv()

    def gather_sent(first, src, dst, n, size):
        for dd, dc in near:
            gather_copy(first, src, dst, n, size, dd, dc).wait_send()
        for k, dd, dc in passing:
            gather_pass(first, dst, n, size, k, dd, dc).wait_send()

    q_cuts = (0, 256, 512, kp)
    weights = tuple(wq.at[:, q_cuts[p] : q_cuts[p + 1]] for p in range(3)) + (wo, wu, wd)
    inputs = (wq_in, None, None, wo_in, wu_in, wd_in)
    whole = (wq, wq, wq, wo, wu, wd)
    n_w = len(weights)
    steps = nz - 1
    nw = nz if zin else 1
    wz0 = take((n_w + 2) * nw)
    wc0 = take(4 * nw)

    def zrows(zz, core):
        return pl.ds(pl.multiple_of(core * half + zz * fb_rows, 16), fb_rows)

    def w_rows(i, zz, core):
        return weights[i].at[zrows(zz, core), :]

    def whole_rows(i, zz, core):
        return whole[i].at[zrows(zz, core), :]

    def hop(i, s, d):
        origin = z - (s - 1) if d == 0 else z + (s - 1)
        here = jnp.logical_and(z >= s - 1, z < nz - 1) if d == 0 else jnp.logical_and(z < nz - s + 1, z > 0)
        to = z + 1 if d == 0 else z - 1
        send = wz0 + n_w * nw + i if s == 1 and d == 1 else None
        return here, lambda: rcopy(w_rows(i, origin, c), w_rows(i, origin, c), wz0 + i * nw + origin, (to, g, c), send)

    def arrival(s, d):
        return (z >= s, z - s) if d == 0 else (z < nz - s, z + s)

    def pass_on(i, zz):
        first = max(i - 2, 0)
        return rcopy(whole_rows(i, zz, c), whole_rows(i, zz, c), wc0 + first * nw + zz, partner)

    def z_send(i, s):
        if not zin:
            if s == 1 and inputs[i] is not None:
                lcopy(inputs[i], whole[i], wz0 + i * nw).start()
            return
        for d in (0, 1):
            here, make = hop(i, s, d)
            pl.when(here)(lambda make=make: make().start())
        if s == 1 and i >= 2:
            pass_on(i, z).start()

    def z_recv(i, s):
        if not zin:
            return
        for d in (0, 1):
            here, origin = arrival(s, d)

            @pl.when(here)
            def _(s=s, d=d, origin=origin):
                rows = w_rows(i, origin, c)
                rcopy(rows, rows, wz0 + i * nw + origin, partner).wait_recv()
                if i >= 2:
                    pass_on(i, origin).start()

        if s < steps:
            z_send(i, s + 1)

    def weight_ready(i):
        if not zin:
            if inputs[i] is not None:
                lcopy(inputs[i], whole[i], wz0 + i * nw).wait()
            return
        if i >= 2:
            for zz in range(nz):
                rows = whole_rows(i, zz, 1 - c)
                rcopy(rows, rows, wc0 + (i - 2) * nw + zz, partner).wait_recv()

    def weight_passed(i):
        if not zin:
            return
        for s in range(1, nz):
            for d in (0, 1):
                here, make = hop(i, s, d)
                pl.when(here)(lambda make=make: make().wait_send())
        if i >= 2:
            for zz in range(nz):
                pass_on(i, zz).wait_send()

    p0 = take(8)
    xs0 = take(16)
    cs0 = take(32)
    exchange(p0, prm_send, prm_all.at[me])
    lcopy(prm_send, prm_all.at[me], p0).start()
    for n in (0, 1):
        gather_start(xs0, x_ref, x_t, n, th)
    for i in (0, 1, 2):
        z_send(i, 1)

    def par(k):
        return prm_col[:, k : k + 1]

    def z_recv_all(pairs):
        for i, step in pairs:
            if step < nz:
                z_recv(i, step)

    wn0 = take(8)

    def wo_part(gx, core, first=0, last=None):
        rows = (fb_rows if last is None else last) - first
        return wo_n.at[pl.ds(pl.multiple_of(gx * hd + core * fb_rows + first, 16), rows), :]

    cut = fb_rows // 32 * 16 + 16

    def wo_copy(n):
        if n < 2:
            own = wo_part(g, c)
            return rcopy(own, own, wn0 + n + 1, (z, gx_of(n + 1), c))
        if n < 4:
            got = wo_part(gx_of(n - 1), c)
            return rcopy(got, got, wn0 + n + 1, partner)
        if n < 6:
            on = wo_part(gx_of(1), c, 0, cut) if n == 4 else wo_part(gx_of(2), c, cut)
            return rcopy(on, on, wn0 + n + 1, (z, gx_of(6 - n), c))
        far = wo_part(gx_of(3), c)
        return rcopy(far, far, wn0 + 7, partner)

    def wo_first():
        turned = jnp.transpose(wo[...])
        wo_n[pl.ds(pl.multiple_of(g * hd, 16), hd), :] = turned[0:hd, :]
        for n in (0, 1):
            wo_copy(n).start()

    def wo_second():
        for step in (1, 2):
            got = wo_part(gx_of(step), c)
            rcopy(got, got, wn0 + step, partner).wait_recv()
        for n in (4, 5, 2, 3):
            wo_copy(n).start()

    def wo_third():
        for step, on in ((1, wo_part(gx_of(3), c, 0, cut)), (2, wo_part(gx_of(3), c, cut))):
            rcopy(on, on, wn0 + 4 + step, partner).wait_recv()
        wo_copy(6).start()

    def wo_ready():
        for step in (1, 2):
            got = wo_part(gx_of(step), 1 - c)
            rcopy(got, got, wn0 + 2 + step, partner).wait_recv()
        far = wo_part(gx_of(3), 1 - c)
        rcopy(far, far, wn0 + 7, partner).wait_recv()

    def head_rows(part, h):
        return pl.ds(pl.multiple_of((part * heads + h) * HEAD_PAD, 16), HEAD_PAD)

    def project(j, carry):
        t = toks(j)
        x = x_t[:, t].astype(F32)
        m = jnp.sum(x, axis=0, keepdims=True) * (1.0 / width)
        q = jnp.sum(x * x, axis=0, keepdims=True) * (1.0 / width)
        r = lax.rsqrt(q - m * m + EPSILON)
        rows_f[2, 0:1, t] = m
        rows_f[3, 0:1, t] = r
        h1_t[:, t] = ((x - m) * r * par(0) + par(1)).astype(BF16)
        part = mm(wq[...], h1_t[:, t], TN) + prm_col[0:kp, 9:10]
        for p in range(3):
            for h in range(heads):
                first, row = (p * heads + h) * HEAD_PAD, p * hd + h * HEAD_DIM
                qkv_t[first : first + HEAD_DIM, t] = part[row : row + HEAD_DIM, :].astype(BF16)
        return carry

    z_recv_all(((0, 1), (1, 1), (2, 1)))
    z_send(3, 1)
    gather_relay(xs0, x_t, 0, th)
    z_recv_all(((0, 2), (1, 2)))
    gather_relay(xs0, x_t, 1, th)
    z_recv_all(((2, 2), (3, 1)))

    lcopy(prm_send, prm_all.at[me], p0).wait()
    for dd, dc in others:
        rcopy(prm_send, prm_all.at[row_of(dc) * 4 + gx_of(dd)], p0 + dd * 2 + dc, partner).wait_recv()
    for b in range(8):
        rows = jnp.concatenate([prm_all[b], jnp.zeros((120, 256), F32)], axis=0)
        prm_col[b * fb_rows : (b + 1) * fb_rows, 0:8] = jnp.transpose(rows)[:fb_rows, 0:8]

    for step in range(3, nz):
        z_recv_all((i, step) for i in range(3))
    for i in range(3):
        weight_ready(i)
    gather_done(xs0, x_ref, x_t, 0, th)
    for n in (0, 1):
        gather_start(cs0, cot_ref, cot_t, n, tb)
    lax.fori_loop(0, 2, project, 0)
    z_recv_all(((3, 2),))
    z_send(4, 1)
    gather_done(xs0, x_ref, x_t, 1, th)
    lax.fori_loop(2, 4, project, 0)
    z_recv_all((3, step) for step in range(3, nz))
    weight_ready(3)
    wo_first()

    def kept_of(h, t):
        scores = mm(qkv_t[head_rows(1, h), :], qkv_t[head_rows(0, h), t], TN) * factor
        key_pic = pk[...]
        query_pic = rows_f[0, 0:1, t].astype(jnp.int32)
        allowed = jnp.concatenate([key_pic] * (tb // 128), axis=1) == query_pic
        return jnp.where(allowed, jnp.exp(scores), 0.0)

    at0 = take(4 * 3)
    own_heads = pl.ds(pl.multiple_of(g * hd, 16), hd)

    def att_piece(dd, j):
        return att_t.at[pl.ds(pl.multiple_of(gx_of(dd) * hd, 16), hd), toks(j)]

    def att_send(j, start):
        for step in (1, 2):
            piece = att_piece(0, j)
            cp = rcopy(piece, piece, at0 + j * 3 + step - 1, (z, gx_of(step), c))
            cp.start() if start else cp.wait_send()

    def att_relay(j):
        for step in (1, 2):
            piece = att_piece(step, j)
            rcopy(piece, piece, at0 + j * 3 + step - 1, partner).wait_recv()
        step = 1 + j % 2
        piece = att_piece(step, j)
        rcopy(piece, piece, at0 + j * 3 + 2, (z, gx_of(3 - step), c)).start()

    def att_relayed(j):
        piece = att_piece(1 + j % 2, j)
        rcopy(piece, piece, at0 + j * 3 + 2, partner).wait_send()

    def attend(j, carry):
        t = toks(j)

        def head(h, inner):
            kept = kept_of(h, t)
            den = jnp.sum(kept, axis=0, keepdims=True)
            den = jnp.where(rows_f[1, 0:1, t] > 0.5, den, 1.0)
            scale = jnp.where(den > 1e30, 2.0**-40, 1.0)
            inv = 1.0 / (den * scale)
            rows_f[4 + 2 * h, 0:1, t] = scale
            rows_f[5 + 2 * h, 0:1, t] = inv
            probs = (kept * scale * inv).astype(BF16)
            att = mm(qkv_t[head_rows(2, h), :], probs, NN)
            dqf[pl.ds(pl.multiple_of(h * HEAD_DIM, 8), HEAD_DIM), :] = att[0:HEAD_DIM, :]
            return inner

        lax.fori_loop(0, heads, head, 0)
        att_t[own_heads, t] = dqf[...].astype(BF16)

        att_send(j, True)

        @pl.when(j == 0)
        def _():
            z_recv_all(((4, 1),))
            z_send(5, 1)

        @pl.when(j == 1)
        def _():
            wo_second()

        @pl.when(j == 2)
        def _():
            att_relay(0)
            z_recv_all(((4, 2),))

        return carry

    lax.fori_loop(0, 4, attend, 0)
    att_relay(1)
    wo_third()
    z_recv_all(((5, 1),))
    att_relay(2)

    def project_out(j, carry):
        t = toks(j)

        @pl.when(j == 0)
        def _():
            wo_ready()

        far = att_piece(3, j)
        rcopy(far, far, at0 + j * 3 + 2, partner).wait_recv()
        residual = mm(wo_n[...], att_t[:, t], TN) + x_t[:, t].astype(F32) + par(2)
        m2 = jnp.sum(residual, axis=0, keepdims=True) * (1.0 / width)
        q2 = jnp.sum(residual * residual, axis=0, keepdims=True) * (1.0 / width)
        r2 = lax.rsqrt(q2 - m2 * m2 + EPSILON)
        rows_f[2, 1:2, t] = m2
        rows_f[3, 1:2, t] = r2
        h2_t[:, t] = ((residual - m2) * r2 * par(3) + par(4)).astype(BF16)

        @pl.when(j == g)
        def _():
            resid[...] = residual

        @pl.when(j == 0)
        def _():
            att_relay(3)
            for n in (2, 3):
                gather_start(cs0, cot_ref, cot_t, n, tb)
            for n in (0, 1):
                gather_relay(cs0, cot_t, n, tb)

        @pl.when(j == 1)
        def _():
            z_recv_all((4, step) for step in range(3, nz))

        @pl.when(j == 2)
        def _():
            z_recv_all(((5, 2),))

        return carry

    lax.fori_loop(0, 4, project_out, 0)
    weight_ready(4)
    for n in range(7):
        wo_copy(n).wait_send()

    def spread(first, buf):
        for step in (1, 2):
            rcopy(buf.at[:, own_t], buf.at[:, own_t], first + step, (z, gx_of(step), c)).start()

    def halves(buf, step, k):
        return buf.at[(k - 1) * half : k * half, toks(gx_of(step))]

    def spread_relay(first, buf):
        for step in (1, 2):
            block = buf.at[:, toks(gx_of(step))]
            rcopy(block, block, first + step, partner).wait_recv()
            part = halves(buf, step, step)
            rcopy(part, part, first + 2 + step, (z, gx_of(3 - step), c)).start()

    def spread_done(first, buf):
        for k in (1, 2):
            part = halves(buf, 3, k)
            rcopy(part, part, first + 2 + k, partner).wait_recv()

    def spread_sent(first, buf):
        for step in (1, 2):
            rcopy(buf.at[:, own_t], buf.at[:, own_t], first + step, partner).wait_send()
            part = halves(buf, step, step)
            rcopy(part, part, first + 2 + step, partner).wait_send()

    def mlp_up(i, carry):
        t = toks(i)
        fa[...] = mm(wu[...], h2_t[:, t], TN) + prm_col[:, 8:9]

        def chunk(n, inner):
            rows = pl.ds(pl.multiple_of(n * 48, 16), 48)
            v = fa[rows, :]
            v2 = v * v
            thv = jnp.tanh(GELU_C * (v + GELU_A * v2 * v))
            hf = 0.5 * (1.0 + thv)
            act_t[rows, t] = (v * hf).astype(BF16)
            slope = hf + (0.5 * GELU_C) * v * (1.0 - thv * thv) * (1.0 + (3.0 * GELU_A) * v2)
            gpre_t[rows, t] = slope.astype(BF16)
            return inner

        lax.fori_loop(0, fa.shape[0] // 48, chunk, 0)

        @pl.when(i == 1)
        def _():
            for n in (2, 3):
                gather_relay(cs0, cot_t, n, tb)

        return carry

    lax.fori_loop(0, 4, mlp_up, 0)
    for n in range(4):
        gather_done(cs0, cot_ref, cot_t, n, tb)
    z_recv_all((5, step) for step in range(3, nz))
    weight_ready(5)

    for n in (0, 1):
        gather_sent(xs0, x_ref, x_t, n, th)
    g20 = xs0

    def tsend(step):
        return wo_n.at[:, (step - 1) * tb : step * tb]

    def g2_copy(n):
        top, bottom = slice(0, half), slice(half, width)
        rows = (top, bottom, top, bottom, bottom, top)[n]
        step = (3, 3, 1, 1, 2, 2)[n]
        slot = (2, 2, 0, 0, 1, 1)[n]
        to = (1, 2, 1, 1, 2, 2)[n]
        src = wo_n.at[rows, (step - 1) * tb : step * tb]
        return rcopy(src, trecv.at[slot, rows, :], g20 + n, (z, gx_of(to), c))

    def mlp_back(i, carry):
        t = toks(gx_of(3 - i))
        gpre_t[:, t] = (mm(wd[...], cot_t[:, t], TN) * gpre_t[:, t].astype(F32)).astype(BF16)
        fa[...] = mm(wu[...], gpre_t[:, t], NN)
        for step, sends in ((3, (0, 1)), (2, (4,)), (1, (2,))):

            @pl.when(i == 3 - step)
            def _(step=step, sends=sends):
                tsend(step)[...] = fa[...].astype(BF16)
                for n in sends:
                    g2_copy(n).start()

        return carry

    lax.fori_loop(0, 4, mlp_back, 0)
    for n, step, rows, then in ((0, 2, slice(0, half), 5), (1, 1, slice(half, width), 3)):
        g2_copy(n).wait_recv()
        cols = slice((step - 1) * tb, step * tb)
        wo_n[rows, cols] = (wo_n[rows, cols].astype(F32) + trecv[2, rows, :].astype(F32)).astype(BF16)
        g2_copy(then).start()

    dwc0 = take(4)
    dwz0 = take(4 * 6)
    do0 = take(4)
    gath = ((0, 1, 2), (3,), (4,), (5,))
    core_recv = (cq, co, cu, cd)
    z_recvs = (zq, zo, zu, zd)
    dw_refs = (wo_n, wo, wu, wd)
    dw_cols = (kp, wo.shape[1], wu.shape[1], wd.shape[1])
    dw_outs = (dq_out, do_out, du_out, dd_out)
    slots = [0]
    leaving = []

    def weight_grad(i, left, right):
        for n in gath[i]:
            weight_passed(n)
        dst, cols = dw_refs[i], dw_cols[i]
        step_cols = 384

        def one(n, carry):
            cs = pl.ds(pl.multiple_of(n * step_cols, 128), step_cols)
            dst[:, cs] = mm(left[...], right[pl.ds(pl.multiple_of(n * step_cols, 16), step_cols), :], NT).astype(BF16)
            return carry

        lax.fori_loop(0, cols // step_cols, one, 0)
        rest = cols // step_cols * step_cols
        if rest < cols:
            dst[:, rest:cols] = mm(left[...], right[rest:cols, :], NT).astype(BF16)

    def core_half(i, core):
        return dw_refs[i].at[pl.ds(pl.multiple_of(core * half, 16), half), 0 : dw_cols[i]]

    def send_core(i):
        if zin:
            rcopy(core_half(i, 1 - c), core_recv[i], dwc0 + i, partner).start()
            pending.append(lambda: rcopy(core_half(i, 1 - c), core_recv[i], dwc0 + i, partner).wait_send())
        else:
            lcopy(dw_refs[i].at[:, 0 : dw_cols[i]], dw_outs[i], dwc0 + i).start()

    def sum_core(i):
        if not zin:
            return
        rcopy(core_half(i, c), core_recv[i], dwc0 + i, partner).wait_recv()
        w = dw_refs[i]
        for zz in range(nz):
            rows = pl.ds(pl.multiple_of(c * half + zz * fb_rows, 16), fb_rows)
            cols = dw_cols[i]
            w[rows, 0:cols] = (
                w[rows, 0:cols].astype(F32) + core_recv[i][zz * fb_rows : (zz + 1) * fb_rows, :].astype(F32)
            ).astype(BF16)

        @pl.when(leaf)
        def _():
            for slot, zz in enumerate((far_end, far_inner, inner)):
                if i or slot < 2:
                    z_piece(i, slot, zz, slot, inner).start()

        @pl.when(jnp.logical_not(leaf))
        def _():
            z_piece(i, 3, end, 0, end).start()

    leaf = z % 3 == 0
    low = z < 2
    end, inner = jnp.where(low, 0, 3), jnp.where(low, 1, 2)
    far_end, far_inner = 3 - end, 3 - inner

    def z_piece(i, sem, zz, slot, to):
        rows = dw_refs[i].at[zrows(zz, c), 0 : dw_cols[i]]
        return rcopy(rows, z_recvs[i].at[slot], dwz0 + i * 6 + sem, (to, g, c))

    def z_land(i, slot):
        rows = dw_refs[i].at[zrows(z, c), 0 : dw_cols[i]]
        return rcopy(rows, z_recvs[i].at[min(slot, 3) if slot != 3 else 0], dwz0 + i * 6 + slot, partner)

    def relay_z(i, slot):
        if not zin:
            return

        @pl.when(jnp.logical_not(leaf))
        def _():
            z_land(i, slot).wait_recv()
            zz = far_end if slot == 0 else far_inner
            w, cols = dw_refs[i], dw_cols[i]
            rows = zrows(zz, c)
            w[rows, 0:cols] = (w[rows, 0:cols].astype(F32) + z_recvs[i][slot].astype(F32)).astype(BF16)
            z_piece(i, 4 + slot, zz, 3, zz).start()

    def z_sent(i):
        if not zin:
            return

        @pl.when(leaf)
        def _():
            for slot, zz in enumerate((far_end, far_inner, inner)):
                z_piece(i, slot, zz, slot, inner).wait_send()

        @pl.when(jnp.logical_not(leaf))
        def _():
            z_piece(i, 3, end, 0, end).wait_send()
            z_piece(i, 4, far_end, 3, far_end).wait_send()
            z_piece(i, 5, far_inner, 3, far_inner).wait_send()

    def sum_z(i):
        if not zin:
            lcopy(dw_refs[i].at[:, 0 : dw_cols[i]], dw_outs[i], dwc0 + i).wait()
            return

        @pl.when(leaf)
        def _():
            z_land(i, 3).wait_recv()
            z_land(i, 4).wait_recv()

        @pl.when(jnp.logical_not(leaf))
        def _():
            z_land(i, 2).wait_recv()
            z_land(i, 5).wait_recv()

        near_slot = jnp.where(leaf, 0, 2)
        cols = dw_cols[i]

        def total_of(n, size):
            part = dw_refs[i][zrows(z, c), n : n + size].astype(F32)
            return part + z_recvs[i][near_slot, :, n : n + size].astype(F32) + z_recvs[i][3, :, n : n + size].astype(F32)

        if i == 0:
            whole = total_of(0, cols)
            gap = jnp.zeros((fb_rows, hw - hd), F32)
            pieces = []
            for p in range(3):
                part = jnp.concatenate([whole[:, p * hd : (p + 1) * hd], gap], axis=1)
                for n in range(0, hw, tb):
                    size = min(tb, hw - n)
                    pieces.append((part[:, n : n + size], dq_out.at[p, :, n : n + size]))
        else:
            pieces = []
            for n in range(0, cols, tb):
                size = min(tb, cols - n)
                pieces.append((total_of(n, size), dw_outs[i].at[:, n : n + size]))
        for part, goes in pieces:
            size = part.shape[1]
            slot = slots[0] % 16
            if slots[0] >= 4:
                leaving[slots[0] - 4].wait()
            slots[0] += 1
            stage = (fa, fb)[slot // 8].at[(slot % 8) * fb_rows : (slot % 8 + 1) * fb_rows, 0:size]
            stage[...] = part
            cp = lcopy(stage, goes, do0 + slot % 4)
            cp.start()
            leaving.append(cp)

    ml0, gh0, uv0, sm0 = cs0, xs0, at0, p0
    for n in range(4):
        gather_sent(cs0, cot_ref, cot_t, n, tb)
    for j in range(4):
        att_send(j, False)
        att_relayed(j)
    for wait in pending:
        wait()
    pending.clear()
    sz0 = take(nz)

    direct, added = ((1, 0), (2, 1), (0, 1)), ((1, 1), (2, 0))

    def hand(buf, relay, first, j, n):
        part = relay.at[n, :, toks(j)]
        return rcopy(buf.at[feat(3, n), toks(j)], part, first + 8 + j * 2 + n, (z, gx_of(n + 1), c))

    def block_copy(buf, recv, first, dd, dc):
        slot = dd * 2 + dc
        return rcopy(buf.at[feat(dd, dc), :], recv.at[slot], first + slot, dev(dd, dc))

    def add_relayed(buf, relay, recv, first):
        for n, (dd, dc) in ((0, (2, 0)), (1, (1, 1))):
            for j in range(4):
                hand(buf, relay, first, j, n).wait_recv()
            rows = feat(dd, dc)
            buf[rows, :] = (buf[rows, :].astype(F32) + relay[n].astype(F32)).astype(BF16)
            block_copy(buf, recv, first, dd, dc).start()

    def scatter_sent(buf, relay, recv, first):
        for dd, dc in direct + added:
            block_copy(buf, recv, first, dd, dc).wait_send()
        for n in (0, 1):
            for j in range(4):
                hand(buf, relay, first, j, n).wait_send()

    def scatter_start(buf, recv, first):
        for dd, dc in direct:
            block_copy(buf, recv, first, dd, dc).start()
        lcopy(buf.at[own_feat, :], recv.at[0], first).start()

    def scatter_sum(buf, recv, first, dc):
        if dc == 0:
            lcopy(buf.at[own_feat, :], recv.at[0], first).wait()
        acc = 0.0
        for dd in (0, 1, 2):
            if dd or dc:
                block_copy(buf, recv, first, dd, dc).wait_recv()
            acc = acc + recv[dd * 2 + dc].astype(F32)
        return acc

    weight_grad(2, h2_t, gpre_t)
    send_core(2)
    ones = jnp.ones((tok, 128), BF16)
    sums_col[0 : act_t.shape[0], 6:7] = mm(gpre_t[...], ones, NN)[:, 0:1]
    sum_core(2)


    def lower(j, carry):
        t = toks(j)
        h2_t[:, t] = mm(wd[...], act_t[:, t], NN).astype(BF16)
        return carry

    lax.fori_loop(0, 4, lower, 0)
    h2_t[:, own_t] = (mm(wd[...], act_t[:, own_t], NN) + resid[...] + par(5)).astype(BF16)

    for n in (2, 3, 4, 5):
        g2_copy(n).wait_recv()
    gh2 = fa[...] + trecv[0].astype(F32) + trecv[1].astype(F32)
    m2 = rows_f[2, 1:2, own_t]
    r2 = rows_f[3, 1:2, own_t]
    normed2 = (resid[...] - m2) * r2
    gn = gh2 * par(3)
    s1 = jnp.sum(gn, axis=0, keepdims=True) * (1.0 / width)
    s2 = jnp.sum(gn * normed2, axis=0, keepdims=True) * (1.0 / width)
    cot_own = cot_t[:, own_t].astype(F32)
    g_res = cot_own + r2 * (gn - s1 - normed2 * s2)
    g_low = g_res.astype(BF16)
    gb_t[:, own_t] = g_low
    gb0 = wn0
    spread(gb0, gb_t)
    resid[...] = g_res
    sums_col[0:width, 2:3] = jnp.sum(g_low.astype(F32), axis=1, keepdims=True)
    sums_col[0:width, 3:4] = jnp.sum(gh2 * normed2, axis=1, keepdims=True)
    sums_col[0:width, 4:5] = jnp.sum(gh2, axis=1, keepdims=True)
    sums_col[0:width, 5:6] = jnp.sum(cot_own, axis=1, keepdims=True)
    for n in range(6):
        g2_copy(n).wait_send()
    weight_grad(3, cot_t, act_t)
    send_core(3)
    relay_z(2, 0)
    sum_core(3)

    fa[...] = jnp.zeros_like(fa)
    fb[...] = jnp.zeros_like(fb)
    act_t[3 * hd : kp, :] = jnp.zeros((kp - 3 * hd, tok), BF16)

    def attend_back(i, carry):
        t = toks(gx_of(i))

        @pl.when(i == 1)
        def _():
            spread_relay(gb0, gb_t)
            relay_z(2, 1)
            for n in (0, 1):
                for k in range(4):
                    hand(h2_t, mrelay, ml0, k, n).start()
            scatter_start(h2_t, mrecv, ml0)

        @pl.when(i == 3)
        def _():
            spread_done(gb0, gb_t)
            relay_z(3, 0)

        gatt = mm(wo[...], gb_t[:, t], TN)
        for h in range(heads):
            gatt_t[h * HEAD_PAD : h * HEAD_PAD + HEAD_DIM, :] = gatt[h * HEAD_DIM : (h + 1) * HEAD_DIM, :].astype(BF16)

        @pl.when(i == 3)
        def _():
            weight_passed(3)
            wo[:, 0:hd] = mm(gb_t[...], att_t[own_heads, :], NT).astype(BF16)
            send_core(1)
            add_relayed(h2_t, mrelay, mrecv, ml0)

        def head(h, inner):
            kept = kept_of(h, t)
            probs = kept * rows_f[4 + 2 * h, 0:1, t] * rows_f[5 + 2 * h, 0:1, t]
            q_rows = head_rows(0, h)
            grad = gatt_t[q_rows, :]
            grad_probs = mm(qkv_t[head_rows(2, h), :], grad, TN)
            weighted = probs * grad_probs
            delta = jnp.sum(weighted, axis=0, keepdims=True)
            grad_scores = (weighted - probs * delta).astype(BF16)
            dq = mm(qkv_t[head_rows(1, h), :], grad_scores, NN) * factor
            dqf[pl.ds(pl.multiple_of(h * HEAD_DIM, 8), HEAD_DIM), :] = dq[0:HEAD_DIM, :]
            dk = mm(qkv_t[q_rows, t], grad_scores, NT)
            dv = mm(grad, probs.astype(BF16), NT)
            for kb in range(4):
                rows = pl.ds(pl.multiple_of(kb * hd + h * HEAD_DIM, 8), HEAD_DIM)
                fa[rows, :] += dk[0:HEAD_DIM, kb * tb : (kb + 1) * tb]
                fb[rows, :] += dv[0:HEAD_DIM, kb * tb : (kb + 1) * tb]
            return inner

        lax.fori_loop(0, heads, head, 0)
        act_t[0:hd, t] = dqf[...].astype(BF16)
        return carry

    lax.fori_loop(0, 4, attend_back, 0)

    for kb in range(4):
        cols, rows = slice(kb * tb, (kb + 1) * tb), slice(kb * hd, (kb + 1) * hd)
        act_t[hd : 2 * hd, cols] = (fa[rows, :] * factor).astype(BF16)
        act_t[2 * hd : 3 * hd, cols] = fb[rows, :].astype(BF16)
    relay_z(3, 1)
    weight_grad(0, h1_t, act_t)
    send_core(0)
    sum_core(1)

    def back1(j, carry):
        t = toks(j)
        gh1 = mm(wq[...], act_t[0:kp, t], NN)
        m = rows_f[2, 0:1, t]
        r = rows_f[3, 0:1, t]
        normed = (x_t[:, t].astype(F32) - m) * r
        gn1 = gh1 * par(0)
        prod = gh1 * normed
        sums_col[0:width, 0:1] += jnp.sum(prod, axis=1, keepdims=True)
        sums_col[0:width, 1:2] += jnp.sum(gh1, axis=1, keepdims=True)
        a1 = jnp.sum(gn1, axis=0, keepdims=True) * (1.0 / width)
        a2 = jnp.sum(gn1 * normed, axis=0, keepdims=True) * (1.0 / width)
        v = r * r * a2
        u = r * a1 - m * v
        for n in range(tb // 128):
            row = j * (tb // 128) + n
            uv_send[pl.ds(row, 1), :] = u[:, n * 128 : (n + 1) * 128]
            uv_send[pl.ds(tok // 128 + row, 1), :] = v[:, n * 128 : (n + 1) * 128]
        fa[...] = r * gn1

        @pl.when(j == g)
        def _():
            fa[...] += resid[...]

        cot_t[:, t] = fa[...].astype(BF16)
        for n in (0, 1):
            hand(cot_t, grelay, gh0, j, n).start()

        @pl.when(j == 0)
        def _():
            sum_core(0)

        return carry

    lax.fori_loop(0, 4, back1, 0)
    relay_z(1, 0)
    relay_z(1, 1)

    sums_col[0:kp, 7:8] = mm(act_t[0:kp, :], ones, NN)[:, 0:1]

    for n in range(0, sm_send.shape[1], 128):
        sm_send[:, n : n + 128] = jnp.transpose(sums_col[n : n + 128, :])[0:8, :]
    exchange(uv0, uv_send, uv_recv.at[me])
    lcopy(uv_send, uv_recv.at[me], uv0).start()
    rcopy(sm_send, sm_part, sm0 + 1, partner).start()
    rcopy(sm_send, sm_part, sm0 + 1, partner).wait_recv()
    sm_chip[...] = sm_send[...] + sm_part[...]
    win = sm_win.shape[2]

    def window(dd):
        first = (c * half + gx_of(dd) * fb_rows) // 128 * 128
        return pl.ds(pl.multiple_of(jnp.minimum(first, sm_chip.shape[1] - win), 128), win)

    def window_copy(dd):
        return rcopy(sm_chip.at[:, window(dd)], sm_win.at[dd], sm0 + dd * 2, (z, gx_of(dd), c))

    for dd in (1, 2, 3):
        window_copy(dd).start()
    scatter_start(cot_t, grecv, gh0)
    add_relayed(cot_t, grelay, grecv, gh0)
    relay_z(0, 0)

    for dc in (0, 1):
        out_ref[:, row_tok(dc)] = scatter_sum(h2_t, mrecv, ml0, dc).astype(BF16)

    sum_z(2)
    sum_z(3)
    relay_z(0, 1)

    total_sm = sm_chip[:, window(0)]
    for dd in (1, 2, 3):
        window_copy(dd).wait_recv()
        total_sm = total_sm + sm_win[dd]
    smz_recv[0, 0:8, :] = total_sm
    for n in range(6):
        smz_recv[0, 8 + n : 9 + n, :] = sm_chip[6 + n // 3 : 7 + n // 3, n % 3 * win : (n % 3 + 1) * win]
    for k in range(1, nz):

        def make(k=k):
            return rcopy(smz_recv.at[0], smz_recv.at[k], sz0 + k, ((z + k) % nz, g, c))

        make().start()
        pending.append(lambda make=make: make().wait_send())

    if zin:

        @pl.when(leaf)
        def _():
            z_piece(0, 2, inner, 2, inner).start()

    sum_z(1)

    lcopy(uv_send, uv_recv.at[me], uv0).wait()
    for dd, dc in others:
        rcopy(uv_send, uv_recv.at[row_of(dc) * 4 + gx_of(dd)], uv0 + dd * 2 + dc, partner).wait_recv()
    for dc in (0, 1):
        acc = scatter_sum(cot_t, grecv, gh0, dc)
        uv = uv_recv[row_of(dc) * 4 + g]
        for dd in (1, 2, 3):
            uv = uv + uv_recv[row_of(dc) * 4 + gx_of(dd)]
        n_rows = tok // 128
        u_row = jnp.concatenate([uv[n : n + 1, :] for n in range(n_rows)], axis=1)
        v_row = jnp.concatenate([uv[n_rows + n : n_rows + n + 1, :] for n in range(n_rows)], axis=1)
        x_own = x_ref[:, row_tok(dc)].astype(F32)
        ig_ref[:, row_tok(dc)] = acc - u_row - x_own * v_row

    sum_z(0)
    total_z = smz_recv[0]
    for k in range(1, nz):
        rcopy(smz_recv.at[0], smz_recv.at[k], sz0 + k, partner).wait_recv()
        total_z = total_z + smz_recv[k]
    sm_out[...] = total_z

    for cp in leaving[-4:]:
        cp.wait()
    rcopy(sm_send, sm_part, sm0 + 1, partner).wait_send()
    for dd in (1, 2, 3):
        window_copy(dd).wait_send()
    for wait in pending:
        wait()
    scatter_sent(h2_t, mrelay, mrecv, ml0)
    scatter_sent(cot_t, grelay, grecv, gh0)
    for i in range(4):
        z_sent(i)
    spread_sent(gb0, gb_t)


def finish_kernel(cfg, out_in, ig_in, sm_in, *refs):
    fb_rows, hd, n_dw = cfg["fb"], cfg["hd"], cfg["n_dw"]
    dw_in, (out_ref, ig_ref, *small), dw_ref = refs[:n_dw], refs[n_dw : n_dw + 10], refs[n_dw + 10 :]
    out_ref[...] = out_in[...]
    ig_ref[...] = ig_in[...]
    sums = sm_in[...]
    win = sums.shape[1]
    mine = lax.axis_index("gy") * (4 * fb_rows) + lax.axis_index("gx") * fb_rows
    first = jnp.minimum(mine // 128 * 128, 2 * win)
    turned = pltpu.roll(sums[0:8, :], (win - (mine - first)) % win, 1)
    for k in range(6):
        small[k][...] = turned[k : k + 1, 0:fb_rows]
    up_row, qkv_row = (jnp.concatenate([sums[r + n : r + n + 1, :] for n in range(3)], axis=1) for r in (8, 11))
    small[6][0:1, :] = qkv_row[:, 0:hd]
    small[6][1:2, :] = qkv_row[:, 2 * hd : 3 * hd]
    small[7][...] = up_row[:, 0 : small[7].shape[0]].reshape(small[7].shape[0])
    for src, dst in zip(dw_in, dw_ref):
        dst[...] = src[:, :, 0 : dst.shape[2]] if len(dst.shape) == 3 else src[:, 0 : dst.shape[1]]


def local(
    block_input,
    lengths,
    ln1_gain,
    ln1_bias,
    w_qkv,
    qv_bias,
    w_out,
    out_bias,
    ln2_gain,
    ln2_bias,
    w_up,
    up_bias,
    w_down,
    down_bias,
    cotangent,
):
    nz = lax.axis_size("dp")
    fb_rows, tok2 = block_input.shape[1], block_input.shape[2]
    tok = tok2 // 2
    width = 8 * fb_rows
    heads = w_qkv.shape[3] // HEAD_DIM
    hd = heads * HEAD_DIM
    hw = round_up(hd, 128)
    hp = heads * HEAD_PAD
    hid = w_up.shape[2]
    kh = round_up(hid, 384)
    kp = round_up(3 * hd, 128)
    zrow = w_qkv.shape[1]
    zin = zrow == fb_rows and nz == 4

    wq, wo = jnp.transpose(w_qkv[0], (1, 0, 2)), jnp.transpose(w_out[:, 0, :])
    wu, wd = w_up[0], jnp.transpose(w_down[:, 0, :])
    if not zin:

        def gather(w, cols):
            w = jnp.pad(w, ((0, 0), (0, cols - w.shape[1])))
            return lax.all_gather(lax.all_gather(w, "dp", axis=0, tiled=True), "gy", axis=0, tiled=True)

        wq = gather(w_qkv[0].reshape(zrow, 3 * hd), kp)
        wo, wu, wd = gather(wo, hw), gather(wu, kh), gather(wd, kh)

    win = max(width, kh) // 3
    if win % 128:
        raise ValueError("window")
    cfg = dict(nz=nz, zin=zin, fb=fb_rows, tok=tok, heads=heads, hw=hw, kp=kp)
    tb = tok // 4
    half = width // 2
    vm = pltpu.VMEM
    n_sems = 108 + nz + (12 * nz if zin else 12)
    dw_specs = [pl.BlockSpec(memory_space=pl.ANY)] * 4
    if zin:
        dw_shapes = (jax.ShapeDtypeStruct((3, fb_rows, hw), F32),)
        dw_shapes += tuple(jax.ShapeDtypeStruct((fb_rows, k), F32) for k in (hw, kh, kh))
        core_shapes = [vm((half, k), BF16) for k in (kp, hw, kh, kh)]
        z_shapes = [vm((4, fb_rows, k), BF16) for k in (kp, hw, kh, kh)]
    else:
        dw_shapes = tuple(jax.ShapeDtypeStruct((width, k), BF16) for k in (kp, hw, kh, kh))
        core_shapes = [vm((16, 128), BF16)] * 4
        z_shapes = [vm((16, 128), BF16)] * 4
    scratch = [
        vm((8, 256), F32),
        vm((8, 8, 256), F32),
        vm((width, 128), F32),
        vm((width, tok), BF16),
        vm((width, tok), BF16),
        vm((width, tok), BF16),
        vm((width, tok), BF16),
        vm((width, tok), BF16),
        vm((width, kp), BF16),
        vm((width, hw), BF16),
        vm((width, kh), BF16),
        vm((width, kh), BF16),
        vm((3 * hp, tok), BF16),
        vm((4 * hd, tok), BF16),
        vm((4 * hd, width), BF16),
        vm((hp, tb), BF16),
        vm((kh, tok), BF16),
        vm((kh, tok), BF16),
        vm((width, tb), F32),
        vm((3, width, tb), BF16),
        vm((6, fb_rows, tok), BF16),
        vm((6, fb_rows, tok), BF16),
        vm((2, fb_rows, tok), BF16),
        vm((2, fb_rows, tok), BF16),
        vm((hd, tb), F32),
        vm((max(width, kh), tb), F32),
        vm((max(width, kh), tb), F32),
        vm((tok, 128), jnp.int32),
        vm((4 + 2 * heads, 8, tok), F32),
        vm((max(width, kh), 128), F32),
        vm((tok // 64, 128), F32),
        vm((8, tok // 64, 128), F32),
        vm((8, max(width, kh)), F32),
        vm((8, max(width, kh)), F32),
        vm((8, max(width, kh)), F32),
        vm((4, 8, win), F32),
        vm((nz, 16, win), F32),
        *core_shapes,
        *z_shapes,
        pltpu.SemaphoreType.DMA((n_sems,)),
        pltpu.SemaphoreType.DMA((n_sems,)),
    ]
    any_spec = pl.BlockSpec(memory_space=pl.ANY)
    vmem_spec = pl.BlockSpec(memory_space=pltpu.VMEM)
    w_spec = vmem_spec if zin else any_spec
    out, ig, dq, do, du, dd, sm = pl.pallas_call(
        functools.partial(block_kernel, cfg),
        out_shape=(
            jax.ShapeDtypeStruct((fb_rows, tok2), BF16),
            jax.ShapeDtypeStruct((fb_rows, tok2), F32),
            *dw_shapes,
            jax.ShapeDtypeStruct((16, win), F32),
        ),
        in_specs=[pl.BlockSpec(memory_space=pltpu.SMEM)] + [vmem_spec] * 7 + [any_spec] + [w_spec] * 4 + [vmem_spec] * 2,
        out_specs=(vmem_spec, vmem_spec, *dw_specs, vmem_spec),
        scratch_shapes=scratch,
        compiler_params=pltpu.CompilerParams(
            collective_id=0, has_side_effects=True, vmem_limit_bytes=67043328
        ),
        name="encoder_block",
    )(
        lengths,
        ln1_gain,
        ln1_bias,
        out_bias,
        ln2_gain,
        ln2_bias,
        down_bias,
        block_input[0],
        cotangent[0],
        wq,
        wo,
        wu,
        wd,
        qv_bias,
        up_bias,
    )

    if not zin:

        def reduce(a):
            a = lax.psum_scatter(a, "gy", scatter_dimension=0, tiled=True)
            return lax.optimization_barrier(lax.psum_scatter(a, "dp", scatter_dimension=0, tiled=True)).astype(F32)

        dq, do, du, dd = reduce(dq), reduce(do), reduce(du), reduce(dd)
        dq = jnp.transpose(dq[:, : 3 * hd].reshape(zrow, 3, hd), (1, 0, 2))

    shapes = [(fb_rows, tok2, BF16), (fb_rows, tok2, F32)] + [(1, fb_rows, F32)] * 6 + [(2, hd, F32), (hid, F32)]
    shapes = [jax.ShapeDtypeStruct(a[:-1], a[-1]) for a in shapes]
    given = []
    if zin:
        given = [dq, do, du, dd]
        shapes += [jax.ShapeDtypeStruct((3, fb_rows, hd), F32), jax.ShapeDtypeStruct((fb_rows, hd), F32)]
        shapes += [jax.ShapeDtypeStruct((fb_rows, hid), F32)] * 2
    final = pl.pallas_call(
        functools.partial(finish_kernel, dict(fb=fb_rows, hd=hd, n_dw=len(given))),
        out_shape=tuple(shapes),
        in_specs=[vmem_spec] * (3 + len(given)),
        out_specs=(vmem_spec,) * len(shapes),
        compiler_params=pltpu.CompilerParams(vmem_limit_bytes=67043328),
        name="finish",
    )(out, ig, sm, *given)
    out, ig, g1, b1, ob, g2, b2, db, qv, up = final[:10]
    if zin:
        dq, do, du, dd = final[10:]
    else:
        do, du, dd = do[:, :hd], du[:, :hid], dd[:, :hid]
    return (
        out[None],
        ig[None],
        g1,
        b1,
        jnp.transpose(dq, (1, 0, 2))[None],
        qv,
        jnp.transpose(do)[:, None, :],
        ob,
        g2,
        b2,
        du[None],
        up,
        jnp.transpose(dd)[:, None, :],
        db,
    )


def solution(mesh):
    in_specs = (
        P("gy", "gx", "dp"),
        P(("dp", "gy"), None),
        P("gy", "gx"),
        P("gy", "gx"),
        P("gy", "dp", None, "gx"),
        P(None, "gx"),
        P("gx", "gy", "dp"),
        P("gy", "gx"),
        P("gy", "gx"),
        P("gy", "gx"),
        P("gy", "dp", "gx"),
        P("gx"),
        P("gx", "gy", "dp"),
        P("gy", "gx"),
        P("gy", "gx", "dp"),
    )
    out_specs = (
        P("gy", "gx", "dp"),
        P("gy", "gx", "dp"),
        P("gy", "gx"),
        P("gy", "gx"),
        P("gy", "dp", None, "gx"),
        P(None, "gx"),
        P("gx", "gy", "dp"),
        P("gy", "gx"),
        P("gy", "gx"),
        P("gy", "gx"),
        P("gy", "dp", "gx"),
        P("gx"),
        P("gx", "gy", "dp"),
        P("gy", "gx"),
    )
    return jax.shard_map(local, mesh=mesh, in_specs=in_specs, out_specs=out_specs, check_vma=False)
```

```python
import functools

import jax
import jax.numpy as jnp
from jax import lax
from jax.experimental import pallas as pl
from jax.experimental.pallas import tpu as pltpu
from jax.sharding import PartitionSpec as P

HEAD_DIM = 72
HEAD_PAD = 80
EPSILON = 1e-06
MESH = pl.DeviceIdType.MESH
BF16 = jnp.bfloat16
F32 = jnp.float32
NN = (((1,), (0,)), ((), ()))
NT = (((1,), (1,)), ((), ()))
TN = (((0,), (0,)), ((), ()))
GELU_A = 0.044715
GELU_C = 0.7978845608028654


def mm(a, b, dims):
    return lax.dot_general(a, b, dims, preferred_element_type=F32)


def round_up(value, unit):
    return (value + unit - 1) // unit * unit


def block_kernel(
    cfg,
    len_ref,
    g1_ref,
    b1_ref,
    ob_ref,
    g2_ref,
    b2_ref,
    db_ref,
    x_ref,
    cot_ref,
    wq_in,
    wo_in,
    wu_in,
    wd_in,
    qv_ref,
    up_ref,
    out_ref,
    ig_ref,
    dq_out,
    do_out,
    du_out,
    dd_out,
    sm_out,
    prm_send,
    prm_all,
    prm_col,
    x_t,
    cot_t,
    h1_t,
    h2_t,
    gb_t,
    wq,
    wo,
    wu,
    wd,
    qkv_t,
    att_t,
    wo_n,
    gatt_t,
    act_t,
    gpre_t,
    resid,
    trecv,
    mrecv,
    grecv,
    mrelay,
    grelay,
    dqf,
    fa,
    fb,
    pk,
    rows_f,
    sums_col,
    uv_send,
    uv_recv,
    sm_send,
    sm_part,
    sm_chip,
    sm_win,
    smz_recv,
    cq,
    co,
    cu,
    cd,
    cv,
    zq,
    zo,
    zu,
    zd,
    zv,
    out_s,
    ig_s,
    sem_s,
    sem_r,
):
    prm_refs = (g1_ref, b1_ref, ob_ref, g2_ref, b2_ref, db_ref)
    nz, zin = cfg["nz"], cfg["zin"]
    fb_rows, tok, heads = cfg["fb"], cfg["tok"], cfg["heads"]
    half, width = 4 * fb_rows, 8 * fb_rows
    tb = tok // 4
    hd = heads * HEAD_DIM
    hw, kp = cfg["hw"], cfg["kp"]
    factor = HEAD_DIM ** (-0.5)
    z, g, c = lax.axis_index("dp"), lax.axis_index("gx"), lax.axis_index("gy")
    g_hi, g_lo = g // 2, g % 2

    def gx_of(dd):
        return ((g_hi + dd // 2) % 2) * 2 + (g_lo + dd % 2) % 2

    def row_of(dc):
        return (c + dc) % 2

    counter = [0]

    def take(count):
        first = counter[0]
        counter[0] += count
        return first

    def rcopy(src, dst, sem, dev, send=None):
        return pltpu.make_async_remote_copy(
            src_ref=src,
            dst_ref=dst,
            send_sem=sem_s.at[sem if send is None else send],
            recv_sem=sem_r.at[sem],
            device_id=dev,
            device_id_type=MESH,
        )

    def lcopy(src, dst, sem):
        return pltpu.make_async_copy(src, dst, sem_r.at[sem])

    others = [(dd, dc) for dd in (1, 2, 3, 0) for dc in (0, 1) if dd or dc]
    near = [(dd, dc) for dd, dc in others if dd < 3]

    def dev(dd, dc):
        return (z, gx_of(dd), row_of(dc))

    def feat(dd, dc):
        return pl.ds(pl.multiple_of(row_of(dc) * half + gx_of(dd) * fb_rows, 16), fb_rows)

    def toks(j):
        return pl.ds(pl.multiple_of(j * tb, 128), tb)

    def row_tok(dc):
        return pl.ds(pl.multiple_of(row_of(dc) * tok, 128), tok)

    pending = []

    barrier = pltpu.get_barrier_semaphore()
    for dd, dc in others:
        pl.semaphore_signal(barrier, inc=1, device_id=dev(dd, dc), device_id_type=MESH)
    for k in range(1, nz):
        pl.semaphore_signal(barrier, inc=1, device_id=((z + k) % nz, g, c), device_id_type=MESH)
    ends = []
    total = len_ref[0, 0]
    ends.append(total)
    for s in range(1, len_ref.shape[1]):
        total = total + len_ref[0, s]
        ends.append(total)

    def pictures(pos):
        picture = jnp.zeros_like(pos)
        for end in ends:
            picture = picture + jnp.where(pos >= end, 1, 0)
        return picture

    pos_col = lax.broadcasted_iota(jnp.int32, (tok, 128), 0)
    pk[...] = jnp.where(pos_col < total, pictures(pos_col), -1)
    pos_row = lax.broadcasted_iota(jnp.int32, (8, tok), 1)
    pic_row = pictures(pos_row)
    rows_f[0, :, :] = pic_row.astype(F32)
    rows_f[1, :, :] = jnp.where(pos_row < total, 1.0, 0.0)
    sums_col[...] = jnp.zeros_like(sums_col)
    qkv_t[...] = jnp.zeros_like(qkv_t)
    gatt_t[...] = jnp.zeros_like(gatt_t)

    prm_send[...] = jnp.zeros_like(prm_send)
    for k, ref in enumerate(prm_refs):
        prm_send[k : k + 1, 0:fb_rows] = ref[...]
    sm_send[...] = jnp.zeros_like(sm_send)
    sm_send[0:1, 0 : up_ref.shape[0]] = up_ref[...].reshape(1, up_ref.shape[0])
    sm_send[1:2, 0:hd] = qv_ref[0:1, :]
    sm_send[1:2, 2 * hd : 3 * hd] = qv_ref[1:2, :]
    for n in range(0, sm_send.shape[1], 128):
        rows = jnp.concatenate([sm_send[:, n : n + 128], jnp.zeros((120, 128), F32)], axis=0)
        prm_col[n : n + 128, 8:16] = jnp.transpose(rows)[:, 0:8]
    if zin:
        rows = pl.ds(pl.multiple_of(c * half + z * fb_rows, 16), fb_rows)
        gap = jnp.zeros((fb_rows, kp - 3 * hd), BF16)
        wq[rows, :] = jnp.concatenate([wq_in[0], wq_in[1], wq_in[2], gap], axis=1)
        for src, dst in ((wo_in, wo), (wu_in, wu), (wd_in, wd)):
            gap = jnp.zeros((fb_rows, dst.shape[1] - src.shape[1]), BF16)
            dst[rows, :] = jnp.concatenate([src[...], gap], axis=1)
    pl.semaphore_wait(barrier, 7 + nz - 1)

    own_feat = feat(0, 0)
    own_t = toks(g)
    partner = (z, g, 1 - c)
    me = c * 4 + g
    th = tok // 2

    def exchange(first, src, dst):
        for dd, dc in others:
            rcopy(src, dst, first + dd * 2 + dc, dev(dd, dc)).start()
            pending.append(lambda dd=dd, dc=dc: rcopy(src, dst, first + dd * 2 + dc, dev(dd, dc)).wait_send())

    passing = ((0, 1, 0), (1, 2, 1))

    def gather_copy(first, src, dst, n, size, dd, dc):
        tokens = pl.ds(pl.multiple_of(row_of(dc) * tok + n * size, 128), size)
        part = dst.at[own_feat, n * size : (n + 1) * size]
        return rcopy(src.at[:, tokens], part, first + n * 8 + dd * 2 + dc, dev(dd, dc))

    def gather_land(first, dst, n, size, dd, dc, sem):
        part = dst.at[feat(dd, dc), n * size : (n + 1) * size]
        return rcopy(part, part, first + n * 8 + sem, partner)

    def gather_pass(first, dst, n, size, k, dd, dc):
        part = dst.at[feat(dd, dc), n * size : (n + 1) * size]
        return rcopy(part, part, first + n * 8 + 6 + k, dev(3 - dd, 0))

    def gather_own(first, src, dst, n, size):
        tokens = pl.ds(pl.multiple_of(row_of(0) * tok + n * size, 128), size)
        return lcopy(src.at[:, tokens], dst.at[own_feat, n * size : (n + 1) * size], first + n * 8)

    def gather_start(first, src, dst, n, size):
        for dd, dc in near:
            gather_copy(first, src, dst, n, size, dd, dc).start()
        gather_own(first, src, dst, n, size).start()

    def gather_relay(first, dst, n, size):
        for k, dd, dc in passing:
            gather_land(first, dst, n, size, dd, dc, dd * 2 + dc).wait_recv()
            gather_pass(first, dst, n, size, k, dd, dc).start()

    def gather_done(first, src, dst, n, size):
        gather_own(first, src, dst, n, size).wait()
        for dd, dc in ((0, 1), (1, 1), (2, 0)):
            gather_land(first, dst, n, size, dd, dc, dd * 2 + dc).wait_recv()
        for k in (0, 1):
            gather_land(first, dst, n, size, 3, k, 6 + k).wait_recv()

    def gather_sent(first, src, dst, n, size):
        for dd, dc in near:
            gather_copy(first, src, dst, n, size, dd, dc).wait_send()
        for k, dd, dc in passing:
            gather_pass(first, dst, n, size, k, dd, dc).wait_send()

    q_cuts = (0, 256, 512, kp)
    weights = tuple(wq.at[:, q_cuts[p] : q_cuts[p + 1]] for p in range(3)) + (wo, wu, wd)
    inputs = (wq_in, None, None, wo_in, wu_in, wd_in)
    whole = (wq, wq, wq, wo, wu, wd)
    n_w = len(weights)
    steps = nz - 1
    nw = nz if zin else 1
    wz0 = take((n_w + 2) * nw)
    wc0 = take(4 * nw)

    def zrows(zz, core):
        return pl.ds(pl.multiple_of(core * half + zz * fb_rows, 16), fb_rows)

    def w_rows(i, zz, core):
        return weights[i].at[zrows(zz, core), :]

    def whole_rows(i, zz, core):
        return whole[i].at[zrows(zz, core), :]

    def hop(i, s, d):
        origin = z - (s - 1) if d == 0 else z + (s - 1)
        here = jnp.logical_and(z >= s - 1, z < nz - 1) if d == 0 else jnp.logical_and(z < nz - s + 1, z > 0)
        to = z + 1 if d == 0 else z - 1
        send = wz0 + n_w * nw + i if s == 1 and d == 1 else None
        return here, lambda: rcopy(w_rows(i, origin, c), w_rows(i, origin, c), wz0 + i * nw + origin, (to, g, c), send)

    def arrival(s, d):
        return (z >= s, z - s) if d == 0 else (z < nz - s, z + s)

    def pass_on(i, zz):
        first = max(i - 2, 0)
        return rcopy(whole_rows(i, zz, c), whole_rows(i, zz, c), wc0 + first * nw + zz, partner)

    def z_send(i, s):
        if not zin:
            if s == 1 and inputs[i] is not None:
                lcopy(inputs[i], whole[i], wz0 + i * nw).start()
            return
        for d in (0, 1):
            here, make = hop(i, s, d)
            pl.when(here)(lambda make=make: make().start())
        if s == 1 and i >= 2:
            pass_on(i, z).start()

    def z_recv(i, s):
        if not zin:
            return
        for d in (0, 1):
            here, origin = arrival(s, d)

            @pl.when(here)
            def _(s=s, d=d, origin=origin):
                rows = w_rows(i, origin, c)
                rcopy(rows, rows, wz0 + i * nw + origin, partner).wait_recv()
                if i >= 2:
                    pass_on(i, origin).start()

        if s < steps:
            z_send(i, s + 1)

    def weight_ready(i):
        if not zin:
            if inputs[i] is not None:
                lcopy(inputs[i], whole[i], wz0 + i * nw).wait()
            return
        if i >= 2:
            for zz in range(nz):
                rows = whole_rows(i, zz, 1 - c)
                rcopy(rows, rows, wc0 + (i - 2) * nw + zz, partner).wait_recv()

    def weight_passed(i):
        if not zin:
            return
        for s in range(1, nz):
            for d in (0, 1):
                here, make = hop(i, s, d)
                pl.when(here)(lambda make=make: make().wait_send())
        if i >= 2:
            for zz in range(nz):
                pass_on(i, zz).wait_send()

    p0 = take(8)
    xs0 = take(16)
    cs0 = take(32)
    exchange(p0, prm_send, prm_all.at[me])
    lcopy(prm_send, prm_all.at[me], p0).start()
    for n in (0, 1):
        gather_start(xs0, x_ref, x_t, n, th)
    for i in (0, 1, 2):
        z_send(i, 1)

    def par(k):
        return prm_col[:, k : k + 1]

    def z_recv_all(pairs):
        for i, step in pairs:
            if step < nz:
                z_recv(i, step)

    wn0 = take(8)

    def wo_part(gx, core, first=0, last=None):
        rows = (fb_rows if last is None else last) - first
        return wo_n.at[pl.ds(pl.multiple_of(gx * hd + core * fb_rows + first, 16), rows), :]

    cut = fb_rows // 32 * 16 + 16

    def wo_copy(n):
        if n < 2:
            own = wo_part(g, c)
            return rcopy(own, own, wn0 + n + 1, (z, gx_of(n + 1), c))
        if n < 4:
            got = wo_part(gx_of(n - 1), c)
            return rcopy(got, got, wn0 + n + 1, partner)
        if n < 6:
            on = wo_part(gx_of(1), c, 0, cut) if n == 4 else wo_part(gx_of(2), c, cut)
            return rcopy(on, on, wn0 + n + 1, (z, gx_of(6 - n), c))
        far = wo_part(gx_of(3), c)
        return rcopy(far, far, wn0 + 7, partner)

    def wo_first():
        turned = jnp.transpose(wo[...])
        wo_n[pl.ds(pl.multiple_of(g * hd, 16), hd), :] = turned[0:hd, :]
        for n in (0, 1):
            wo_copy(n).start()

    def wo_second():
        for step in (1, 2):
            got = wo_part(gx_of(step), c)
            rcopy(got, got, wn0 + step, partner).wait_recv()
        for n in (4, 5, 2, 3):
            wo_copy(n).start()

    def wo_third():
        for step, on in ((1, wo_part(gx_of(3), c, 0, cut)), (2, wo_part(gx_of(3), c, cut))):
            rcopy(on, on, wn0 + 4 + step, partner).wait_recv()
        wo_copy(6).start()

    def wo_ready():
        for step in (1, 2):
            got = wo_part(gx_of(step), 1 - c)
            rcopy(got, got, wn0 + 2 + step, partner).wait_recv()
        far = wo_part(gx_of(3), 1 - c)
        rcopy(far, far, wn0 + 7, partner).wait_recv()

    def head_rows(part, h):
        return pl.ds(pl.multiple_of((part * heads + h) * HEAD_PAD, 16), HEAD_PAD)

    def project(j, carry):
        t = toks(j)
        x = x_t[:, t].astype(F32)
        m = jnp.sum(x, axis=0, keepdims=True) * (1.0 / width)
        q = jnp.sum(x * x, axis=0, keepdims=True) * (1.0 / width)
        r = lax.rsqrt(q - m * m + EPSILON)
        rows_f[2, 0:1, t] = m
        rows_f[3, 0:1, t] = r
        h1_t[:, t] = ((x - m) * r * par(0) + par(1)).astype(BF16)
        part = mm(wq[...], h1_t[:, t], TN) + prm_col[0:kp, 9:10]
        for p in range(3):
            for h in range(heads):
                first, row = (p * heads + h) * HEAD_PAD, p * hd + h * HEAD_DIM
                qkv_t[first : first + HEAD_DIM, t] = part[row : row + HEAD_DIM, :].astype(BF16)
        return carry

    z_recv_all(((0, 1), (1, 1), (2, 1)))
    z_send(3, 1)
    gather_relay(xs0, x_t, 0, th)
    z_recv_all(((0, 2), (1, 2)))
    gather_relay(xs0, x_t, 1, th)
    z_recv_all(((2, 2), (3, 1)))

    lcopy(prm_send, prm_all.at[me], p0).wait()
    for dd, dc in others:
        rcopy(prm_send, prm_all.at[row_of(dc) * 4 + gx_of(dd)], p0 + dd * 2 + dc, partner).wait_recv()
    for b in range(8):
        rows = jnp.concatenate([prm_all[b], jnp.zeros((120, 256), F32)], axis=0)
        prm_col[b * fb_rows : (b + 1) * fb_rows, 0:8] = jnp.transpose(rows)[:fb_rows, 0:8]

    for step in range(3, nz):
        z_recv_all((i, step) for i in range(3))
    for i in range(3):
        weight_ready(i)
    gather_done(xs0, x_ref, x_t, 0, th)
    for n in (0, 1):
        gather_start(cs0, cot_ref, cot_t, n, tb)
    lax.fori_loop(0, 2, project, 0)
    z_recv_all(((3, 2),))
    z_send(4, 1)
    gather_done(xs0, x_ref, x_t, 1, th)
    lax.fori_loop(2, 4, project, 0)
    z_recv_all((3, step) for step in range(3, nz))
    weight_ready(3)
    wo_first()

    def kept_of(h, t):
        scores = mm(qkv_t[head_rows(1, h), :], qkv_t[head_rows(0, h), t], TN) * factor
        key_pic = pk[...]
        query_pic = rows_f[0, 0:1, t].astype(jnp.int32)
        allowed = jnp.concatenate([key_pic] * (tb // 128), axis=1) == query_pic
        return jnp.where(allowed, jnp.exp(scores), 0.0)

    at0 = take(4 * 3)
    own_heads = pl.ds(pl.multiple_of(g * hd, 16), hd)

    def att_piece(dd, j):
        return att_t.at[pl.ds(pl.multiple_of(gx_of(dd) * hd, 16), hd), toks(j)]

    def att_send(j, start):
        for step in (1, 2):
            piece = att_piece(0, j)
            cp = rcopy(piece, piece, at0 + j * 3 + step - 1, (z, gx_of(step), c))
            cp.start() if start else cp.wait_send()

    def att_relay(j):
        for step in (1, 2):
            piece = att_piece(step, j)
            rcopy(piece, piece, at0 + j * 3 + step - 1, partner).wait_recv()
        step = 1 + j % 2
        piece = att_piece(step, j)
        rcopy(piece, piece, at0 + j * 3 + 2, (z, gx_of(3 - step), c)).start()

    def att_relayed(j):
        piece = att_piece(1 + j % 2, j)
        rcopy(piece, piece, at0 + j * 3 + 2, partner).wait_send()

    def attend(j, carry):
        t = toks(j)

        def head(h, inner):
            kept = kept_of(h, t)
            den = jnp.sum(kept, axis=0, keepdims=True)
            den = jnp.where(rows_f[1, 0:1, t] > 0.5, den, 1.0)
            scale = jnp.where(den > 1e30, 2.0**-40, 1.0)
            inv = 1.0 / (den * scale)
            rows_f[4 + 2 * h, 0:1, t] = scale
            rows_f[5 + 2 * h, 0:1, t] = inv
            probs = (kept * scale * inv).astype(BF16)
            att = mm(qkv_t[head_rows(2, h), :], probs, NN)
            dqf[pl.ds(pl.multiple_of(h * HEAD_DIM, 8), HEAD_DIM), :] = att[0:HEAD_DIM, :]
            return inner

        lax.fori_loop(0, heads, head, 0)
        att_t[own_heads, t] = dqf[...].astype(BF16)

        att_send(j, True)

        @pl.when(j == 0)
        def _():
            z_recv_all(((4, 1),))
            z_send(5, 1)

        @pl.when(j == 1)
        def _():
            wo_second()

        @pl.when(j == 2)
        def _():
            att_relay(0)
            z_recv_all(((4, 2),))

        return carry

    lax.fori_loop(0, 4, attend, 0)
    att_relay(1)
    wo_third()
    z_recv_all(((5, 1),))
    att_relay(2)

    def project_out(j, carry):
        t = toks(j)

        @pl.when(j == 0)
        def _():
            wo_ready()

        far = att_piece(3, j)
        rcopy(far, far, at0 + j * 3 + 2, partner).wait_recv()
        residual = mm(wo_n[...], att_t[:, t], TN) + x_t[:, t].astype(F32) + par(2)
        m2 = jnp.sum(residual, axis=0, keepdims=True) * (1.0 / width)
        q2 = jnp.sum(residual * residual, axis=0, keepdims=True) * (1.0 / width)
        r2 = lax.rsqrt(q2 - m2 * m2 + EPSILON)
        rows_f[2, 1:2, t] = m2
        rows_f[3, 1:2, t] = r2
        h2_t[:, t] = ((residual - m2) * r2 * par(3) + par(4)).astype(BF16)

        @pl.when(j == g)
        def _():
            resid[...] = residual

        @pl.when(j == 0)
        def _():
            att_relay(3)
            for n in (2, 3):
                gather_start(cs0, cot_ref, cot_t, n, tb)
            for n in (0, 1):
                gather_relay(cs0, cot_t, n, tb)

        @pl.when(j == 1)
        def _():
            z_recv_all((4, step) for step in range(3, nz))

        @pl.when(j == 2)
        def _():
            z_recv_all(((5, 2),))

        return carry

    lax.fori_loop(0, 4, project_out, 0)
    weight_ready(4)
    for n in range(7):
        wo_copy(n).wait_send()

    def spread(first, buf):
        for step in (1, 2):
            rcopy(buf.at[:, own_t], buf.at[:, own_t], first + step, (z, gx_of(step), c)).start()

    def halves(buf, step, k):
        return buf.at[(k - 1) * half : k * half, toks(gx_of(step))]

    def spread_relay(first, buf):
        for step in (1, 2):
            block = buf.at[:, toks(gx_of(step))]
            rcopy(block, block, first + step, partner).wait_recv()
            part = halves(buf, step, step)
            rcopy(part, part, first + 2 + step, (z, gx_of(3 - step), c)).start()

    def spread_done(first, buf):
        for k in (1, 2):
            part = halves(buf, 3, k)
            rcopy(part, part, first + 2 + k, partner).wait_recv()

    def spread_sent(first, buf):
        for step in (1, 2):
            rcopy(buf.at[:, own_t], buf.at[:, own_t], first + step, partner).wait_send()
            part = halves(buf, step, step)
            rcopy(part, part, first + 2 + step, partner).wait_send()

    def mlp_up(i, carry):
        t = toks(i)
        fa[...] = mm(wu[...], h2_t[:, t], TN) + prm_col[:, 8:9]

        def chunk(n, inner):
            rows = pl.ds(pl.multiple_of(n * 48, 16), 48)
            v = fa[rows, :]
            v2 = v * v
            thv = jnp.tanh(GELU_C * (v + GELU_A * v2 * v))
            hf = 0.5 * (1.0 + thv)
            act_t[rows, t] = (v * hf).astype(BF16)
            slope = hf + (0.5 * GELU_C) * v * (1.0 - thv * thv) * (1.0 + (3.0 * GELU_A) * v2)
            gpre_t[rows, t] = slope.astype(BF16)
            return inner

        lax.fori_loop(0, fa.shape[0] // 48, chunk, 0)

        @pl.when(i == 1)
        def _():
            for n in (2, 3):
                gather_relay(cs0, cot_t, n, tb)

        return carry

    lax.fori_loop(0, 4, mlp_up, 0)
    for n in range(4):
        gather_done(cs0, cot_ref, cot_t, n, tb)
    z_recv_all((5, step) for step in range(3, nz))
    weight_ready(5)

    for n in (0, 1):
        gather_sent(xs0, x_ref, x_t, n, th)
    g20 = xs0

    def tsend(step):
        return wo_n.at[:, (step - 1) * tb : step * tb]

    def g2_copy(n):
        top, bottom = slice(0, half), slice(half, width)
        rows = (top, bottom, top, bottom, bottom, top)[n]
        step = (3, 3, 1, 1, 2, 2)[n]
        slot = (2, 2, 0, 0, 1, 1)[n]
        to = (1, 2, 1, 1, 2, 2)[n]
        src = wo_n.at[rows, (step - 1) * tb : step * tb]
        return rcopy(src, trecv.at[slot, rows, :], g20 + n, (z, gx_of(to), c))

    def mlp_back(i, carry):
        t = toks(gx_of(3 - i))
        gpre_t[:, t] = (mm(wd[...], cot_t[:, t], TN) * gpre_t[:, t].astype(F32)).astype(BF16)
        fa[...] = mm(wu[...], gpre_t[:, t], NN)
        for step, sends in ((3, (0, 1)), (2, (4,)), (1, (2,))):

            @pl.when(i == 3 - step)
            def _(step=step, sends=sends):
                tsend(step)[...] = fa[...].astype(BF16)
                for n in sends:
                    g2_copy(n).start()

        return carry

    lax.fori_loop(0, 4, mlp_back, 0)
    for n, step, rows, then in ((0, 2, slice(0, half), 5), (1, 1, slice(half, width), 3)):
        g2_copy(n).wait_recv()
        cols = slice((step - 1) * tb, step * tb)
        wo_n[rows, cols] = (wo_n[rows, cols].astype(F32) + trecv[2, rows, :].astype(F32)).astype(BF16)
        g2_copy(then).start()

    dwc0 = take(5)
    dwz0 = take(5 * 6)
    first_up = 2 * wu.shape[1] // 3
    do0 = take(4)
    gath = ((0, 1, 2), (3,), (4,), (5,), ())
    core_recv = (cq, co, cu, cd, cv)
    z_recvs = (zq, zo, zu, zd, zv)
    dw_refs = (wo_n, wo, wu.at[:, 0:first_up], wd, wu.at[:, first_up : wu.shape[1]])
    dw_cols = (kp, wo.shape[1], first_up, wd.shape[1], wu.shape[1] - first_up)
    up_outs = (du_out.at[:, 0:first_up], du_out.at[:, first_up : wu.shape[1]])
    dw_outs = (dq_out, do_out, up_outs[0], dd_out, up_outs[1])
    slots = [0]
    leaving = []

    def weight_grad(i, left, right):
        for n in gath[i]:
            weight_passed(n)
        dst, cols = dw_refs[i], dw_cols[i]
        step_cols = 384

        def one(n, carry):
            cs = pl.ds(pl.multiple_of(n * step_cols, 128), step_cols)
            dst[:, cs] = mm(left[...], right[pl.ds(pl.multiple_of(n * step_cols, 16), step_cols), :], NT).astype(BF16)
            return carry

        lax.fori_loop(0, cols // step_cols, one, 0)
        rest = cols // step_cols * step_cols
        if rest < cols:
            dst[:, rest:cols] = mm(left[...], right[rest:cols, :], NT).astype(BF16)

    def core_half(i, core):
        return dw_refs[i].at[pl.ds(pl.multiple_of(core * half, 16), half), 0 : dw_cols[i]]

    def send_core(i):
        if zin:
            rcopy(core_half(i, 1 - c), core_recv[i], dwc0 + i, partner).start()
            pending.append(lambda: rcopy(core_half(i, 1 - c), core_recv[i], dwc0 + i, partner).wait_send())
        else:
            lcopy(dw_refs[i].at[:, 0 : dw_cols[i]], dw_outs[i], dwc0 + i).start()

    def sum_core(i):
        if not zin:
            return
        rcopy(core_half(i, c), core_recv[i], dwc0 + i, partner).wait_recv()
        w = dw_refs[i]
        for zz in range(nz):
            rows = pl.ds(pl.multiple_of(c * half + zz * fb_rows, 16), fb_rows)
            cols = dw_cols[i]
            w[rows, 0:cols] = (
                w[rows, 0:cols].astype(F32) + core_recv[i][zz * fb_rows : (zz + 1) * fb_rows, :].astype(F32)
            ).astype(BF16)

        @pl.when(leaf)
        def _():
            for slot, zz in enumerate((far_end, far_inner, inner)):
                if i or slot < 2:
                    z_piece(i, slot, zz, slot, inner).start()

        @pl.when(jnp.logical_not(leaf))
        def _():
            z_piece(i, 3, end, 0, end).start()

    leaf = z % 3 == 0
    low = z < 2
    end, inner = jnp.where(low, 0, 3), jnp.where(low, 1, 2)
    far_end, far_inner = 3 - end, 3 - inner

    def z_piece(i, sem, zz, slot, to):
        rows = dw_refs[i].at[zrows(zz, c), 0 : dw_cols[i]]
        return rcopy(rows, z_recvs[i].at[slot], dwz0 + i * 6 + sem, (to, g, c))

    def z_land(i, slot):
        rows = dw_refs[i].at[zrows(z, c), 0 : dw_cols[i]]
        return rcopy(rows, z_recvs[i].at[min(slot, 3) if slot != 3 else 0], dwz0 + i * 6 + slot, partner)

    def relay_z(i, slot):
        if not zin:
            return

        @pl.when(jnp.logical_not(leaf))
        def _():
            z_land(i, slot).wait_recv()
            zz = far_end if slot == 0 else far_inner
            w, cols = dw_refs[i], dw_cols[i]
            rows = zrows(zz, c)
            w[rows, 0:cols] = (w[rows, 0:cols].astype(F32) + z_recvs[i][slot].astype(F32)).astype(BF16)
            z_piece(i, 4 + slot, zz, 3, zz).start()

    def z_sent(i):
        if not zin:
            return

        @pl.when(leaf)
        def _():
            for slot, zz in enumerate((far_end, far_inner, inner)):
                z_piece(i, slot, zz, slot, inner).wait_send()

        @pl.when(jnp.logical_not(leaf))
        def _():
            z_piece(i, 3, end, 0, end).wait_send()
            z_piece(i, 4, far_end, 3, far_end).wait_send()
            z_piece(i, 5, far_inner, 3, far_inner).wait_send()

    def sum_z(i):
        if not zin:
            lcopy(dw_refs[i].at[:, 0 : dw_cols[i]], dw_outs[i], dwc0 + i).wait()
            return

        @pl.when(leaf)
        def _():
            z_land(i, 3).wait_recv()
            z_land(i, 4).wait_recv()

        @pl.when(jnp.logical_not(leaf))
        def _():
            z_land(i, 2).wait_recv()
            z_land(i, 5).wait_recv()

        near_slot = jnp.where(leaf, 0, 2)
        cols = dw_cols[i]

        def total_of(n, size):
            part = dw_refs[i][zrows(z, c), n : n + size].astype(F32)
            return part + z_recvs[i][near_slot, :, n : n + size].astype(F32) + z_recvs[i][3, :, n : n + size].astype(F32)

        if i == 0:
            whole = total_of(0, cols)
            gap = jnp.zeros((fb_rows, hw - hd), F32)
            pieces = []
            for p in range(3):
                part = jnp.concatenate([whole[:, p * hd : (p + 1) * hd], gap], axis=1)
                for n in range(0, hw, tb):
                    size = min(tb, hw - n)
                    pieces.append((part[:, n : n + size], dq_out.at[p, :, n : n + size]))
        else:
            pieces = []
            for n in range(0, cols, tb):
                size = min(tb, cols - n)
                pieces.append((total_of(n, size), dw_outs[i].at[:, n : n + size]))
        for part, goes in pieces:
            size = part.shape[1]
            slot = slots[0] % 16
            if slots[0] >= 4:
                leaving[slots[0] - 4].wait()
            slots[0] += 1
            stage = (fa, fb)[slot // 8].at[(slot % 8) * fb_rows : (slot % 8 + 1) * fb_rows, 0:size]
            stage[...] = part
            cp = lcopy(stage, goes, do0 + slot % 4)
            cp.start()
            leaving.append(cp)

    ml0, gh0, uv0, sm0 = cs0, xs0, at0, p0
    for n in range(4):
        gather_sent(cs0, cot_ref, cot_t, n, tb)
    for j in range(4):
        att_send(j, False)
        att_relayed(j)
    for wait in pending:
        wait()
    pending.clear()
    sz0 = take(nz)
    fin0 = take(2)

    direct, added = ((1, 0), (2, 1), (0, 1)), ((1, 1), (2, 0))

    def hand(buf, relay, first, j, n):
        part = relay.at[n, :, toks(j)]
        return rcopy(buf.at[feat(3, n), toks(j)], part, first + 8 + j * 2 + n, (z, gx_of(n + 1), c))

    def block_copy(buf, recv, first, dd, dc):
        slot = dd * 2 + dc
        return rcopy(buf.at[feat(dd, dc), :], recv.at[slot], first + slot, dev(dd, dc))

    def add_relayed(buf, relay, recv, first):
        for n, (dd, dc) in ((0, (2, 0)), (1, (1, 1))):
            for j in range(4):
                hand(buf, relay, first, j, n).wait_recv()
            rows = feat(dd, dc)
            buf[rows, :] = (buf[rows, :].astype(F32) + relay[n].astype(F32)).astype(BF16)
            block_copy(buf, recv, first, dd, dc).start()

    def scatter_sent(buf, relay, recv, first):
        for dd, dc in direct + added:
            block_copy(buf, recv, first, dd, dc).wait_send()
        for n in (0, 1):
            for j in range(4):
                hand(buf, relay, first, j, n).wait_send()

    def scatter_start(buf, recv, first):
        for dd, dc in direct:
            block_copy(buf, recv, first, dd, dc).start()
        lcopy(buf.at[own_feat, :], recv.at[0], first).start()

    def scatter_sum(buf, recv, first, dc):
        if dc == 0:
            lcopy(buf.at[own_feat, :], recv.at[0], first).wait()
        acc = 0.0
        for dd in (0, 1, 2):
            if dd or dc:
                block_copy(buf, recv, first, dd, dc).wait_recv()
            acc = acc + recv[dd * 2 + dc].astype(F32)
        return acc

    weight_grad(2, h2_t, gpre_t)
    send_core(2)
    weight_grad(4, h2_t, gpre_t.at[first_up : wu.shape[1], :])
    send_core(4)
    sum_core(2)
    ones = jnp.ones((tok, 128), BF16)
    sums_col[0 : act_t.shape[0], 6:7] = mm(gpre_t[...], ones, NN)[:, 0:1]
    sum_core(4)


    def lower(j, carry):
        t = toks(j)
        h2_t[:, t] = mm(wd[...], act_t[:, t], NN).astype(BF16)
        return carry

    lax.fori_loop(0, 4, lower, 0)
    h2_t[:, own_t] = (mm(wd[...], act_t[:, own_t], NN) + resid[...] + par(5)).astype(BF16)

    for n in (2, 3, 4, 5):
        g2_copy(n).wait_recv()
    gh2 = fa[...] + trecv[0].astype(F32) + trecv[1].astype(F32)
    m2 = rows_f[2, 1:2, own_t]
    r2 = rows_f[3, 1:2, own_t]
    normed2 = (resid[...] - m2) * r2
    gn = gh2 * par(3)
    s1 = jnp.sum(gn, axis=0, keepdims=True) * (1.0 / width)
    s2 = jnp.sum(gn * normed2, axis=0, keepdims=True) * (1.0 / width)
    cot_own = cot_t[:, own_t].astype(F32)
    g_res = cot_own + r2 * (gn - s1 - normed2 * s2)
    g_low = g_res.astype(BF16)
    gb_t[:, own_t] = g_low
    gb0 = wn0
    spread(gb0, gb_t)
    resid[...] = g_res
    sums_col[0:width, 2:3] = jnp.sum(g_low.astype(F32), axis=1, keepdims=True)
    sums_col[0:width, 3:4] = jnp.sum(gh2 * normed2, axis=1, keepdims=True)
    sums_col[0:width, 4:5] = jnp.sum(gh2, axis=1, keepdims=True)
    sums_col[0:width, 5:6] = jnp.sum(cot_own, axis=1, keepdims=True)
    for n in range(6):
        g2_copy(n).wait_send()
    weight_grad(3, cot_t, act_t)
    send_core(3)
    relay_z(2, 0)
    relay_z(2, 1)
    sum_core(3)

    fa[...] = jnp.zeros_like(fa)
    fb[...] = jnp.zeros_like(fb)
    act_t[3 * hd : kp, :] = jnp.zeros((kp - 3 * hd, tok), BF16)

    def attend_back(i, carry):
        t = toks(gx_of(i))

        @pl.when(i == 1)
        def _():
            spread_relay(gb0, gb_t)
            relay_z(4, 0)
            relay_z(4, 1)
            for n in (0, 1):
                for k in range(4):
                    hand(h2_t, mrelay, ml0, k, n).start()
            scatter_start(h2_t, mrecv, ml0)

        @pl.when(i == 3)
        def _():
            spread_done(gb0, gb_t)
            relay_z(3, 0)

        gatt = mm(wo[...], gb_t[:, t], TN)
        for h in range(heads):
            gatt_t[h * HEAD_PAD : h * HEAD_PAD + HEAD_DIM, :] = gatt[h * HEAD_DIM : (h + 1) * HEAD_DIM, :].astype(BF16)

        @pl.when(i == 3)
        def _():
            weight_passed(3)
            wo[:, 0:hd] = mm(gb_t[...], att_t[own_heads, :], NT).astype(BF16)
            send_core(1)
            add_relayed(h2_t, mrelay, mrecv, ml0)

        def head(h, inner):
            kept = kept_of(h, t)
            probs = kept * rows_f[4 + 2 * h, 0:1, t] * rows_f[5 + 2 * h, 0:1, t]
            q_rows = head_rows(0, h)
            grad = gatt_t[q_rows, :]
            grad_probs = mm(qkv_t[head_rows(2, h), :], grad, TN)
            weighted = probs * grad_probs
            delta = jnp.sum(weighted, axis=0, keepdims=True)
            grad_scores = (weighted - probs * delta).astype(BF16)
            dq = mm(qkv_t[head_rows(1, h), :], grad_scores, NN) * factor
            dqf[pl.ds(pl.multiple_of(h * HEAD_DIM, 8), HEAD_DIM), :] = dq[0:HEAD_DIM, :]
            dk = mm(qkv_t[q_rows, t], grad_scores, NT)
            dv = mm(grad, probs.astype(BF16), NT)
            for kb in range(4):
                rows = pl.ds(pl.multiple_of(kb * hd + h * HEAD_DIM, 8), HEAD_DIM)
                fa[rows, :] += dk[0:HEAD_DIM, kb * tb : (kb + 1) * tb]
                fb[rows, :] += dv[0:HEAD_DIM, kb * tb : (kb + 1) * tb]
            return inner

        lax.fori_loop(0, heads, head, 0)
        act_t[0:hd, t] = dqf[...].astype(BF16)
        return carry

    lax.fori_loop(0, 4, attend_back, 0)

    for kb in range(4):
        cols, rows = slice(kb * tb, (kb + 1) * tb), slice(kb * hd, (kb + 1) * hd)
        act_t[hd : 2 * hd, cols] = (fa[rows, :] * factor).astype(BF16)
        act_t[2 * hd : 3 * hd, cols] = fb[rows, :].astype(BF16)
    relay_z(3, 1)
    weight_grad(0, h1_t, act_t)
    send_core(0)
    sum_core(1)

    def back1(j, carry):
        t = toks(j)
        gh1 = mm(wq[...], act_t[0:kp, t], NN)
        m = rows_f[2, 0:1, t]
        r = rows_f[3, 0:1, t]
        normed = (x_t[:, t].astype(F32) - m) * r
        gn1 = gh1 * par(0)
        prod = gh1 * normed
        sums_col[0:width, 0:1] += jnp.sum(prod, axis=1, keepdims=True)
        sums_col[0:width, 1:2] += jnp.sum(gh1, axis=1, keepdims=True)
        a1 = jnp.sum(gn1, axis=0, keepdims=True) * (1.0 / width)
        a2 = jnp.sum(gn1 * normed, axis=0, keepdims=True) * (1.0 / width)
        v = r * r * a2
        u = r * a1 - m * v
        for n in range(tb // 128):
            row = j * (tb // 128) + n
            uv_send[pl.ds(row, 1), :] = u[:, n * 128 : (n + 1) * 128]
            uv_send[pl.ds(tok // 128 + row, 1), :] = v[:, n * 128 : (n + 1) * 128]
        fa[...] = r * gn1

        @pl.when(j == g)
        def _():
            fa[...] += resid[...]

        cot_t[:, t] = fa[...].astype(BF16)
        for n in (0, 1):
            hand(cot_t, grelay, gh0, j, n).start()

        @pl.when(j == 0)
        def _():
            sum_core(0)

        return carry

    lax.fori_loop(0, 4, back1, 0)
    relay_z(1, 0)
    relay_z(1, 1)

    sums_col[0:kp, 7:8] = mm(act_t[0:kp, :], ones, NN)[:, 0:1]

    for n in range(0, sm_send.shape[1], 128):
        sm_send[:, n : n + 128] = jnp.transpose(sums_col[n : n + 128, :])[0:8, :]
    exchange(uv0, uv_send, uv_recv.at[me])
    lcopy(uv_send, uv_recv.at[me], uv0).start()
    rcopy(sm_send, sm_part, sm0 + 1, partner).start()
    rcopy(sm_send, sm_part, sm0 + 1, partner).wait_recv()
    sm_chip[...] = sm_send[...] + sm_part[...]
    win = sm_win.shape[2]

    def window(dd):
        first = (c * half + gx_of(dd) * fb_rows) // 128 * 128
        return pl.ds(pl.multiple_of(jnp.minimum(first, sm_chip.shape[1] - win), 128), win)

    def window_copy(dd):
        return rcopy(sm_chip.at[:, window(dd)], sm_win.at[dd], sm0 + dd * 2, (z, gx_of(dd), c))

    for dd in (1, 2, 3):
        window_copy(dd).start()
    scatter_start(cot_t, grecv, gh0)
    add_relayed(cot_t, grelay, grecv, gh0)
    relay_z(0, 0)

    for dc in (0, 1):
        out_s[:, row_tok(dc)] = scatter_sum(h2_t, mrecv, ml0, dc).astype(BF16)
    lcopy(out_s, out_ref, fin0).start()

    sum_z(2)
    sum_z(4)
    sum_z(3)
    relay_z(0, 1)

    total_sm = sm_chip[:, window(0)]
    for dd in (1, 2, 3):
        window_copy(dd).wait_recv()
        total_sm = total_sm + sm_win[dd]
    smz_recv[0, 0:8, :] = total_sm
    for n in range(6):
        smz_recv[0, 8 + n : 9 + n, :] = sm_chip[6 + n // 3 : 7 + n // 3, n % 3 * win : (n % 3 + 1) * win]
    for k in range(1, nz):

        def make(k=k):
            return rcopy(smz_recv.at[0], smz_recv.at[k], sz0 + k, ((z + k) % nz, g, c))

        make().start()
        pending.append(lambda make=make: make().wait_send())

    if zin:

        @pl.when(leaf)
        def _():
            z_piece(0, 2, inner, 2, inner).start()

    sum_z(1)

    lcopy(uv_send, uv_recv.at[me], uv0).wait()
    for dd, dc in others:
        rcopy(uv_send, uv_recv.at[row_of(dc) * 4 + gx_of(dd)], uv0 + dd * 2 + dc, partner).wait_recv()
    for dc in (0, 1):
        acc = scatter_sum(cot_t, grecv, gh0, dc)
        uv = uv_recv[row_of(dc) * 4 + g]
        for dd in (1, 2, 3):
            uv = uv + uv_recv[row_of(dc) * 4 + gx_of(dd)]
        n_rows = tok // 128
        u_row = jnp.concatenate([uv[n : n + 1, :] for n in range(n_rows)], axis=1)
        v_row = jnp.concatenate([uv[n_rows + n : n_rows + n + 1, :] for n in range(n_rows)], axis=1)
        x_own = x_ref[:, row_tok(dc)].astype(F32)
        ig_s[:, row_tok(dc)] = acc - u_row - x_own * v_row
    lcopy(ig_s, ig_ref, fin0 + 1).start()

    sum_z(0)
    total_z = smz_recv[0]
    for k in range(1, nz):
        rcopy(smz_recv.at[0], smz_recv.at[k], sz0 + k, partner).wait_recv()
        total_z = total_z + smz_recv[k]
    sm_out[...] = total_z

    for cp in leaving[-4:]:
        cp.wait()
    lcopy(out_s, out_ref, fin0).wait()
    lcopy(ig_s, ig_ref, fin0 + 1).wait()
    rcopy(sm_send, sm_part, sm0 + 1, partner).wait_send()
    for dd in (1, 2, 3):
        window_copy(dd).wait_send()
    for wait in pending:
        wait()
    scatter_sent(h2_t, mrelay, mrecv, ml0)
    scatter_sent(cot_t, grelay, grecv, gh0)
    for i in range(5):
        z_sent(i)
    spread_sent(gb0, gb_t)


def finish_kernel(cfg, out_in, ig_in, sm_in, *refs):
    fb_rows, hd, n_dw = cfg["fb"], cfg["hd"], cfg["n_dw"]
    dw_in, (out_ref, ig_ref, *small), dw_ref = refs[:n_dw], refs[n_dw : n_dw + 10], refs[n_dw + 10 :]
    out_ref[...] = out_in[...]
    ig_ref[...] = ig_in[...]
    sums = sm_in[...]
    win = sums.shape[1]
    mine = lax.axis_index("gy") * (4 * fb_rows) + lax.axis_index("gx") * fb_rows
    first = jnp.minimum(mine // 128 * 128, 2 * win)
    turned = pltpu.roll(sums[0:8, :], (win - (mine - first)) % win, 1)
    for k in range(6):
        small[k][...] = turned[k : k + 1, 0:fb_rows]
    up_row, qkv_row = (jnp.concatenate([sums[r + n : r + n + 1, :] for n in range(3)], axis=1) for r in (8, 11))
    small[6][0:1, :] = qkv_row[:, 0:hd]
    small[6][1:2, :] = qkv_row[:, 2 * hd : 3 * hd]
    small[7][...] = up_row[:, 0 : small[7].shape[0]].reshape(small[7].shape[0])
    for src, dst in zip(dw_in, dw_ref):
        dst[...] = src[:, :, 0 : dst.shape[2]] if len(dst.shape) == 3 else src[:, 0 : dst.shape[1]]


def local(
    block_input,
    lengths,
    ln1_gain,
    ln1_bias,
    w_qkv,
    qv_bias,
    w_out,
    out_bias,
    ln2_gain,
    ln2_bias,
    w_up,
    up_bias,
    w_down,
    down_bias,
    cotangent,
):
    nz = lax.axis_size("dp")
    fb_rows, tok2 = block_input.shape[1], block_input.shape[2]
    tok = tok2 // 2
    width = 8 * fb_rows
    heads = w_qkv.shape[3] // HEAD_DIM
    hd = heads * HEAD_DIM
    hw = round_up(hd, 128)
    hp = heads * HEAD_PAD
    hid = w_up.shape[2]
    kh = round_up(hid, 384)
    kp = round_up(3 * hd, 128)
    up_a = 2 * kh // 3
    zrow = w_qkv.shape[1]
    zin = zrow == fb_rows and nz == 4

    wq, wo = jnp.transpose(w_qkv[0], (1, 0, 2)), jnp.transpose(w_out[:, 0, :])
    wu, wd = w_up[0], jnp.transpose(w_down[:, 0, :])
    if not zin:

        def gather(w, cols):
            w = jnp.pad(w, ((0, 0), (0, cols - w.shape[1])))
            return lax.all_gather(lax.all_gather(w, "dp", axis=0, tiled=True), "gy", axis=0, tiled=True)

        wq = gather(w_qkv[0].reshape(zrow, 3 * hd), kp)
        wo, wu, wd = gather(wo, hw), gather(wu, kh), gather(wd, kh)

    win = max(width, kh) // 3
    if win % 128:
        raise ValueError("window")
    cfg = dict(nz=nz, zin=zin, fb=fb_rows, tok=tok, heads=heads, hw=hw, kp=kp)
    tb = tok // 4
    half = width // 2
    vm = pltpu.VMEM
    n_sems = 118 + nz + (12 * nz if zin else 12)
    dw_specs = [pl.BlockSpec(memory_space=pl.ANY)] * 4
    if zin:
        dw_shapes = (jax.ShapeDtypeStruct((3, fb_rows, hw), F32),)
        dw_shapes += tuple(jax.ShapeDtypeStruct((fb_rows, k), F32) for k in (hw, kh, kh))
        core_shapes = [vm((half, k), BF16) for k in (kp, hw, up_a, kh, kh - up_a)]
        z_shapes = [vm((4, fb_rows, k), BF16) for k in (kp, hw, up_a, kh, kh - up_a)]
    else:
        dw_shapes = tuple(jax.ShapeDtypeStruct((width, k), BF16) for k in (kp, hw, kh, kh))
        core_shapes = [vm((16, 128), BF16)] * 5
        z_shapes = [vm((16, 128), BF16)] * 5
    scratch = [
        vm((8, 256), F32),
        vm((8, 8, 256), F32),
        vm((width, 128), F32),
        vm((width, tok), BF16),
        vm((width, tok), BF16),
        vm((width, tok), BF16),
        vm((width, tok), BF16),
        vm((width, tok), BF16),
        vm((width, kp), BF16),
        vm((width, hw), BF16),
        vm((width, kh), BF16),
        vm((width, kh), BF16),
        vm((3 * hp, tok), BF16),
        vm((4 * hd, tok), BF16),
        vm((4 * hd, width), BF16),
        vm((hp, tb), BF16),
        vm((kh, tok), BF16),
        vm((kh, tok), BF16),
        vm((width, tb), F32),
        vm((3, width, tb), BF16),
        vm((6, fb_rows, tok), BF16),
        vm((6, fb_rows, tok), BF16),
        vm((2, fb_rows, tok), BF16),
        vm((2, fb_rows, tok), BF16),
        vm((hd, tb), F32),
        vm((max(width, kh), tb), F32),
        vm((max(width, kh), tb), F32),
        vm((tok, 128), jnp.int32),
        vm((4 + 2 * heads, 8, tok), F32),
        vm((max(width, kh), 128), F32),
        vm((tok // 64, 128), F32),
        vm((8, tok // 64, 128), F32),
        vm((8, max(width, kh)), F32),
        vm((8, max(width, kh)), F32),
        vm((8, max(width, kh)), F32),
        vm((4, 8, win), F32),
        vm((nz, 16, win), F32),
        *core_shapes,
        *z_shapes,
        vm((fb_rows, tok2), BF16),
        vm((fb_rows, tok2), F32),
        pltpu.SemaphoreType.DMA((n_sems,)),
        pltpu.SemaphoreType.DMA((n_sems,)),
    ]
    any_spec = pl.BlockSpec(memory_space=pl.ANY)
    vmem_spec = pl.BlockSpec(memory_space=pltpu.VMEM)
    w_spec = vmem_spec if zin else any_spec
    out, ig, dq, do, du, dd, sm = pl.pallas_call(
        functools.partial(block_kernel, cfg),
        out_shape=(
            jax.ShapeDtypeStruct((fb_rows, tok2), BF16),
            jax.ShapeDtypeStruct((fb_rows, tok2), F32),
            *dw_shapes,
            jax.ShapeDtypeStruct((16, win), F32),
        ),
        in_specs=[pl.BlockSpec(memory_space=pltpu.SMEM)] + [vmem_spec] * 7 + [any_spec] + [w_spec] * 4 + [vmem_spec] * 2,
        out_specs=(any_spec, any_spec, *dw_specs, vmem_spec),
        scratch_shapes=scratch,
        compiler_params=pltpu.CompilerParams(
            collective_id=0, has_side_effects=True, vmem_limit_bytes=67043328
        ),
        name="encoder_block",
    )(
        lengths,
        ln1_gain,
        ln1_bias,
        out_bias,
        ln2_gain,
        ln2_bias,
        down_bias,
        block_input[0],
        cotangent[0],
        wq,
        wo,
        wu,
        wd,
        qv_bias,
        up_bias,
    )

    if not zin:

        def reduce(a):
            a = lax.psum_scatter(a, "gy", scatter_dimension=0, tiled=True)
            return lax.optimization_barrier(lax.psum_scatter(a, "dp", scatter_dimension=0, tiled=True)).astype(F32)

        dq, do, du, dd = reduce(dq), reduce(do), reduce(du), reduce(dd)
        dq = jnp.transpose(dq[:, : 3 * hd].reshape(zrow, 3, hd), (1, 0, 2))

    shapes = [(fb_rows, tok2, BF16), (fb_rows, tok2, F32)] + [(1, fb_rows, F32)] * 6 + [(2, hd, F32), (hid, F32)]
    shapes = [jax.ShapeDtypeStruct(a[:-1], a[-1]) for a in shapes]
    given = []
    if zin:
        given = [dq, do, du, dd]
        shapes += [jax.ShapeDtypeStruct((3, fb_rows, hd), F32), jax.ShapeDtypeStruct((fb_rows, hd), F32)]
        shapes += [jax.ShapeDtypeStruct((fb_rows, hid), F32)] * 2
    final = pl.pallas_call(
        functools.partial(finish_kernel, dict(fb=fb_rows, hd=hd, n_dw=len(given))),
        out_shape=tuple(shapes),
        in_specs=[vmem_spec] * (3 + len(given)),
        out_specs=(vmem_spec,) * len(shapes),
        compiler_params=pltpu.CompilerParams(vmem_limit_bytes=67043328),
        name="finish",
    )(out, ig, sm, *given)
    out, ig, g1, b1, ob, g2, b2, db, qv, up = final[:10]
    if zin:
        dq, do, du, dd = final[10:]
    else:
        do, du, dd = do[:, :hd], du[:, :hid], dd[:, :hid]
    return (
        out[None],
        ig[None],
        g1,
        b1,
        jnp.transpose(dq, (1, 0, 2))[None],
        qv,
        jnp.transpose(do)[:, None, :],
        ob,
        g2,
        b2,
        du[None],
        up,
        jnp.transpose(dd)[:, None, :],
        db,
    )


def solution(mesh):
    in_specs = (
        P("gy", "gx", "dp"),
        P(("dp", "gy"), None),
        P("gy", "gx"),
        P("gy", "gx"),
        P("gy", "dp", None, "gx"),
        P(None, "gx"),
        P("gx", "gy", "dp"),
        P("gy", "gx"),
        P("gy", "gx"),
        P("gy", "gx"),
        P("gy", "dp", "gx"),
        P("gx"),
        P("gx", "gy", "dp"),
        P("gy", "gx"),
        P("gy", "gx", "dp"),
    )
    out_specs = (
        P("gy", "gx", "dp"),
        P("gy", "gx", "dp"),
        P("gy", "gx"),
        P("gy", "gx"),
        P("gy", "dp", None, "gx"),
        P(None, "gx"),
        P("gx", "gy", "dp"),
        P("gy", "gx"),
        P("gy", "gx"),
        P("gy", "gx"),
        P("gy", "dp", "gx"),
        P("gx"),
        P("gx", "gy", "dp"),
        P("gy", "gx"),
    )
    return jax.shard_map(local, mesh=mesh, in_specs=in_specs, out_specs=out_specs, check_vma=False)
```
